8 devices in a mesh: tp: 4 (over z, y, x), dp: 2 (over core).
Axes of the slice: x: 2, y: 2, z: 1, core: 2. Of those that a mesh axis runs over, the one named last changes fastest.
Arguments:
- x_in: bfloat16 [128, 3072], P(('dp', 'tp'))
- w_gate: bfloat16 [3072, 8192], P('dp', 'tp')
- w_up: bfloat16 [3072, 8192], P('dp', 'tp')
- w_down: bfloat16 [8192, 3072], P('tp', 'dp')
- grad_y: bfloat16 [128, 3072], P(('dp', 'tp'))
Outputs:
- output 1: bfloat16 [128, 3072], P(('dp', 'tp'))
- output 2: bfloat16 [128, 3072], P(('dp', 'tp'))
- output 3: float32 [3072, 8192], P('dp', 'tp')
- output 4: float32 [3072, 8192], P('dp', 'tp')
- output 5: float32 [8192, 3072], P('tp', 'dp')
All inputs are finite; a program needn't handle non-finite values.
Results may differ from the reference program's by a relative error of at most 0.001.
Values are sent between devices in bfloat16 or wider.
A program may use at most 1 GiB of HBM per device.

```python
import jax
import jax.numpy as jnp

D = 3072
FF = 8192
TOKENS = 128


def setup_inputs(seed: int = 0) -> dict:
    base_key = jax.random.key(seed)
    key_list = jax.random.split(base_key, 5)
    x_in = jax.random.normal(key_list[0], (TOKENS, D), jnp.float32).astype(jnp.bfloat16)
    w_gate = (jax.random.normal(key_list[1], (D, FF), jnp.float32) * D ** -0.5).astype(jnp.bfloat16)
    w_up = (jax.random.normal(key_list[2], (D, FF), jnp.float32) * D ** -0.5).astype(jnp.bfloat16)
    w_down = (jax.random.normal(key_list[3], (FF, D), jnp.float32) * FF ** -0.5).astype(jnp.bfloat16)
    grad_y = jax.random.normal(key_list[4], (TOKENS, D), jnp.float32).astype(jnp.bfloat16)
    return {"x_in": x_in, "w_gate": w_gate, "w_up": w_up, "w_down": w_down, "grad_y": grad_y}


def reference(x_in, w_gate, w_up, w_down, grad_y):
    gate_pre = jnp.dot(x_in, w_gate, preferred_element_type=jnp.float32)
    up_pre = jnp.dot(x_in, w_up, preferred_element_type=jnp.float32)
    sig_gate = jax.nn.sigmoid(gate_pre)
    silu_gate = gate_pre * sig_gate
    hidden = (silu_gate * up_pre).astype(jnp.bfloat16)
    y_out = (x_in.astype(jnp.float32) + jnp.dot(hidden, w_down, preferred_element_type=jnp.float32)).astype(jnp.bfloat16)
    grad_h = jnp.dot(grad_y, w_down.T, preferred_element_type=jnp.float32)
    silu_deriv = sig_gate * (1.0 + gate_pre * (1.0 - sig_gate))
    grad_gate = (grad_h * up_pre * silu_deriv).astype(jnp.bfloat16)
    grad_up = (grad_h * silu_gate).astype(jnp.bfloat16)
    grad_x = (grad_y.astype(jnp.float32)
              + jnp.dot(grad_gate, w_gate.T, preferred_element_type=jnp.float32)
              + jnp.dot(grad_up, w_up.T, preferred_element_type=jnp.float32)).astype(jnp.bfloat16)
    grad_w_gate = jnp.dot(x_in.T, grad_gate, preferred_element_type=jnp.float32)
    grad_w_up = jnp.dot(x_in.T, grad_up, preferred_element_type=jnp.float32)
    grad_w_down = jnp.dot(hidden.T, grad_y, preferred_element_type=jnp.float32)
    return (y_out, grad_x, grad_w_gate, grad_w_up, grad_w_down)
```

```python
import functools

import jax
import jax.numpy as jnp
from jax import lax
from jax.experimental import pallas as pl
from jax.experimental.pallas import tpu as pltpu
from jax.sharding import PartitionSpec as P

MESH = pl.DeviceIdType.MESH
F32 = jnp.float32
BF16 = jnp.bfloat16

NT = (((1,), (1,)), ((), ()))
TN = (((0,), (0,)), ((), ()))

FC = 512
DC = 512


def _front(x_hbm, wg_hbm, wu_hbm, wd_hbm, gy_hbm,
           y_ref, dx_ref, xc_out, gc_out, h_out, da_out, db_out,
           x_v, gy_v, wg, wu, wd, xc, gc,
           pa, pb, pg, ra, rb, rg, sd, h, da, db,
           yp, yr, dxp, dxr,
           w_sem, o_sem, xs, xrs, gs, grs, es, ers, ys, yrs, ds, drs):
    rows, d_full = x_v.shape
    tok, d_half = xc.shape
    ff = wg.shape[1]
    nf = ff // FC
    nd = d_half // DC
    t = lax.axis_index("tp")
    c = lax.axis_index("dp")
    ty, tx = t // 2, t % 2
    peers = []
    for kt in range(4):
        for kc in range(2):
            px = tx if kt % 2 == 0 else 1 - tx
            py = ty if kt // 2 == 0 else 1 - ty
            pc = c if kc == 0 else 1 - c
            peers.append((py * 2 + px, pc))
    order = (6, 7, 2, 3, 4, 5, 1)

    def dev(k):
        return {"tp": peers[k][0], "dp": peers[k][1]}

    def row_of(k):
        return pl.multiple_of((peers[k][1] * 4 + peers[k][0]) * rows, rows)

    def col_of(k):
        return pl.multiple_of(peers[k][1] * d_half, d_half)

    cx = pltpu.make_async_copy(x_hbm, x_v, w_sem.at[0])
    cg = pltpu.make_async_copy(gy_hbm, gy_v, w_sem.at[1])
    cw = [pltpu.make_async_copy(a, b, w_sem.at[2 + i])
          for i, (a, b) in enumerate(((wg_hbm, wg), (wu_hbm, wu), (wd_hbm, wd)))]
    cx.start()
    cg.start()
    for w in cw:
        w.start()

    barrier = pltpu.get_barrier_semaphore()
    for k in range(1, 8):
        pl.semaphore_signal(barrier, inc=1, device_id=dev(k), device_id_type=MESH)
    pl.semaphore_wait(barrier, 7)

    def remote(src, dst, ssem, rsem, k):
        return pltpu.make_async_remote_copy(src_ref=src, dst_ref=dst, send_sem=ssem, recv_sem=rsem,
                                            device_id=dev(k), device_id_type=MESH)

    def spread(own, cols, ssem, rsem):
        out = []
        for k in order:
            cp = remote(own.at[:, pl.ds(col_of(k), d_half)], cols.at[pl.ds(row_of(0), rows), :],
                        ssem.at[k], rsem.at[k], k)
            cp.start()
            out.append(cp)
        return out

    cx.wait()
    sx = spread(x_v, xc, xs, xrs)
    cg.wait()
    sg = spread(gy_v, gc, gs, grs)
    xc[pl.ds(row_of(0), rows), :] = x_v[:, pl.ds(col_of(0), d_half)]
    gc[pl.ds(row_of(0), rows), :] = gy_v[:, pl.ds(col_of(0), d_half)]

    cw[0].wait()
    cw[1].wait()
    for cp in sx:
        cp.wait_recv()
    outs = [pltpu.make_async_copy(xc, xc_out, o_sem.at[0])]
    outs[0].start()
    ex = []
    for j in range(nf):
        f = slice(j * FC, (j + 1) * FC)
        pa[j] = jnp.dot(xc[...], wg[:, f], preferred_element_type=F32)
        ea = remote(pa.at[j], ra.at[j], es.at[3 * j], ers.at[3 * j], 1)
        ea.start()
        pb[j] = jnp.dot(xc[...], wu[:, f], preferred_element_type=F32)
        eb = remote(pb.at[j], rb.at[j], es.at[3 * j + 1], ers.at[3 * j + 1], 1)
        eb.start()
        ex.append((ea, eb))

    rb_rows = 16

    for j in range(nf):
        f = slice(j * FC, (j + 1) * FC)
        ex[j][0].wait_recv()
        ex[j][1].wait_recv()

        def act(i, carry, j=j, f=f):
            r = pl.ds(pl.multiple_of(i * rb_rows, rb_rows), rb_rows)
            a = pa[j, r, :] + ra[j, r, :]
            b = pb[j, r, :] + rb[j, r, :]
            s = jax.nn.sigmoid(a)
            u = a * s
            h[r, f] = (u * b).astype(BF16)
            sd[j, r, :] = s * (1.0 + a * (1.0 - s))
            ra[j, r, :] = u
            rb[j, r, :] = b
            return carry

        lax.fori_loop(0, tok // rb_rows, act, 0)
    outs.append(pltpu.make_async_copy(h, h_out, o_sem.at[1]))
    outs[1].start()

    def reduce_rows(part, recv, n, ssem, rsem):
        out = []
        for k in order:
            cp = remote(part.at[pl.ds(row_of(k), rows), pl.ds(n * DC, DC)],
                        recv.at[k, :, pl.ds(n * DC, DC)],
                        ssem.at[k * nd + n], rsem.at[k * nd + n], k)
            cp.start()
            out.append(cp)
        return out

    cw[2].wait()
    sy = []
    for n in range(nd):
        yp[:, n * DC:(n + 1) * DC] = jnp.dot(h[...], wd[:, n * DC:(n + 1) * DC], preferred_element_type=F32)
        sy += reduce_rows(yp, yr, n, ys, yrs)

    for cp in sg:
        cp.wait_recv()
    outs.append(pltpu.make_async_copy(gc, gc_out, o_sem.at[2]))
    outs[2].start()
    eg = []
    for j in range(nf):
        pg[j] = lax.dot_general(gc[...], wd[j * FC:(j + 1) * FC, :], NT, preferred_element_type=F32)
        e = remote(pg.at[j], rg.at[j], es.at[3 * j + 2], ers.at[3 * j + 2], 1)
        e.start()
        eg.append(e)
    for j in range(nf):
        f = slice(j * FC, (j + 1) * FC)
        eg[j].wait_recv()

        def grad(i, carry, j=j, f=f):
            r = pl.ds(pl.multiple_of(i * rb_rows, rb_rows), rb_rows)
            g = pg[j, r, :] + rg[j, r, :]
            da[r, f] = (g * rb[j, r, :] * sd[j, r, :]).astype(BF16)
            db[r, f] = (g * ra[j, r, :]).astype(BF16)
            return carry

        lax.fori_loop(0, tok // rb_rows, grad, 0)
    outs.append(pltpu.make_async_copy(da, da_out, o_sem.at[3]))
    outs.append(pltpu.make_async_copy(db, db_out, o_sem.at[4]))
    outs[3].start()
    outs[4].start()

    sdx = []
    for n in range(nd):
        dxp[:, n * DC:(n + 1) * DC] = (
            lax.dot_general(da[...], wg[n * DC:(n + 1) * DC, :], NT, preferred_element_type=F32)
            + lax.dot_general(db[...], wu[n * DC:(n + 1) * DC, :], NT, preferred_element_type=F32))
        sdx += reduce_rows(dxp, dxr, n, ds, drs)

    def finish(own, part, recv, out_ref):
        for kc in range(2):
            cols = pl.ds(col_of(kc), d_half)
            if kc == 0:
                tot = part[pl.ds(row_of(0), rows), :] + recv[2] + recv[4] + recv[6]
            else:
                tot = recv[1] + recv[3] + recv[5] + recv[7]
            out_ref[:, cols] = (own[:, cols].astype(F32) + tot).astype(BF16)

    for cp in sy:
        cp.wait_recv()
    finish(x_v, yp, yr, y_ref)
    for cp in sdx:
        cp.wait_recv()
    finish(gy_v, dxp, dxr, dx_ref)

    for cp in sx + sg + sy + sdx + eg:
        cp.wait_send()
    for ea, eb in ex:
        ea.wait_send()
        eb.wait_send()
    for o in outs:
        o.wait()


def _grads(h, da, db, xc, gc, dwd_hbm, dwg_hbm, dwu_hbm, buf_d, buf_g, sem_d, sem_g):
    ff = h.shape[1]
    d_half = xc.shape[1]
    nb_d, tr_d = buf_d.shape[:2]
    nb_g, tr_g = buf_g.shape[:2]

    def run(lhs, rhs, out, buf, sem, n, tr, nb, start, prev_out):
        def step(i, carry):
            slot = lax.rem(i + start, nb)
            r = pl.multiple_of(i * tr, tr)

            def drain():
                pltpu.make_async_copy(buf.at[slot], prev_out.at[pl.ds(0, tr), :], sem.at[slot]).wait()

            if start >= nb:
                drain()
            else:
                pl.when(i + start >= nb)(drain)
            buf[slot] = lax.dot_general(lhs[:, pl.ds(r, tr)], rhs[...], TN, preferred_element_type=F32)
            pltpu.make_async_copy(buf.at[slot], out.at[pl.ds(r, tr), :], sem.at[slot]).start()
            return carry

        lax.fori_loop(0, n, step, 0)

    n_d = ff // tr_d
    n_g = d_half // tr_g
    run(h, gc, dwd_hbm, buf_d, sem_d, n_d, tr_d, nb_d, 0, dwd_hbm)
    run(xc, da, dwg_hbm, buf_g, sem_g, n_g, tr_g, nb_g, 0, dwg_hbm)
    run(xc, db, dwu_hbm, buf_g, sem_g, n_g, tr_g, nb_g, n_g, dwu_hbm)
    for s in range(nb_d):
        pltpu.make_async_copy(buf_d.at[s], dwd_hbm.at[pl.ds(0, tr_d), :], sem_d.at[s]).wait()
    for s in range(nb_g):
        pltpu.make_async_copy(buf_g.at[s], dwu_hbm.at[pl.ds(0, tr_g), :], sem_g.at[s]).wait()


def solution(mesh):
    def local_step(x, wg, wu, wd, gy):
        rows, d_full = x.shape
        d_half, ff = wg.shape
        tok = rows * 8
        nf = ff // FC
        nd = d_half // DC
        any_ = pl.BlockSpec(memory_space=pl.ANY)
        vm = pl.BlockSpec(memory_space=pltpu.VMEM)
        S = jax.ShapeDtypeStruct
        dma = pltpu.SemaphoreType.DMA
        part = pltpu.VMEM((nf, tok, FC), F32)
        y, dx, xc, gc, h, da, db = pl.pallas_call(
            _front,
            name="front",
            out_shape=(S((rows, d_full), BF16), S((rows, d_full), BF16),
                       S((tok, d_half), BF16), S((tok, d_half), BF16),
                       S((tok, ff), BF16), S((tok, ff), BF16), S((tok, ff), BF16)),
            in_specs=[any_] * 5,
            out_specs=(vm, vm) + (any_,) * 5,
            scratch_shapes=[
                pltpu.VMEM((rows, d_full), BF16), pltpu.VMEM((rows, d_full), BF16),
                pltpu.VMEM((d_half, ff), BF16), pltpu.VMEM((d_half, ff), BF16), pltpu.VMEM((ff, d_half), BF16),
                pltpu.VMEM((tok, d_half), BF16), pltpu.VMEM((tok, d_half), BF16),
                part, part, part, part, part, part, part,
                pltpu.VMEM((tok, ff), BF16), pltpu.VMEM((tok, ff), BF16), pltpu.VMEM((tok, ff), BF16),
                pltpu.VMEM((tok, d_half), F32), pltpu.VMEM((8, rows, d_half), F32),
                pltpu.VMEM((tok, d_half), F32), pltpu.VMEM((8, rows, d_half), F32),
                dma((5,)), dma((5,)), dma((8,)), dma((8,)), dma((8,)), dma((8,)),
                dma((3 * nf,)), dma((3 * nf,)),
                dma((8 * nd,)), dma((8 * nd,)), dma((8 * nd,)), dma((8 * nd,)),
            ],
            compiler_params=pltpu.CompilerParams(collective_id=0, has_side_effects=True,
                                                 vmem_limit_bytes=50 * 1024 * 1024),
        )(x, wg, wu, wd, gy)

        tr = 256
        dwd, dwg, dwu = pl.pallas_call(
            _grads,
            name="grads",
            out_shape=(S((ff, d_half), F32), S((d_half, ff), F32), S((d_half, ff), F32)),
            in_specs=[vm] * 5,
            out_specs=(any_, any_, any_),
            scratch_shapes=[pltpu.VMEM((8, tr, d_half), F32), pltpu.VMEM((6, tr, ff), F32),
                            dma((8,)), dma((6,))],
            compiler_params=pltpu.CompilerParams(vmem_limit_bytes=50 * 1024 * 1024),
        )(h, da, db, xc, gc)
        return y, dx, dwg, dwu, dwd

    row_spec = P(("dp", "tp"), None)
    up_spec = P("dp", "tp")
    down_spec = P("tp", "dp")
    return jax.shard_map(local_step, mesh=mesh,
                         in_specs=(row_spec, up_spec, up_spec, down_spec, row_spec),
                         out_specs=(row_spec, row_spec, up_spec, up_spec, down_spec),
                         check_vma=False)
```

```python
import functools

import jax
import jax.numpy as jnp
from jax import lax
from jax.experimental import pallas as pl
from jax.experimental.pallas import tpu as pltpu
from jax.sharding import PartitionSpec as P

MESH = pl.DeviceIdType.MESH
F32 = jnp.float32
BF16 = jnp.bfloat16

NT = (((1,), (1,)), ((), ()))
TN = (((0,), (0,)), ((), ()))


FC = 512
DC = 512


def _front(x_hbm, wg_hbm, wu_hbm, wd_hbm, gy_hbm,
           y_ref, xc_out, gc_out, h_out, da_out, db_out, p0, p1, p2, p3, p4, p5, p6, p7,
           x_v, gy_v, wg, wu, wd, xc, gc,
           pa, pb, pg, ra, rb, rg, sd, h, da, db,
           yp, yr, dxp,
           w_sem, o_sem, xs, xrs, gs, grs, es, ers, ys, yrs):
    rows, d_full = x_v.shape
    tok, d_half = xc.shape
    ff = wg.shape[1]
    nf = ff // FC
    nd = d_half // DC
    t = lax.axis_index("tp")
    c = lax.axis_index("dp")
    ty, tx = t // 2, t % 2
    peers = []
    for kt in range(4):
        for kc in range(2):
            px = tx if kt % 2 == 0 else 1 - tx
            py = ty if kt // 2 == 0 else 1 - ty
            pc = c if kc == 0 else 1 - c
            peers.append((py * 2 + px, pc))
    order = (6, 7, 2, 3, 4, 5, 1)

    def dev(k):
        return {"tp": peers[k][0], "dp": peers[k][1]}

    def row_of(k):
        return pl.multiple_of((peers[k][1] * 4 + peers[k][0]) * rows, rows)

    def col_of(k):
        return pl.multiple_of(peers[k][1] * d_half, d_half)

    cx = pltpu.make_async_copy(x_hbm, x_v, w_sem.at[0])
    cg = pltpu.make_async_copy(gy_hbm, gy_v, w_sem.at[1])
    cw = [pltpu.make_async_copy(a, b, w_sem.at[2 + i])
          for i, (a, b) in enumerate(((wg_hbm, wg), (wu_hbm, wu), (wd_hbm, wd)))]
    cx.start()
    cg.start()
    for w in cw:
        w.start()

    barrier = pltpu.get_barrier_semaphore()
    for k in range(1, 8):
        pl.semaphore_signal(barrier, inc=1, device_id=dev(k), device_id_type=MESH)
    pl.semaphore_wait(barrier, 7)

    def remote(src, dst, ssem, rsem, k):
        return pltpu.make_async_remote_copy(src_ref=src, dst_ref=dst, send_sem=ssem, recv_sem=rsem,
                                            device_id=dev(k), device_id_type=MESH)

    def spread(own, cols, ssem, rsem):
        out = []
        for k in order:
            cp = remote(own.at[:, pl.ds(col_of(k), d_half)], cols.at[pl.ds(row_of(0), rows), :],
                        ssem.at[k], rsem.at[k], k)
            cp.start()
            out.append(cp)
        return out

    cx.wait()
    sx = spread(x_v, xc, xs, xrs)
    cg.wait()
    sg = spread(gy_v, gc, gs, grs)
    xc[pl.ds(row_of(0), rows), :] = x_v[:, pl.ds(col_of(0), d_half)]
    gc[pl.ds(row_of(0), rows), :] = gy_v[:, pl.ds(col_of(0), d_half)]

    cw[0].wait()
    cw[1].wait()
    for cp in sx:
        cp.wait_recv()
    outs = [pltpu.make_async_copy(xc, xc_out, o_sem.at[0])]
    outs[0].start()
    ex = []
    for j in range(nf):
        f = slice(j * FC, (j + 1) * FC)
        pa[j] = jnp.dot(xc[...], wg[:, f], preferred_element_type=F32)
        ea = remote(pa.at[j], ra.at[j], es.at[3 * j], ers.at[3 * j], 1)
        ea.start()
        pb[j] = jnp.dot(xc[...], wu[:, f], preferred_element_type=F32)
        eb = remote(pb.at[j], rb.at[j], es.at[3 * j + 1], ers.at[3 * j + 1], 1)
        eb.start()
        ex.append((ea, eb))

    rb_rows = 16

    for j in range(nf):
        f = slice(j * FC, (j + 1) * FC)
        ex[j][0].wait_recv()
        ex[j][1].wait_recv()

        def act(i, carry, j=j, f=f):
            r = pl.ds(pl.multiple_of(i * rb_rows, rb_rows), rb_rows)
            a = pa[j, r, :] + ra[j, r, :]
            b = pb[j, r, :] + rb[j, r, :]
            s = jax.nn.sigmoid(a)
            u = a * s
            h[r, f] = (u * b).astype(BF16)
            sd[j, r, :] = s * (1.0 + a * (1.0 - s))
            ra[j, r, :] = u
            rb[j, r, :] = b
            return carry

        lax.fori_loop(0, tok // rb_rows, act, 0)
    outs.append(pltpu.make_async_copy(h, h_out, o_sem.at[1]))
    outs[1].start()

    def reduce_rows(part, recv, n, ssem, rsem):
        out = []
        for k in order:
            cp = remote(part.at[pl.ds(row_of(k), rows), pl.ds(n * DC, DC)],
                        recv.at[k, :, pl.ds(n * DC, DC)],
                        ssem.at[k * nd + n], rsem.at[k * nd + n], k)
            cp.start()
            out.append(cp)
        return out

    cw[2].wait()
    sy = []
    for n in range(nd):
        yp[:, n * DC:(n + 1) * DC] = jnp.dot(h[...], wd[:, n * DC:(n + 1) * DC], preferred_element_type=F32)
        sy += reduce_rows(yp, yr, n, ys, yrs)

    for cp in sg:
        cp.wait_recv()
    outs.append(pltpu.make_async_copy(gc, gc_out, o_sem.at[2]))
    outs[2].start()
    eg = []
    for j in range(nf):
        pg[j] = lax.dot_general(gc[...], wd[j * FC:(j + 1) * FC, :], NT, preferred_element_type=F32)
        e = remote(pg.at[j], rg.at[j], es.at[3 * j + 2], ers.at[3 * j + 2], 1)
        e.start()
        eg.append(e)
    for j in range(nf):
        f = slice(j * FC, (j + 1) * FC)
        eg[j].wait_recv()

        def grad(i, carry, j=j, f=f):
            r = pl.ds(pl.multiple_of(i * rb_rows, rb_rows), rb_rows)
            g = pg[j, r, :] + rg[j, r, :]
            da[r, f] = (g * rb[j, r, :] * sd[j, r, :]).astype(BF16)
            db[r, f] = (g * ra[j, r, :]).astype(BF16)
            return carry

        lax.fori_loop(0, tok // rb_rows, grad, 0)
    outs.append(pltpu.make_async_copy(da, da_out, o_sem.at[3]))
    outs.append(pltpu.make_async_copy(db, db_out, o_sem.at[4]))
    outs[3].start()
    outs[4].start()

    for n in range(nd):
        dxp[:, n * DC:(n + 1) * DC] = (
            lax.dot_general(da[...], wg[n * DC:(n + 1) * DC, :], NT, preferred_element_type=F32)
            + lax.dot_general(db[...], wu[n * DC:(n + 1) * DC, :], NT, preferred_element_type=F32))
    for k, p in enumerate((p0, p1, p2, p3, p4, p5, p6, p7)):
        p[...] = dxp[pl.ds(row_of(k), rows), :]

    def finish(own, part, recv, out_ref):
        for kc in range(2):
            cols = pl.ds(col_of(kc), d_half)
            if kc == 0:
                tot = part[pl.ds(row_of(0), rows), :] + recv[2] + recv[4] + recv[6]
            else:
                tot = recv[1] + recv[3] + recv[5] + recv[7]
            out_ref[:, cols] = (own[:, cols].astype(F32) + tot).astype(BF16)

    for cp in sy:
        cp.wait_recv()
    finish(x_v, yp, yr, y_ref)

    for cp in sx + sg + sy + eg:
        cp.wait_send()
    for ea, eb in ex:
        ea.wait_send()
        eb.wait_send()
    for o in outs:
        o.wait()


def _finish(gy, p0, r1, r2, r3, r4, r5, r6, r7, dx_ref):
    d_half = p0.shape[1]
    c = lax.axis_index("dp")
    mine = pl.ds(pl.multiple_of(c * d_half, d_half), d_half)
    other = pl.ds(pl.multiple_of((1 - c) * d_half, d_half), d_half)
    dx_ref[:, mine] = (gy[:, mine].astype(F32) + (p0[...] + r2[...] + r4[...] + r6[...])).astype(BF16)
    dx_ref[:, other] = (gy[:, other].astype(F32) + (r1[...] + r3[...] + r5[...] + r7[...])).astype(BF16)


def _grads(h, da, db, xc, gc, dwd_hbm, dwg_hbm, dwu_hbm, buf_d, buf_g, sem_d, sem_g):
    ff = h.shape[1]
    d_half = xc.shape[1]
    nb_d, tr_d = buf_d.shape[:2]
    nb_g, tr_g = buf_g.shape[:2]

    def run(lhs, rhs, out, buf, sem, n, tr, nb, start, prev_out):
        def step(i, carry):
            slot = lax.rem(i + start, nb)
            r = pl.multiple_of(i * tr, tr)

            def drain():
                pltpu.make_async_copy(buf.at[slot], prev_out.at[pl.ds(0, tr), :], sem.at[slot]).wait()

            if start >= nb:
                drain()
            else:
                pl.when(i + start >= nb)(drain)
            buf[slot] = lax.dot_general(lhs[:, pl.ds(r, tr)], rhs[...], TN, preferred_element_type=F32)
            pltpu.make_async_copy(buf.at[slot], out.at[pl.ds(r, tr), :], sem.at[slot]).start()
            return carry

        lax.fori_loop(0, n, step, 0)

    n_d = ff // tr_d
    n_g = d_half // tr_g
    run(h, gc, dwd_hbm, buf_d, sem_d, n_d, tr_d, nb_d, 0, dwd_hbm)
    run(xc, da, dwg_hbm, buf_g, sem_g, n_g, tr_g, nb_g, 0, dwg_hbm)
    run(xc, db, dwu_hbm, buf_g, sem_g, n_g, tr_g, nb_g, n_g, dwu_hbm)
    for s in range(nb_d):
        pltpu.make_async_copy(buf_d.at[s], dwd_hbm.at[pl.ds(0, tr_d), :], sem_d.at[s]).wait()
    for s in range(nb_g):
        pltpu.make_async_copy(buf_g.at[s], dwu_hbm.at[pl.ds(0, tr_g), :], sem_g.at[s]).wait()


def solution(mesh):
    def local_step(x, wg, wu, wd, gy):
        rows, d_full = x.shape
        d_half, ff = wg.shape
        tok = rows * 8
        nf = ff // FC
        nd = d_half // DC
        any_ = pl.BlockSpec(memory_space=pl.ANY)
        hbm = pl.BlockSpec(memory_space=pltpu.HBM)
        vm = pl.BlockSpec(memory_space=pltpu.VMEM)
        S = jax.ShapeDtypeStruct
        dma = pltpu.SemaphoreType.DMA
        part = pltpu.VMEM((nf, tok, FC), F32)
        y, xc, gc, h, da, db, *parts = pl.pallas_call(
            _front,
            name="front",
            out_shape=(S((rows, d_full), BF16),
                       S((tok, d_half), BF16), S((tok, d_half), BF16),
                       S((tok, ff), BF16), S((tok, ff), BF16), S((tok, ff), BF16))
            + (S((rows, d_half), F32),) * 8,
            in_specs=[hbm] * 5,
            out_specs=(vm,) + (any_,) * 5 + (vm,) * 8,
            scratch_shapes=[
                pltpu.VMEM((rows, d_full), BF16), pltpu.VMEM((rows, d_full), BF16),
                pltpu.VMEM((d_half, ff), BF16), pltpu.VMEM((d_half, ff), BF16), pltpu.VMEM((ff, d_half), BF16),
                pltpu.VMEM((tok, d_half), BF16), pltpu.VMEM((tok, d_half), BF16),
                part, part, part, part, part, part, part,
                pltpu.VMEM((tok, ff), BF16), pltpu.VMEM((tok, ff), BF16), pltpu.VMEM((tok, ff), BF16),
                pltpu.VMEM((tok, d_half), F32), pltpu.VMEM((8, rows, d_half), F32),
                pltpu.VMEM((tok, d_half), F32),
                dma((5,)), dma((5,)), dma((8,)), dma((8,)), dma((8,)), dma((8,)),
                dma((3 * nf,)), dma((3 * nf,)),
                dma((8 * nd,)), dma((8 * nd,)),
            ],
            compiler_params=pltpu.CompilerParams(collective_id=0, has_side_effects=True,
                                                 vmem_limit_bytes=50 * 1024 * 1024),
        )(pltpu.with_memory_space_constraint(x, pltpu.HBM), wg, wu, wd,
          pltpu.with_memory_space_constraint(gy, pltpu.HBM))
        got = [lax.ppermute(parts[k], ("tp", "dp"), [(i, i ^ k) for i in range(8)]) for k in (6, 7, 2, 3, 4, 5, 1)]
        got = dict(zip((6, 7, 2, 3, 4, 5, 1), got))

        tr = 256
        dwd, dwg, dwu = pl.pallas_call(
            _grads,
            name="grads",
            out_shape=(S((ff, d_half), F32), S((d_half, ff), F32), S((d_half, ff), F32)),
            in_specs=[vm] * 5,
            out_specs=(any_, any_, any_),
            scratch_shapes=[pltpu.VMEM((8, tr, d_half), F32), pltpu.VMEM((6, tr, ff), F32),
                            dma((8,)), dma((6,))],
            cost_estimate=pl.CostEstimate(flops=6 * tok * d_half * ff, bytes_accessed=12 * d_half * ff,
                                          transcendentals=0),
            compiler_params=pltpu.CompilerParams(vmem_limit_bytes=50 * 1024 * 1024),
        )(h, da, db, xc, gc)
        dx = pl.pallas_call(
            _finish,
            name="finish",
            out_shape=S((rows, d_full), BF16),
            in_specs=[vm] * 9,
            out_specs=vm,
            compiler_params=pltpu.CompilerParams(vmem_limit_bytes=4 * 1024 * 1024),
        )(gy, parts[0], *(got[k] for k in range(1, 8)))
        return y, dx, dwg, dwu, dwd

    row_spec = P(("dp", "tp"), None)
    up_spec = P("dp", "tp")
    down_spec = P("tp", "dp")
    return jax.shard_map(local_step, mesh=mesh,
                         in_specs=(row_spec, up_spec, up_spec, down_spec, row_spec),
                         out_specs=(row_spec, row_spec, up_spec, up_spec, down_spec),
                         check_vma=False)
```

```python
import functools

import jax
import jax.numpy as jnp
from jax import lax
from jax.experimental import pallas as pl
from jax.experimental.pallas import tpu as pltpu
from jax.sharding import PartitionSpec as P

MESH = pl.DeviceIdType.MESH
F32 = jnp.float32
BF16 = jnp.bfloat16

NT = (((1,), (1,)), ((), ()))
TN = (((0,), (0,)), ((), ()))

FC = 512
DC = 512
NY = 3


def _front(x_hbm, wg_hbm, wu_hbm, wd_hbm, gy_hbm,
           y_ref, xc_out, gc_out, h_out, da_out, db_out, p_out,
           x_v, gy_v, wg, wu, wd, xc, gc,
           pa, pb, pg, ra, rb, rg, sd, h, da, db,
           yp, yr, dxp,
           w_sem, o_sem, xs, xrs, gs, grs, es, ers, ys, yrs):
    rows, d_full = x_v.shape
    tok, d_half = xc.shape
    ff = wg.shape[1]
    nf = ff // FC
    nd = d_half // DC
    t = lax.axis_index("tp")
    c = lax.axis_index("dp")
    ty, tx = t // 2, t % 2
    peers = []
    for kt in range(4):
        for kc in range(2):
            px = tx if kt % 2 == 0 else 1 - tx
            py = ty if kt // 2 == 0 else 1 - ty
            pc = c if kc == 0 else 1 - c
            peers.append((py * 2 + px, pc))
    order = (6, 7, 2, 3, 4, 5, 1)

    def dev(k):
        return {"tp": peers[k][0], "dp": peers[k][1]}

    def row_of(k):
        return pl.multiple_of((peers[k][1] * 4 + peers[k][0]) * rows, rows)

    def col_of(k):
        return pl.multiple_of(peers[k][1] * d_half, d_half)

    cx = pltpu.make_async_copy(x_hbm, x_v, w_sem.at[0])
    cg = pltpu.make_async_copy(gy_hbm, gy_v, w_sem.at[1])
    cw = [pltpu.make_async_copy(a, b, w_sem.at[2 + i])
          for i, (a, b) in enumerate(((wg_hbm, wg), (wu_hbm, wu), (wd_hbm, wd)))]
    cx.start()
    cg.start()
    for w in cw:
        w.start()

    barrier = pltpu.get_barrier_semaphore()
    for k in range(1, 8):
        pl.semaphore_signal(barrier, inc=1, device_id=dev(k), device_id_type=MESH)
    pl.semaphore_wait(barrier, 7)

    def remote(src, dst, ssem, rsem, k):
        return pltpu.make_async_remote_copy(src_ref=src, dst_ref=dst, send_sem=ssem, recv_sem=rsem,
                                            device_id=dev(k), device_id_type=MESH)

    def spread(own, cols, ssem, rsem):
        out = []
        for k in order:
            cp = remote(own.at[:, pl.ds(col_of(k), d_half)], cols.at[pl.ds(row_of(0), rows), :],
                        ssem.at[k], rsem.at[k], k)
            cp.start()
            out.append(cp)
        return out

    cx.wait()
    sx = spread(x_v, xc, xs, xrs)
    cg.wait()
    sg = spread(gy_v, gc, gs, grs)
    xc[pl.ds(row_of(0), rows), :] = x_v[:, pl.ds(col_of(0), d_half)]
    gc[pl.ds(row_of(0), rows), :] = gy_v[:, pl.ds(col_of(0), d_half)]

    cw[0].wait()
    cw[1].wait()
    for cp in sx:
        cp.wait_recv()
    outs = [pltpu.make_async_copy(xc, xc_out, o_sem.at[0])]
    outs[0].start()
    ex = []
    for j in range(nf):
        f = slice(j * FC, (j + 1) * FC)
        pa[j] = jnp.dot(xc[...], wg[:, f], preferred_element_type=F32)
        ea = remote(pa.at[j], ra.at[j], es.at[3 * j], ers.at[3 * j], 1)
        ea.start()
        pb[j] = jnp.dot(xc[...], wu[:, f], preferred_element_type=F32)
        eb = remote(pb.at[j], rb.at[j], es.at[3 * j + 1], ers.at[3 * j + 1], 1)
        eb.start()
        ex.append((ea, eb))

    rb_rows = 16

    for j in range(nf):
        f = slice(j * FC, (j + 1) * FC)
        ex[j][0].wait_recv()
        ex[j][1].wait_recv()

        def act(i, carry, j=j, f=f):
            r = pl.ds(pl.multiple_of(i * rb_rows, rb_rows), rb_rows)
            a = pa[j, r, :] + ra[j, r, :]
            b = pb[j, r, :] + rb[j, r, :]
            s = jax.nn.sigmoid(a)
            u = a * s
            h[r, f] = (u * b).astype(BF16)
            sd[j, r, :] = s * (1.0 + a * (1.0 - s))
            ra[j, r, :] = u
            rb[j, r, :] = b
            return carry

        lax.fori_loop(0, tok // rb_rows, act, 0)
    outs.append(pltpu.make_async_copy(h, h_out, o_sem.at[1]))
    outs[1].start()

    def reduce_rows(part, recv, n, ssem, rsem):
        out = []
        for k in order:
            cp = remote(part.at[pl.ds(row_of(k), rows), pl.ds(n * DC, DC)],
                        recv.at[k, :, pl.ds(n * DC, DC)],
                        ssem.at[k * nd + n], rsem.at[k * nd + n], k)
            cp.start()
            out.append(cp)
        return out

    cw[2].wait()
    sy = []
    for n in range(nd):
        yp[:, n * DC:(n + 1) * DC] = jnp.dot(h[...], wd[:, n * DC:(n + 1) * DC], preferred_element_type=F32)
        if n < NY:
            sy += reduce_rows(yp, yr, n, ys, yrs)

    for cp in sg:
        cp.wait_recv()
    outs.append(pltpu.make_async_copy(gc, gc_out, o_sem.at[2]))
    outs[2].start()
    eg = []
    for j in range(nf):
        pg[j] = lax.dot_general(gc[...], wd[j * FC:(j + 1) * FC, :], NT, preferred_element_type=F32)
        e = remote(pg.at[j], rg.at[j], es.at[3 * j + 2], ers.at[3 * j + 2], 1)
        e.start()
        eg.append(e)
    for j in range(nf):
        f = slice(j * FC, (j + 1) * FC)
        eg[j].wait_recv()

        def grad(i, carry, j=j, f=f):
            r = pl.ds(pl.multiple_of(i * rb_rows, rb_rows), rb_rows)
            g = pg[j, r, :] + rg[j, r, :]
            da[r, f] = (g * rb[j, r, :] * sd[j, r, :]).astype(BF16)
            db[r, f] = (g * ra[j, r, :]).astype(BF16)
            return carry

        lax.fori_loop(0, tok // rb_rows, grad, 0)
    outs.append(pltpu.make_async_copy(da, da_out, o_sem.at[3]))
    outs.append(pltpu.make_async_copy(db, db_out, o_sem.at[4]))
    outs[3].start()
    outs[4].start()

    for n in range(nd):
        dxp[:, n * DC:(n + 1) * DC] = (
            lax.dot_general(da[...], wg[n * DC:(n + 1) * DC, :], NT, preferred_element_type=F32)
            + lax.dot_general(db[...], wu[n * DC:(n + 1) * DC, :], NT, preferred_element_type=F32))
    for i in range(8):
        r = ((i % 2) * 4 + i // 2) * rows
        p_out[i, :, :d_half] = dxp[r:r + rows, :]
        if NY < nd:
            p_out[i, :, d_half:] = yp[r:r + rows, NY * DC:]

    for cp in sy:
        cp.wait_recv()
    wy = NY * DC
    for kc in range(2 if NY else 0):
        cols = pl.ds(col_of(kc), wy)
        if kc == 0:
            tot = yp[pl.ds(row_of(0), rows), :wy] + yr[2, :, :wy] + yr[4, :, :wy] + yr[6, :, :wy]
        else:
            tot = yr[1, :, :wy] + yr[3, :, :wy] + yr[5, :, :wy] + yr[7, :, :wy]
        y_ref[:, cols] = (x_v[:, cols].astype(F32) + tot).astype(BF16)

    for cp in sx + sg + sy + eg:
        cp.wait_send()
    for ea, eb in ex:
        ea.wait_send()
        eb.wait_send()
    for o in outs:
        o.wait()


def _finish(x, gy, y_part, p, y_ref, dx_ref):
    d_half = x.shape[1] // 2
    wy = NY * DC
    for q in range(2):
        o = q * d_half
        tot = p[q] + p[q + 2] + p[q + 4] + p[q + 6]
        dx_ref[:, o:o + d_half] = (gy[:, o:o + d_half].astype(F32) + tot[:, :d_half]).astype(BF16)
        if NY:
            y_ref[:, o:o + wy] = y_part[:, o:o + wy]
        if wy < d_half:
            y_ref[:, o + wy:o + d_half] = (x[:, o + wy:o + d_half].astype(F32) + tot[:, d_half:]).astype(BF16)


def _grads(h, da, db, xc, gc, dwd_hbm, dwg_hbm, dwu_hbm, buf_d, buf_g, sem_d, sem_g):
    ff = h.shape[1]
    d_half = xc.shape[1]
    nb_d, tr_d = buf_d.shape[:2]
    nb_g, tr_g = buf_g.shape[:2]

    def run(lhs, rhs, out, buf, sem, n, tr, nb, start, prev_out):
        def step(i, carry):
            slot = lax.rem(i + start, nb)
            r = pl.multiple_of(i * tr, tr)

            def drain():
                pltpu.make_async_copy(buf.at[slot], prev_out.at[pl.ds(0, tr), :], sem.at[slot]).wait()

            if start >= nb:
                drain()
            else:
                pl.when(i + start >= nb)(drain)
            buf[slot] = lax.dot_general(lhs[:, pl.ds(r, tr)], rhs[...], TN, preferred_element_type=F32)
            pltpu.make_async_copy(buf.at[slot], out.at[pl.ds(r, tr), :], sem.at[slot]).start()
            return carry

        lax.fori_loop(0, n, step, 0)

    n_d = ff // tr_d
    n_g = d_half // tr_g
    run(h, gc, dwd_hbm, buf_d, sem_d, n_d, tr_d, nb_d, 0, dwd_hbm)
    run(xc, da, dwg_hbm, buf_g, sem_g, n_g, tr_g, nb_g, 0, dwg_hbm)
    run(xc, db, dwu_hbm, buf_g, sem_g, n_g, tr_g, nb_g, n_g, dwu_hbm)
    for s in range(nb_d):
        pltpu.make_async_copy(buf_d.at[s], dwd_hbm.at[pl.ds(0, tr_d), :], sem_d.at[s]).wait()
    for s in range(nb_g):
        pltpu.make_async_copy(buf_g.at[s], dwu_hbm.at[pl.ds(0, tr_g), :], sem_g.at[s]).wait()


def solution(mesh):
    def local_step(x, wg, wu, wd, gy):
        rows, d_full = x.shape
        d_half, ff = wg.shape
        tok = rows * 8
        nf = ff // FC
        nd = d_half // DC
        any_ = pl.BlockSpec(memory_space=pl.ANY)
        hbm = pl.BlockSpec(memory_space=pltpu.HBM)
        vm = pl.BlockSpec(memory_space=pltpu.VMEM)
        S = jax.ShapeDtypeStruct
        dma = pltpu.SemaphoreType.DMA
        part = pltpu.VMEM((nf, tok, FC), F32)
        y, xc, gc, h, da, db, parts = pl.pallas_call(
            _front,
            name="front",
            out_shape=(S((rows, d_full), BF16),
                       S((tok, d_half), BF16), S((tok, d_half), BF16),
                       S((tok, ff), BF16), S((tok, ff), BF16), S((tok, ff), BF16))
            + (S((8, rows, 2 * d_half - NY * DC), F32),),
            in_specs=[hbm] * 5,
            out_specs=(vm,) + (any_,) * 5 + (vm,),
            scratch_shapes=[
                pltpu.VMEM((rows, d_full), BF16), pltpu.VMEM((rows, d_full), BF16),
                pltpu.VMEM((d_half, ff), BF16), pltpu.VMEM((d_half, ff), BF16), pltpu.VMEM((ff, d_half), BF16),
                pltpu.VMEM((tok, d_half), BF16), pltpu.VMEM((tok, d_half), BF16),
                part, part, part, part, part, part, part,
                pltpu.VMEM((tok, ff), BF16), pltpu.VMEM((tok, ff), BF16), pltpu.VMEM((tok, ff), BF16),
                pltpu.VMEM((tok, d_half), F32), pltpu.VMEM((8, rows, d_half), F32),
                pltpu.VMEM((tok, d_half), F32),
                dma((5,)), dma((5,)), dma((8,)), dma((8,)), dma((8,)), dma((8,)),
                dma((3 * nf,)), dma((3 * nf,)),
                dma((8 * nd,)), dma((8 * nd,)),
            ],
            compiler_params=pltpu.CompilerParams(collective_id=0, has_side_effects=True,
                                                 vmem_limit_bytes=50 * 1024 * 1024),
        )(pltpu.with_memory_space_constraint(x, pltpu.HBM), wg, wu, wd,
          pltpu.with_memory_space_constraint(gy, pltpu.HBM))
        parts = lax.all_to_all(parts, ("tp", "dp"), 0, 0, tiled=True)

        tr = 256
        dwd, dwg, dwu = pl.pallas_call(
            _grads,
            name="grads",
            out_shape=(S((ff, d_half), F32), S((d_half, ff), F32), S((d_half, ff), F32)),
            in_specs=[vm] * 5,
            out_specs=(any_, any_, any_),
            scratch_shapes=[pltpu.VMEM((8, tr, d_half), F32), pltpu.VMEM((6, tr, ff), F32),
                            dma((8,)), dma((6,))],
            cost_estimate=pl.CostEstimate(flops=6 * tok * d_half * ff, bytes_accessed=12 * d_half * ff,
                                          transcendentals=0),
            compiler_params=pltpu.CompilerParams(vmem_limit_bytes=50 * 1024 * 1024),
        )(h, da, db, xc, gc)
        y, dx = pl.pallas_call(
            _finish,
            name="finish",
            out_shape=(S((rows, d_full), BF16), S((rows, d_full), BF16)),
            in_specs=[vm] * 4,
            out_specs=(vm, vm),
            compiler_params=pltpu.CompilerParams(vmem_limit_bytes=6 * 1024 * 1024),
        )(x, gy, y, parts)
        return y, dx, dwg, dwu, dwd

    row_spec = P(("dp", "tp"), None)
    up_spec = P("dp", "tp")
    down_spec = P("tp", "dp")
    return jax.shard_map(local_step, mesh=mesh,
                         in_specs=(row_spec, up_spec, up_spec, down_spec, row_spec),
                         out_specs=(row_spec, row_spec, up_spec, up_spec, down_spec),
                         check_vma=False)
```

```python
import functools

import jax
import jax.numpy as jnp
from jax import lax
from jax.experimental import pallas as pl
from jax.experimental.pallas import tpu as pltpu
from jax.sharding import PartitionSpec as P

MESH = pl.DeviceIdType.MESH
F32 = jnp.float32
BF16 = jnp.bfloat16

NT = (((1,), (1,)), ((), ()))
TN = (((0,), (0,)), ((), ()))

FC = 512
DC = 512
NY = 1


def _front(x_hbm, wg_hbm, wu_hbm, wd_hbm, gy_hbm,
           y_ref, xc_out, gc_out, h_out, da_out, db_out, p_out,
           x_v, gy_v, wg, wu, wd, xc, gc,
           pa, pb, pg, ra, rb, rg, sd, h, da, db,
           yp, yr, dxp,
           w_sem, o_sem, xs, xrs, gs, grs, es, ers, ys, yrs):
    rows, d_full = x_v.shape
    tok, d_half = xc.shape
    ff = wg.shape[1]
    nf = ff // FC
    nd = d_half // DC
    t = lax.axis_index("tp")
    c = lax.axis_index("dp")
    ty, tx = t // 2, t % 2
    peers = []
    for kt in range(4):
        for kc in range(2):
            px = tx if kt % 2 == 0 else 1 - tx
            py = ty if kt // 2 == 0 else 1 - ty
            pc = c if kc == 0 else 1 - c
            peers.append((py * 2 + px, pc))
    order = (6, 7, 2, 3, 4, 5, 1)

    def dev(k):
        return {"tp": peers[k][0], "dp": peers[k][1]}

    def row_of(k):
        return pl.multiple_of((peers[k][1] * 4 + peers[k][0]) * rows, rows)

    def col_of(k):
        return pl.multiple_of(peers[k][1] * d_half, d_half)

    cx = pltpu.make_async_copy(x_hbm, x_v, w_sem.at[0])
    cg = pltpu.make_async_copy(gy_hbm, gy_v, w_sem.at[1])
    cw = [pltpu.make_async_copy(a, b, w_sem.at[2 + i])
          for i, (a, b) in enumerate(((wg_hbm, wg), (wu_hbm, wu), (wd_hbm, wd)))]
    cx.start()
    cg.start()
    for w in cw:
        w.start()

    barrier = pltpu.get_barrier_semaphore()
    for k in range(1, 8):
        pl.semaphore_signal(barrier, inc=1, device_id=dev(k), device_id_type=MESH)
    pl.semaphore_wait(barrier, 7)

    def remote(src, dst, ssem, rsem, k):
        return pltpu.make_async_remote_copy(src_ref=src, dst_ref=dst, send_sem=ssem, recv_sem=rsem,
                                            device_id=dev(k), device_id_type=MESH)

    def spread(own, cols, ssem, rsem):
        out = []
        for k in order:
            cp = remote(own.at[:, pl.ds(col_of(k), d_half)], cols.at[pl.ds(row_of(0), rows), :],
                        ssem.at[k], rsem.at[k], k)
            cp.start()
            out.append(cp)
        return out

    cx.wait()
    sx = spread(x_v, xc, xs, xrs)
    cg.wait()
    sg = spread(gy_v, gc, gs, grs)
    xc[pl.ds(row_of(0), rows), :] = x_v[:, pl.ds(col_of(0), d_half)]
    gc[pl.ds(row_of(0), rows), :] = gy_v[:, pl.ds(col_of(0), d_half)]

    cw[0].wait()
    cw[1].wait()
    for cp in sx:
        cp.wait_recv()
    outs = [pltpu.make_async_copy(xc, xc_out, o_sem.at[0])]
    outs[0].start()
    ex = []
    for j in range(nf):
        f = slice(j * FC, (j + 1) * FC)
        pa[j] = jnp.dot(xc[...], wg[:, f], preferred_element_type=F32)
        ea = remote(pa.at[j], ra.at[j], es.at[3 * j], ers.at[3 * j], 1)
        ea.start()
        pb[j] = jnp.dot(xc[...], wu[:, f], preferred_element_type=F32)
        eb = remote(pb.at[j], rb.at[j], es.at[3 * j + 1], ers.at[3 * j + 1], 1)
        eb.start()
        ex.append((ea, eb))

    rb_rows = 16

    for j in range(nf):
        f = slice(j * FC, (j + 1) * FC)
        ex[j][0].wait_recv()
        ex[j][1].wait_recv()

        def act(i, carry, j=j, f=f):
            r = pl.ds(pl.multiple_of(i * rb_rows, rb_rows), rb_rows)
            a = pa[j, r, :] + ra[j, r, :]
            b = pb[j, r, :] + rb[j, r, :]
            s = jax.nn.sigmoid(a)
            u = a * s
            h[r, f] = (u * b).astype(BF16)
            sd[j, r, :] = s * (1.0 + a * (1.0 - s))
            ra[j, r, :] = u
            rb[j, r, :] = b
            return carry

        lax.fori_loop(0, tok // rb_rows, act, 0)
    outs.append(pltpu.make_async_copy(h, h_out, o_sem.at[1]))
    outs[1].start()

    def reduce_rows(part, recv, n, ssem, rsem):
        out = []
        for k in order:
            cp = remote(part.at[pl.ds(row_of(k), rows), pl.ds(n * DC, DC)],
                        recv.at[k, :, pl.ds(n * DC, DC)],
                        ssem.at[k * nd + n], rsem.at[k * nd + n], k)
            cp.start()
            out.append(cp)
        return out

    cw[2].wait()
    sy = []
    for n in range(nd):
        yp[:, n * DC:(n + 1) * DC] = jnp.dot(h[...], wd[:, n * DC:(n + 1) * DC], preferred_element_type=F32)
        if n < NY:
            sy += reduce_rows(yp, yr, n, ys, yrs)

    for cp in sg:
        cp.wait_recv()
    outs.append(pltpu.make_async_copy(gc, gc_out, o_sem.at[2]))
    outs[2].start()
    eg = []
    for j in range(nf):
        pg[j] = lax.dot_general(gc[...], wd[j * FC:(j + 1) * FC, :], NT, preferred_element_type=F32)
        e = remote(pg.at[j], rg.at[j], es.at[3 * j + 2], ers.at[3 * j + 2], 1)
        e.start()
        eg.append(e)
    for j in range(nf):
        f = slice(j * FC, (j + 1) * FC)
        eg[j].wait_recv()

        def grad(i, carry, j=j, f=f):
            r = pl.ds(pl.multiple_of(i * rb_rows, rb_rows), rb_rows)
            g = pg[j, r, :] + rg[j, r, :]
            da[r, f] = (g * rb[j, r, :] * sd[j, r, :]).astype(BF16)
            db[r, f] = (g * ra[j, r, :]).astype(BF16)
            return carry

        lax.fori_loop(0, tok // rb_rows, grad, 0)
    outs.append(pltpu.make_async_copy(da, da_out, o_sem.at[3]))
    outs.append(pltpu.make_async_copy(db, db_out, o_sem.at[4]))
    outs[3].start()
    outs[4].start()

    for n in range(nd):
        dxp[:, n * DC:(n + 1) * DC] = (
            lax.dot_general(da[...], wg[n * DC:(n + 1) * DC, :], NT, preferred_element_type=F32)
            + lax.dot_general(db[...], wu[n * DC:(n + 1) * DC, :], NT, preferred_element_type=F32))
    for i in range(8):
        r = ((i % 2) * 4 + i // 2) * rows
        p_out[i, :, :d_half] = dxp[r:r + rows, :]
        if NY < nd:
            p_out[i, :, d_half:] = yp[r:r + rows, NY * DC:]

    for cp in sy:
        cp.wait_recv()
    wy = NY * DC
    for kc in range(2 if NY else 0):
        cols = pl.ds(col_of(kc), wy)
        if kc == 0:
            tot = yp[pl.ds(row_of(0), rows), :wy] + yr[2, :, :wy] + yr[4, :, :wy] + yr[6, :, :wy]
        else:
            tot = yr[1, :, :wy] + yr[3, :, :wy] + yr[5, :, :wy] + yr[7, :, :wy]
        y_ref[:, cols] = (x_v[:, cols].astype(F32) + tot).astype(BF16)

    for cp in sx + sg + sy + eg:
        cp.wait_send()
    for ea, eb in ex:
        ea.wait_send()
        eb.wait_send()
    for o in outs:
        o.wait()


def _finish(x, gy, y_part, p, y_ref, dx_ref):
    d_half = x.shape[1] // 2
    wy = NY * DC
    for q in range(2):
        o = q * d_half
        tot = p[q] + p[q + 2] + p[q + 4] + p[q + 6]
        dx_ref[:, o:o + d_half] = (gy[:, o:o + d_half].astype(F32) + tot[:, :d_half]).astype(BF16)
        if NY:
            y_ref[:, o:o + wy] = y_part[:, o:o + wy]
        if wy < d_half:
            y_ref[:, o + wy:o + d_half] = (x[:, o + wy:o + d_half].astype(F32) + tot[:, d_half:]).astype(BF16)


def _grads(h, da, db, xc, gc, dwd_hbm, dwg_hbm, dwu_hbm, buf_d, buf_g, sem_d, sem_g):
    ff = h.shape[1]
    d_half = xc.shape[1]
    nb_d, tr_d = buf_d.shape[:2]
    nb_g, tr_g = buf_g.shape[:2]

    def run(lhs, rhs, out, buf, sem, n, tr, nb, start, prev_out):
        def step(i, carry):
            slot = lax.rem(i + start, nb)
            r = pl.multiple_of(i * tr, tr)

            def drain():
                pltpu.make_async_copy(buf.at[slot], prev_out.at[pl.ds(0, tr), :], sem.at[slot]).wait()

            if start >= nb:
                drain()
            else:
                pl.when(i + start >= nb)(drain)
            buf[slot] = lax.dot_general(lhs[:, pl.ds(r, tr)], rhs[...], TN, preferred_element_type=F32)
            pltpu.make_async_copy(buf.at[slot], out.at[pl.ds(r, tr), :], sem.at[slot]).start()
            return carry

        lax.fori_loop(0, n, step, 0)

    n_d = ff // tr_d
    n_g = d_half // tr_g
    run(h, gc, dwd_hbm, buf_d, sem_d, n_d, tr_d, nb_d, 0, dwd_hbm)
    run(xc, da, dwg_hbm, buf_g, sem_g, n_g, tr_g, nb_g, 0, dwg_hbm)
    run(xc, db, dwu_hbm, buf_g, sem_g, n_g, tr_g, nb_g, n_g, dwu_hbm)
    for s in range(nb_d):
        pltpu.make_async_copy(buf_d.at[s], dwd_hbm.at[pl.ds(0, tr_d), :], sem_d.at[s]).wait()
    for s in range(nb_g):
        pltpu.make_async_copy(buf_g.at[s], dwu_hbm.at[pl.ds(0, tr_g), :], sem_g.at[s]).wait()


def solution(mesh):
    def local_step(x, wg, wu, wd, gy):
        rows, d_full = x.shape
        d_half, ff = wg.shape
        tok = rows * 8
        nf = ff // FC
        nd = d_half // DC
        any_ = pl.BlockSpec(memory_space=pl.ANY)
        hbm = pl.BlockSpec(memory_space=pltpu.HBM)
        vm = pl.BlockSpec(memory_space=pltpu.VMEM)
        S = jax.ShapeDtypeStruct
        dma = pltpu.SemaphoreType.DMA
        part = pltpu.VMEM((nf, tok, FC), F32)
        y, xc, gc, h, da, db, parts = pl.pallas_call(
            _front,
            name="front",
            out_shape=(S((rows, d_full), BF16),
                       S((tok, d_half), BF16), S((tok, d_half), BF16),
                       S((tok, ff), BF16), S((tok, ff), BF16), S((tok, ff), BF16))
            + (S((8, rows, 2 * d_half - NY * DC), F32),),
            in_specs=[hbm] * 5,
            out_specs=(vm,) + (any_,) * 5 + (vm,),
            scratch_shapes=[
                pltpu.VMEM((rows, d_full), BF16), pltpu.VMEM((rows, d_full), BF16),
                pltpu.VMEM((d_half, ff), BF16), pltpu.VMEM((d_half, ff), BF16), pltpu.VMEM((ff, d_half), BF16),
                pltpu.VMEM((tok, d_half), BF16), pltpu.VMEM((tok, d_half), BF16),
                part, part, part, part, part, part, part,
                pltpu.VMEM((tok, ff), BF16), pltpu.VMEM((tok, ff), BF16), pltpu.VMEM((tok, ff), BF16),
                pltpu.VMEM((tok, d_half), F32), pltpu.VMEM((8, rows, d_half), F32),
                pltpu.VMEM((tok, d_half), F32),
                dma((5,)), dma((5,)), dma((8,)), dma((8,)), dma((8,)), dma((8,)),
                dma((3 * nf,)), dma((3 * nf,)),
                dma((8 * nd,)), dma((8 * nd,)),
            ],
            compiler_params=pltpu.CompilerParams(collective_id=0, has_side_effects=True,
                                                 vmem_limit_bytes=50 * 1024 * 1024),
        )(pltpu.with_memory_space_constraint(x, pltpu.HBM), wg, wu, wd,
          pltpu.with_memory_space_constraint(gy, pltpu.HBM))
        parts = lax.all_to_all(parts, ("tp", "dp"), 0, 0, tiled=True)

        tr = 256
        dwd, dwg, dwu = pl.pallas_call(
            _grads,
            name="grads",
            out_shape=(S((ff, d_half), F32), S((d_half, ff), F32), S((d_half, ff), F32)),
            in_specs=[vm] * 5,
            out_specs=(any_, any_, any_),
            scratch_shapes=[pltpu.VMEM((8, tr, d_half), F32), pltpu.VMEM((6, tr, ff), F32),
                            dma((8,)), dma((6,))],
            cost_estimate=pl.CostEstimate(flops=6 * tok * d_half * ff, bytes_accessed=12 * d_half * ff,
                                          transcendentals=0),
            compiler_params=pltpu.CompilerParams(vmem_limit_bytes=50 * 1024 * 1024),
        )(h, da, db, xc, gc)
        y, dx = pl.pallas_call(
            _finish,
            name="finish",
            out_shape=(S((rows, d_full), BF16), S((rows, d_full), BF16)),
            in_specs=[vm] * 4,
            out_specs=(vm, vm),
            compiler_params=pltpu.CompilerParams(vmem_limit_bytes=6 * 1024 * 1024),
        )(x, gy, y, parts)
        return y, dx, dwg, dwu, dwd

    row_spec = P(("dp", "tp"), None)
    up_spec = P("dp", "tp")
    down_spec = P("tp", "dp")
    return jax.shard_map(local_step, mesh=mesh,
                         in_specs=(row_spec, up_spec, up_spec, down_spec, row_spec),
                         out_specs=(row_spec, row_spec, up_spec, up_spec, down_spec),
                         check_vma=False)
```

```python
import functools

import jax
import jax.numpy as jnp
from jax import lax
from jax.experimental import pallas as pl
from jax.experimental.pallas import tpu as pltpu
from jax.sharding import PartitionSpec as P

MESH = pl.DeviceIdType.MESH
F32 = jnp.float32
BF16 = jnp.bfloat16

NT = (((1,), (1,)), ((), ()))
TN = (((0,), (0,)), ((), ()))

FC = 512
DC = 512
NY = 3


def _front(x_hbm, wg_hbm, wu_hbm, wd_hbm, gy_hbm,
           y_ref, xc_out, gc_out, h_out, da_out, db_out, p_out,
           x_v, gy_v, wg, wu, wd, xc, gc,
           pa, pb, pg, ra, rb, rg, sd, h, da, db,
           yp, yr, dxp,
           w_sem, o_sem, xs, xrs, gs, grs, es, ers, ys, yrs):
    rows, d_full = x_v.shape
    tok, d_half = xc.shape
    ff = wg.shape[1]
    nf = ff // FC
    nd = d_half // DC
    t = lax.axis_index("tp")
    c = lax.axis_index("dp")
    ty, tx = t // 2, t % 2
    peers = []
    for kt in range(4):
        for kc in range(2):
            px = tx if kt % 2 == 0 else 1 - tx
            py = ty if kt // 2 == 0 else 1 - ty
            pc = c if kc == 0 else 1 - c
            peers.append((py * 2 + px, pc))
    order = (6, 7, 2, 3, 4, 5, 1)

    def dev(k):
        return {"tp": peers[k][0], "dp": peers[k][1]}

    def row_of(k):
        return pl.multiple_of((peers[k][1] * 4 + peers[k][0]) * rows, rows)

    def col_of(k):
        return pl.multiple_of(peers[k][1] * d_half, d_half)

    cx = pltpu.make_async_copy(x_hbm, x_v, w_sem.at[0])
    cg = pltpu.make_async_copy(gy_hbm, gy_v, w_sem.at[1])
    cw = [pltpu.make_async_copy(a, b, w_sem.at[2 + i])
          for i, (a, b) in enumerate(((wg_hbm, wg), (wu_hbm, wu), (wd_hbm, wd)))]
    cx.start()
    cg.start()

    barrier = pltpu.get_barrier_semaphore()
    for k in range(1, 8):
        pl.semaphore_signal(barrier, inc=1, device_id=dev(k), device_id_type=MESH)
    pl.semaphore_wait(barrier, 7)

    def remote(src, dst, ssem, rsem, k):
        return pltpu.make_async_remote_copy(src_ref=src, dst_ref=dst, send_sem=ssem, recv_sem=rsem,
                                            device_id=dev(k), device_id_type=MESH)

    def spread(own, cols, ssem, rsem):
        out = []
        for k in order:
            cp = remote(own.at[:, pl.ds(col_of(k), d_half)], cols.at[pl.ds(row_of(0), rows), :],
                        ssem.at[k], rsem.at[k], k)
            cp.start()
            out.append(cp)
        return out

    cx.wait()
    sx = spread(x_v, xc, xs, xrs)
    cg.wait()
    sg = spread(gy_v, gc, gs, grs)
    for w in cw:
        w.start()
    xc[pl.ds(row_of(0), rows), :] = x_v[:, pl.ds(col_of(0), d_half)]
    gc[pl.ds(row_of(0), rows), :] = gy_v[:, pl.ds(col_of(0), d_half)]

    cw[0].wait()
    cw[1].wait()
    for cp in sx:
        cp.wait_recv()
    outs = [pltpu.make_async_copy(xc, xc_out, o_sem.at[0])]
    outs[0].start()
    ex = []
    for j in range(nf):
        f = slice(j * FC, (j + 1) * FC)
        pa[j] = jnp.dot(xc[...], wg[:, f], preferred_element_type=F32)
        ea = remote(pa.at[j], ra.at[j], es.at[3 * j], ers.at[3 * j], 1)
        ea.start()
        pb[j] = jnp.dot(xc[...], wu[:, f], preferred_element_type=F32)
        eb = remote(pb.at[j], rb.at[j], es.at[3 * j + 1], ers.at[3 * j + 1], 1)
        eb.start()
        ex.append((ea, eb))

    rb_rows = 16

    for j in range(nf):
        f = slice(j * FC, (j + 1) * FC)
        ex[j][0].wait_recv()
        ex[j][1].wait_recv()

        def act(i, carry, j=j, f=f):
            r = pl.ds(pl.multiple_of(i * rb_rows, rb_rows), rb_rows)
            a = pa[j, r, :] + ra[j, r, :]
            b = pb[j, r, :] + rb[j, r, :]
            s = jax.nn.sigmoid(a)
            u = a * s
            h[r, f] = (u * b).astype(BF16)
            sd[j, r, :] = s * (1.0 + a * (1.0 - s))
            ra[j, r, :] = u
            rb[j, r, :] = b
            return carry

        lax.fori_loop(0, tok // rb_rows, act, 0)
    outs.append(pltpu.make_async_copy(h, h_out, o_sem.at[1]))
    outs[1].start()

    def reduce_rows(part, recv, n, ssem, rsem):
        out = []
        for k in order:
            cp = remote(part.at[pl.ds(row_of(k), rows), pl.ds(n * DC, DC)],
                        recv.at[k, :, pl.ds(n * DC, DC)],
                        ssem.at[k * nd + n], rsem.at[k * nd + n], k)
            cp.start()
            out.append(cp)
        return out

    cw[2].wait()
    sy = []
    for n in range(nd):
        yp[:, n * DC:(n + 1) * DC] = jnp.dot(h[...], wd[:, n * DC:(n + 1) * DC], preferred_element_type=F32)
        if n < NY:
            sy += reduce_rows(yp, yr, n, ys, yrs)

    for cp in sg:
        cp.wait_recv()
    outs.append(pltpu.make_async_copy(gc, gc_out, o_sem.at[2]))
    outs[2].start()
    eg = []
    for j in range(nf):
        pg[j] = lax.dot_general(gc[...], wd[j * FC:(j + 1) * FC, :], NT, preferred_element_type=F32)
        e = remote(pg.at[j], rg.at[j], es.at[3 * j + 2], ers.at[3 * j + 2], 1)
        e.start()
        eg.append(e)
    for j in range(nf):
        f = slice(j * FC, (j + 1) * FC)
        eg[j].wait_recv()

        def grad(i, carry, j=j, f=f):
            r = pl.ds(pl.multiple_of(i * rb_rows, rb_rows), rb_rows)
            g = pg[j, r, :] + rg[j, r, :]
            da[r, f] = (g * rb[j, r, :] * sd[j, r, :]).astype(BF16)
            db[r, f] = (g * ra[j, r, :]).astype(BF16)
            return carry

        lax.fori_loop(0, tok // rb_rows, grad, 0)
    outs.append(pltpu.make_async_copy(da, da_out, o_sem.at[3]))
    outs.append(pltpu.make_async_copy(db, db_out, o_sem.at[4]))
    outs[3].start()
    outs[4].start()

    for n in range(nd):
        dxp[:, n * DC:(n + 1) * DC] = (
            lax.dot_general(da[...], wg[n * DC:(n + 1) * DC, :], NT, preferred_element_type=F32)
            + lax.dot_general(db[...], wu[n * DC:(n + 1) * DC, :], NT, preferred_element_type=F32))
    for i in range(8):
        r = ((i % 2) * 4 + i // 2) * rows
        p_out[i, :, :d_half] = dxp[r:r + rows, :]
        if NY < nd:
            p_out[i, :, d_half:] = yp[r:r + rows, NY * DC:]

    for cp in sy:
        cp.wait_recv()
    wy = NY * DC
    for kc in range(2 if NY else 0):
        cols = pl.ds(col_of(kc), wy)
        if kc == 0:
            tot = yp[pl.ds(row_of(0), rows), :wy] + yr[2, :, :wy] + yr[4, :, :wy] + yr[6, :, :wy]
        else:
            tot = yr[1, :, :wy] + yr[3, :, :wy] + yr[5, :, :wy] + yr[7, :, :wy]
        y_ref[:, cols] = (x_v[:, cols].astype(F32) + tot).astype(BF16)

    for cp in sx + sg + sy + eg:
        cp.wait_send()
    for ea, eb in ex:
        ea.wait_send()
        eb.wait_send()
    for o in outs:
        o.wait()


def _finish(x, gy, y_part, p, y_ref, dx_ref):
    d_half = x.shape[1] // 2
    wy = NY * DC
    for q in range(2):
        o = q * d_half
        tot = p[q] + p[q + 2] + p[q + 4] + p[q + 6]
        dx_ref[:, o:o + d_half] = (gy[:, o:o + d_half].astype(F32) + tot[:, :d_half]).astype(BF16)
        if NY:
            y_ref[:, o:o + wy] = y_part[:, o:o + wy]
        if wy < d_half:
            y_ref[:, o + wy:o + d_half] = (x[:, o + wy:o + d_half].astype(F32) + tot[:, d_half:]).astype(BF16)


def _grads(h, da, db, xc, gc, dwd_hbm, dwg_hbm, dwu_hbm, buf_d, buf_g, sem_d, sem_g):
    ff = h.shape[1]
    d_half = xc.shape[1]
    nb_d, tr_d = buf_d.shape[:2]
    nb_g, tr_g = buf_g.shape[:2]

    def run(lhs, rhs, out, buf, sem, n, tr, nb, start, prev_out):
        def step(i, carry):
            slot = lax.rem(i + start, nb)
            r = pl.multiple_of(i * tr, tr)

            def drain():
                pltpu.make_async_copy(buf.at[slot], prev_out.at[pl.ds(0, tr), :], sem.at[slot]).wait()

            if start >= nb:
                drain()
            else:
                pl.when(i + start >= nb)(drain)
            buf[slot] = lax.dot_general(lhs[:, pl.ds(r, tr)], rhs[...], TN, preferred_element_type=F32)
            pltpu.make_async_copy(buf.at[slot], out.at[pl.ds(r, tr), :], sem.at[slot]).start()
            return carry

        lax.fori_loop(0, n, step, 0)

    n_d = ff // tr_d
    n_g = d_half // tr_g
    run(h, gc, dwd_hbm, buf_d, sem_d, n_d, tr_d, nb_d, 0, dwd_hbm)
    run(xc, da, dwg_hbm, buf_g, sem_g, n_g, tr_g, nb_g, 0, dwg_hbm)
    run(xc, db, dwu_hbm, buf_g, sem_g, n_g, tr_g, nb_g, n_g, dwu_hbm)
    for s in range(nb_d):
        pltpu.make_async_copy(buf_d.at[s], dwd_hbm.at[pl.ds(0, tr_d), :], sem_d.at[s]).wait()
    for s in range(nb_g):
        pltpu.make_async_copy(buf_g.at[s], dwu_hbm.at[pl.ds(0, tr_g), :], sem_g.at[s]).wait()


def solution(mesh):
    def local_step(x, wg, wu, wd, gy):
        rows, d_full = x.shape
        d_half, ff = wg.shape
        tok = rows * 8
        nf = ff // FC
        nd = d_half // DC
        any_ = pl.BlockSpec(memory_space=pl.ANY)
        hbm = pl.BlockSpec(memory_space=pltpu.HBM)
        vm = pl.BlockSpec(memory_space=pltpu.VMEM)
        S = jax.ShapeDtypeStruct
        dma = pltpu.SemaphoreType.DMA
        part = pltpu.VMEM((nf, tok, FC), F32)
        y, xc, gc, h, da, db, parts = pl.pallas_call(
            _front,
            name="front",
            out_shape=(S((rows, d_full), BF16),
                       S((tok, d_half), BF16), S((tok, d_half), BF16),
                       S((tok, ff), BF16), S((tok, ff), BF16), S((tok, ff), BF16))
            + (S((8, rows, 2 * d_half - NY * DC), F32),),
            in_specs=[hbm] * 5,
            out_specs=(vm,) + (any_,) * 5 + (vm,),
            scratch_shapes=[
                pltpu.VMEM((rows, d_full), BF16), pltpu.VMEM((rows, d_full), BF16),
                pltpu.VMEM((d_half, ff), BF16), pltpu.VMEM((d_half, ff), BF16), pltpu.VMEM((ff, d_half), BF16),
                pltpu.VMEM((tok, d_half), BF16), pltpu.VMEM((tok, d_half), BF16),
                part, part, part, part, part, part, part,
                pltpu.VMEM((tok, ff), BF16), pltpu.VMEM((tok, ff), BF16), pltpu.VMEM((tok, ff), BF16),
                pltpu.VMEM((tok, d_half), F32), pltpu.VMEM((8, rows, d_half), F32),
                pltpu.VMEM((tok, d_half), F32),
                dma((5,)), dma((5,)), dma((8,)), dma((8,)), dma((8,)), dma((8,)),
                dma((3 * nf,)), dma((3 * nf,)),
                dma((8 * nd,)), dma((8 * nd,)),
            ],
            compiler_params=pltpu.CompilerParams(collective_id=0, has_side_effects=True,
                                                 vmem_limit_bytes=50 * 1024 * 1024),
        )(pltpu.with_memory_space_constraint(x, pltpu.HBM), wg, wu, wd,
          pltpu.with_memory_space_constraint(gy, pltpu.HBM))
        parts = lax.all_to_all(parts, ("tp", "dp"), 0, 0, tiled=True)

        tr = 256
        dwd, dwg, dwu = pl.pallas_call(
            _grads,
            name="grads",
            out_shape=(S((ff, d_half), F32), S((d_half, ff), F32), S((d_half, ff), F32)),
            in_specs=[vm] * 5,
            out_specs=(any_, any_, any_),
            scratch_shapes=[pltpu.VMEM((8, tr, d_half), F32), pltpu.VMEM((6, tr, ff), F32),
                            dma((8,)), dma((6,))],
            cost_estimate=pl.CostEstimate(flops=6 * tok * d_half * ff, bytes_accessed=12 * d_half * ff,
                                          transcendentals=0),
            compiler_params=pltpu.CompilerParams(vmem_limit_bytes=50 * 1024 * 1024),
        )(h, da, db, xc, gc)
        y, dx = pl.pallas_call(
            _finish,
            name="finish",
            out_shape=(S((rows, d_full), BF16), S((rows, d_full), BF16)),
            in_specs=[vm] * 4,
            out_specs=(vm, vm),
            compiler_params=pltpu.CompilerParams(vmem_limit_bytes=6 * 1024 * 1024),
        )(x, gy, y, parts)
        return y, dx, dwg, dwu, dwd

    row_spec = P(("dp", "tp"), None)
    up_spec = P("dp", "tp")
    down_spec = P("tp", "dp")
    return jax.shard_map(local_step, mesh=mesh,
                         in_specs=(row_spec, up_spec, up_spec, down_spec, row_spec),
                         out_specs=(row_spec, row_spec, up_spec, up_spec, down_spec),
                         check_vma=False)
```

```python
import functools

import jax
import jax.numpy as jnp
from jax import lax
from jax.experimental import pallas as pl
from jax.experimental.pallas import tpu as pltpu
from jax.sharding import PartitionSpec as P

MESH = pl.DeviceIdType.MESH
F32 = jnp.float32
BF16 = jnp.bfloat16

NT = (((1,), (1,)), ((), ()))
TN = (((0,), (0,)), ((), ()))

FC = 512
DC = 512
NY = 2


def _front(x_hbm, wg_hbm, wu_hbm, wd_hbm, gy_hbm,
           y_ref, xc_out, gc_out, h_out, da_out, db_out, p_out,
           x_v, gy_v, wg, wu, wd, xc, gc,
           pa, pb, pg, ra, rb, rg, sd, h, da, db,
           yp, yr, dxp,
           w_sem, o_sem, xs, xrs, gs, grs, es, ers, ys, yrs):
    rows, d_full = x_v.shape
    tok, d_half = xc.shape
    ff = wg.shape[1]
    nf = ff // FC
    nd = d_half // DC
    t = lax.axis_index("tp")
    c = lax.axis_index("dp")
    ty, tx = t // 2, t % 2
    peers = []
    for kt in range(4):
        for kc in range(2):
            px = tx if kt % 2 == 0 else 1 - tx
            py = ty if kt // 2 == 0 else 1 - ty
            pc = c if kc == 0 else 1 - c
            peers.append((py * 2 + px, pc))
    order = (6, 7, 2, 3, 4, 5, 1)

    def dev(k):
        return {"tp": peers[k][0], "dp": peers[k][1]}

    def row_of(k):
        return pl.multiple_of((peers[k][1] * 4 + peers[k][0]) * rows, rows)

    def col_of(k):
        return pl.multiple_of(peers[k][1] * d_half, d_half)

    cx = pltpu.make_async_copy(x_hbm, x_v, w_sem.at[0])
    cg = pltpu.make_async_copy(gy_hbm, gy_v, w_sem.at[1])
    cw = [pltpu.make_async_copy(a, b, w_sem.at[2 + i])
          for i, (a, b) in enumerate(((wg_hbm, wg), (wu_hbm, wu), (wd_hbm, wd)))]
    cx.start()
    cg.start()
    for w in cw:
        w.start()

    barrier = pltpu.get_barrier_semaphore()
    for k in range(1, 8):
        pl.semaphore_signal(barrier, inc=1, device_id=dev(k), device_id_type=MESH)
    pl.semaphore_wait(barrier, 7)

    def remote(src, dst, ssem, rsem, k):
        return pltpu.make_async_remote_copy(src_ref=src, dst_ref=dst, send_sem=ssem, recv_sem=rsem,
                                            device_id=dev(k), device_id_type=MESH)

    def spread(own, cols, ssem, rsem):
        out = []
        for k in order:
            cp = remote(own.at[:, pl.ds(col_of(k), d_half)], cols.at[pl.ds(row_of(0), rows), :],
                        ssem.at[k], rsem.at[k], k)
            cp.start()
            out.append(cp)
        return out

    cx.wait()
    sx = spread(x_v, xc, xs, xrs)
    xc[pl.ds(row_of(0), rows), :] = x_v[:, pl.ds(col_of(0), d_half)]
    cg.wait()
    for cp in sx:
        cp.wait_send()
    sg = spread(gy_v, gc, gs, grs)
    gc[pl.ds(row_of(0), rows), :] = gy_v[:, pl.ds(col_of(0), d_half)]

    cw[0].wait()
    cw[1].wait()
    for cp in sx:
        cp.wait_recv()
    outs = [pltpu.make_async_copy(xc, xc_out, o_sem.at[0])]
    outs[0].start()
    ex = []
    for j in range(nf):
        f = slice(j * FC, (j + 1) * FC)
        pa[j] = jnp.dot(xc[...], wg[:, f], preferred_element_type=F32)
        ea = remote(pa.at[j], ra.at[j], es.at[3 * j], ers.at[3 * j], 1)
        ea.start()
        pb[j] = jnp.dot(xc[...], wu[:, f], preferred_element_type=F32)
        eb = remote(pb.at[j], rb.at[j], es.at[3 * j + 1], ers.at[3 * j + 1], 1)
        eb.start()
        ex.append((ea, eb))

    rb_rows = 16

    for j in range(nf):
        f = slice(j * FC, (j + 1) * FC)
        ex[j][0].wait_recv()
        ex[j][1].wait_recv()

        def act(i, carry, j=j, f=f):
            r = pl.ds(pl.multiple_of(i * rb_rows, rb_rows), rb_rows)
            a = pa[j, r, :] + ra[j, r, :]
            b = pb[j, r, :] + rb[j, r, :]
            s = jax.nn.sigmoid(a)
            u = a * s
            h[r, f] = (u * b).astype(BF16)
            sd[j, r, :] = s * (1.0 + a * (1.0 - s))
            ra[j, r, :] = u
            rb[j, r, :] = b
            return carry

        lax.fori_loop(0, tok // rb_rows, act, 0)
    outs.append(pltpu.make_async_copy(h, h_out, o_sem.at[1]))
    outs[1].start()

    def reduce_rows(part, recv, n, ssem, rsem):
        out = []
        for k in order:
            cp = remote(part.at[pl.ds(row_of(k), rows), pl.ds(n * DC, DC)],
                        recv.at[k, :, pl.ds(n * DC, DC)],
                        ssem.at[k * nd + n], rsem.at[k * nd + n], k)
            cp.start()
            out.append(cp)
        return out

    cw[2].wait()
    sy = []
    for n in range(nd):
        yp[:, n * DC:(n + 1) * DC] = jnp.dot(h[...], wd[:, n * DC:(n + 1) * DC], preferred_element_type=F32)
        if n < NY:
            sy += reduce_rows(yp, yr, n, ys, yrs)

    for cp in sg:
        cp.wait_recv()
    outs.append(pltpu.make_async_copy(gc, gc_out, o_sem.at[2]))
    outs[2].start()
    eg = []
    for j in range(nf):
        pg[j] = lax.dot_general(gc[...], wd[j * FC:(j + 1) * FC, :], NT, preferred_element_type=F32)
        e = remote(pg.at[j], rg.at[j], es.at[3 * j + 2], ers.at[3 * j + 2], 1)
        e.start()
        eg.append(e)
    for j in range(nf):
        f = slice(j * FC, (j + 1) * FC)
        eg[j].wait_recv()

        def grad(i, carry, j=j, f=f):
            r = pl.ds(pl.multiple_of(i * rb_rows, rb_rows), rb_rows)
            g = pg[j, r, :] + rg[j, r, :]
            da[r, f] = (g * rb[j, r, :] * sd[j, r, :]).astype(BF16)
            db[r, f] = (g * ra[j, r, :]).astype(BF16)
            return carry

        lax.fori_loop(0, tok // rb_rows, grad, 0)
        for n in range(nd):
            o = slice(n * DC, (n + 1) * DC)
            part = (lax.dot_general(da[:, f], wg[o, f], NT, preferred_element_type=F32)
                    + lax.dot_general(db[:, f], wu[o, f], NT, preferred_element_type=F32))
            dxp[:, o] = part if j == 0 else dxp[:, o] + part
    outs.append(pltpu.make_async_copy(da, da_out, o_sem.at[3]))
    outs.append(pltpu.make_async_copy(db, db_out, o_sem.at[4]))
    outs[3].start()
    outs[4].start()
    for i in range(8):
        r = ((i % 2) * 4 + i // 2) * rows
        p_out[i, :, :d_half] = dxp[r:r + rows, :]
        if NY < nd:
            p_out[i, :, d_half:] = yp[r:r + rows, NY * DC:]

    for cp in sy:
        cp.wait_recv()
    wy = NY * DC
    for kc in range(2 if NY else 0):
        cols = pl.ds(col_of(kc), wy)
        if kc == 0:
            tot = yp[pl.ds(row_of(0), rows), :wy] + yr[2, :, :wy] + yr[4, :, :wy] + yr[6, :, :wy]
        else:
            tot = yr[1, :, :wy] + yr[3, :, :wy] + yr[5, :, :wy] + yr[7, :, :wy]
        y_ref[:, cols] = (x_v[:, cols].astype(F32) + tot).astype(BF16)

    for cp in sg + sy + eg:
        cp.wait_send()
    for ea, eb in ex:
        ea.wait_send()
        eb.wait_send()
    for o in outs:
        o.wait()


def _finish(x, gy, y_part, p, y_ref, dx_ref):
    d_half = x.shape[1] // 2
    wy = NY * DC
    for q in range(2):
        o = q * d_half
        tot = p[q] + p[q + 2] + p[q + 4] + p[q + 6]
        dx_ref[:, o:o + d_half] = (gy[:, o:o + d_half].astype(F32) + tot[:, :d_half]).astype(BF16)
        if NY:
            y_ref[:, o:o + wy] = y_part[:, o:o + wy]
        if wy < d_half:
            y_ref[:, o + wy:o + d_half] = (x[:, o + wy:o + d_half].astype(F32) + tot[:, d_half:]).astype(BF16)


def _grads(h, da, db, xc, gc, dwd_hbm, dwg_hbm, dwu_hbm, buf_d, buf_g, sem_d, sem_g):
    ff = h.shape[1]
    d_half = xc.shape[1]
    nb_d, tr_d = buf_d.shape[:2]
    nb_g, tr_g = buf_g.shape[:2]

    def run(lhs, rhs, out, buf, sem, n, tr, nb, start, prev_out):
        def step(i, carry):
            slot = lax.rem(i + start, nb)
            r = pl.multiple_of(i * tr, tr)

            def drain():
                pltpu.make_async_copy(buf.at[slot], prev_out.at[pl.ds(0, tr), :], sem.at[slot]).wait()

            if start >= nb:
                drain()
            else:
                pl.when(i + start >= nb)(drain)
            buf[slot] = lax.dot_general(lhs[:, pl.ds(r, tr)], rhs[...], TN, preferred_element_type=F32)
            pltpu.make_async_copy(buf.at[slot], out.at[pl.ds(r, tr), :], sem.at[slot]).start()
            return carry

        lax.fori_loop(0, n, step, 0)

    n_d = ff // tr_d
    n_g = d_half // tr_g
    run(h, gc, dwd_hbm, buf_d, sem_d, n_d, tr_d, nb_d, 0, dwd_hbm)
    run(xc, da, dwg_hbm, buf_g, sem_g, n_g, tr_g, nb_g, 0, dwg_hbm)
    run(xc, db, dwu_hbm, buf_g, sem_g, n_g, tr_g, nb_g, n_g, dwu_hbm)
    for s in range(nb_d):
        pltpu.make_async_copy(buf_d.at[s], dwd_hbm.at[pl.ds(0, tr_d), :], sem_d.at[s]).wait()
    for s in range(nb_g):
        pltpu.make_async_copy(buf_g.at[s], dwu_hbm.at[pl.ds(0, tr_g), :], sem_g.at[s]).wait()


def solution(mesh):
    def local_step(x, wg, wu, wd, gy):
        rows, d_full = x.shape
        d_half, ff = wg.shape
        tok = rows * 8
        nf = ff // FC
        nd = d_half // DC
        any_ = pl.BlockSpec(memory_space=pl.ANY)
        hbm = pl.BlockSpec(memory_space=pltpu.HBM)
        vm = pl.BlockSpec(memory_space=pltpu.VMEM)
        S = jax.ShapeDtypeStruct
        dma = pltpu.SemaphoreType.DMA
        part = pltpu.VMEM((nf, tok, FC), F32)
        y, xc, gc, h, da, db, parts = pl.pallas_call(
            _front,
            name="front",
            out_shape=(S((rows, d_full), BF16),
                       S((tok, d_half), BF16), S((tok, d_half), BF16),
                       S((tok, ff), BF16), S((tok, ff), BF16), S((tok, ff), BF16))
            + (S((8, rows, 2 * d_half - NY * DC), F32),),
            in_specs=[hbm] * 5,
            out_specs=(vm,) + (any_,) * 5 + (vm,),
            scratch_shapes=[
                pltpu.VMEM((rows, d_full), BF16), pltpu.VMEM((rows, d_full), BF16),
                pltpu.VMEM((d_half, ff), BF16), pltpu.VMEM((d_half, ff), BF16), pltpu.VMEM((ff, d_half), BF16),
                pltpu.VMEM((tok, d_half), BF16), pltpu.VMEM((tok, d_half), BF16),
                part, part, part, part, part, part, part,
                pltpu.VMEM((tok, ff), BF16), pltpu.VMEM((tok, ff), BF16), pltpu.VMEM((tok, ff), BF16),
                pltpu.VMEM((tok, d_half), F32), pltpu.VMEM((8, rows, d_half), F32),
                pltpu.VMEM((tok, d_half), F32),
                dma((5,)), dma((5,)), dma((8,)), dma((8,)), dma((8,)), dma((8,)),
                dma((3 * nf,)), dma((3 * nf,)),
                dma((8 * nd,)), dma((8 * nd,)),
            ],
            compiler_params=pltpu.CompilerParams(collective_id=0, has_side_effects=True,
                                                 vmem_limit_bytes=40 * 1024 * 1024),
        )(pltpu.with_memory_space_constraint(x, pltpu.HBM), wg, wu, wd,
          pltpu.with_memory_space_constraint(gy, pltpu.HBM))
        parts = lax.all_to_all(parts, ("tp", "dp"), 0, 0, tiled=True)

        tr = 256
        dwd, dwg, dwu = pl.pallas_call(
            _grads,
            name="grads",
            out_shape=(S((ff, d_half), F32), S((d_half, ff), F32), S((d_half, ff), F32)),
            in_specs=[vm] * 5,
            out_specs=(any_, any_, any_),
            scratch_shapes=[pltpu.VMEM((8, tr, d_half), F32), pltpu.VMEM((6, tr, ff), F32),
                            dma((8,)), dma((6,))],
            cost_estimate=pl.CostEstimate(flops=6 * tok * d_half * ff, bytes_accessed=12 * d_half * ff,
                                          transcendentals=0),
            compiler_params=pltpu.CompilerParams(vmem_limit_bytes=34 * 1024 * 1024),
        )(h, da, db, xc, gc)
        y, dx = pl.pallas_call(
            _finish,
            name="finish",
            out_shape=(S((rows, d_full), BF16), S((rows, d_full), BF16)),
            in_specs=[vm] * 4,
            out_specs=(vm, vm),
            compiler_params=pltpu.CompilerParams(vmem_limit_bytes=6 * 1024 * 1024),
        )(x, gy, y, parts)
        return y, dx, dwg, dwu, dwd

    row_spec = P(("dp", "tp"), None)
    up_spec = P("dp", "tp")
    down_spec = P("tp", "dp")
    return jax.shard_map(local_step, mesh=mesh,
                         in_specs=(row_spec, up_spec, up_spec, down_spec, row_spec),
                         out_specs=(row_spec, row_spec, up_spec, up_spec, down_spec),
                         check_vma=False)
```

```python
import functools

import jax
import jax.numpy as jnp
from jax import lax
from jax.experimental import pallas as pl
from jax.experimental.pallas import tpu as pltpu
from jax.sharding import PartitionSpec as P

MESH = pl.DeviceIdType.MESH
F32 = jnp.float32
BF16 = jnp.bfloat16

NT = (((1,), (1,)), ((), ()))
TN = (((0,), (0,)), ((), ()))

FC = 512
DC = 512
NY = 2


def _front(x_hbm, wg_hbm, wu_hbm, wd_hbm, gy_hbm,
           y_ref, xc_out, gc_out, h_out, da_out, db_out, p_out,
           x_v, gy_v, wg, wu, wd, xc, gc,
           pa, pb, pg, ra, rb, rg, sd, h, da, db,
           yp, yr, dxp,
           w_sem, o_sem, xs, xrs, gs, grs, es, ers, ys, yrs):
    rows, d_full = x_v.shape
    tok, d_half = xc.shape
    ff = wg.shape[1]
    nf = ff // FC
    nd = d_half // DC
    t = lax.axis_index("tp")
    c = lax.axis_index("dp")
    ty, tx = t // 2, t % 2
    peers = []
    for kt in range(4):
        for kc in range(2):
            px = tx if kt % 2 == 0 else 1 - tx
            py = ty if kt // 2 == 0 else 1 - ty
            pc = c if kc == 0 else 1 - c
            peers.append((py * 2 + px, pc))
    order = (6, 7, 2, 3, 4, 5, 1)

    def dev(k):
        return {"tp": peers[k][0], "dp": peers[k][1]}

    def row_of(k):
        return pl.multiple_of((peers[k][1] * 4 + peers[k][0]) * rows, rows)

    def col_of(k):
        return pl.multiple_of(peers[k][1] * d_half, d_half)

    cx = pltpu.make_async_copy(x_hbm, x_v, w_sem.at[0])
    cg = pltpu.make_async_copy(gy_hbm, gy_v, w_sem.at[1])
    cw = [pltpu.make_async_copy(a, b, w_sem.at[2 + i])
          for i, (a, b) in enumerate(((wg_hbm, wg), (wu_hbm, wu), (wd_hbm, wd)))]
    cx.start()
    cg.start()
    for w in cw:
        w.start()

    barrier = pltpu.get_barrier_semaphore()
    for k in range(1, 8):
        pl.semaphore_signal(barrier, inc=1, device_id=dev(k), device_id_type=MESH)
    pl.semaphore_wait(barrier, 7)

    def remote(src, dst, ssem, rsem, k):
        return pltpu.make_async_remote_copy(src_ref=src, dst_ref=dst, send_sem=ssem, recv_sem=rsem,
                                            device_id=dev(k), device_id_type=MESH)

    def spread(own, cols, ssem, rsem):
        out = []
        for k in order:
            cp = remote(own.at[:, pl.ds(col_of(k), d_half)], cols.at[pl.ds(row_of(0), rows), :],
                        ssem.at[k], rsem.at[k], k)
            cp.start()
            out.append(cp)
        return out

    cx.wait()
    sx = spread(x_v, xc, xs, xrs)
    xc[pl.ds(row_of(0), rows), :] = x_v[:, pl.ds(col_of(0), d_half)]
    cg.wait()
    for cp in sx:
        cp.wait_send()
    sg = spread(gy_v, gc, gs, grs)
    gc[pl.ds(row_of(0), rows), :] = gy_v[:, pl.ds(col_of(0), d_half)]

    cw[0].wait()
    cw[1].wait()
    for cp in sx:
        cp.wait_recv()
    outs = [pltpu.make_async_copy(xc, xc_out, o_sem.at[0])]
    outs[0].start()
    ex = []
    for j in range(nf):
        f = slice(j * FC, (j + 1) * FC)
        pa[j] = jnp.dot(xc[...], wg[:, f], preferred_element_type=F32)
        ea = remote(pa.at[j], ra.at[j], es.at[3 * j], ers.at[3 * j], 1)
        ea.start()
        pb[j] = jnp.dot(xc[...], wu[:, f], preferred_element_type=F32)
        eb = remote(pb.at[j], rb.at[j], es.at[3 * j + 1], ers.at[3 * j + 1], 1)
        eb.start()
        ex.append((ea, eb))

    rb_rows = 16

    for j in range(nf):
        f = slice(j * FC, (j + 1) * FC)
        ex[j][0].wait_recv()
        ex[j][1].wait_recv()

        def act(i, carry, j=j, f=f):
            r = pl.ds(pl.multiple_of(i * rb_rows, rb_rows), rb_rows)
            a = pa[j, r, :] + ra[j, r, :]
            b = pb[j, r, :] + rb[j, r, :]
            s = jax.nn.sigmoid(a)
            u = a * s
            h[r, f] = (u * b).astype(BF16)
            sd[j, r, :] = s * (1.0 + a * (1.0 - s))
            ra[j, r, :] = u
            rb[j, r, :] = b
            return carry

        lax.fori_loop(0, tok // rb_rows, act, 0)
    outs.append(pltpu.make_async_copy(h, h_out, o_sem.at[1]))
    outs[1].start()

    def reduce_rows(part, recv, n, ssem, rsem):
        out = []
        for k in order:
            cp = remote(part.at[pl.ds(row_of(k), rows), pl.ds(n * DC, DC)],
                        recv.at[k, :, pl.ds(n * DC, DC)],
                        ssem.at[k * nd + n], rsem.at[k * nd + n], k)
            cp.start()
            out.append(cp)
        return out

    cw[2].wait()
    sy = []
    for n in range(nd):
        yp[:, n * DC:(n + 1) * DC] = jnp.dot(h[...], wd[:, n * DC:(n + 1) * DC], preferred_element_type=F32)
        if n < NY:
            sy += reduce_rows(yp, yr, n, ys, yrs)

    for cp in sg:
        cp.wait_recv()
    outs.append(pltpu.make_async_copy(gc, gc_out, o_sem.at[2]))
    outs[2].start()
    eg = []
    for j in range(nf):
        pg[j] = lax.dot_general(gc[...], wd[j * FC:(j + 1) * FC, :], NT, preferred_element_type=F32)
        e = remote(pg.at[j], rg.at[j], es.at[3 * j + 2], ers.at[3 * j + 2], 1)
        e.start()
        eg.append(e)
    for j in range(nf):
        f = slice(j * FC, (j + 1) * FC)
        eg[j].wait_recv()

        def grad(i, carry, j=j, f=f):
            r = pl.ds(pl.multiple_of(i * rb_rows, rb_rows), rb_rows)
            g = pg[j, r, :] + rg[j, r, :]
            da[r, f] = (g * rb[j, r, :] * sd[j, r, :]).astype(BF16)
            db[r, f] = (g * ra[j, r, :]).astype(BF16)
            return carry

        lax.fori_loop(0, tok // rb_rows, grad, 0)
        for n in range(nd):
            o = slice(n * DC, (n + 1) * DC)
            part = (lax.dot_general(da[:, f], wg[o, f], NT, preferred_element_type=F32)
                    + lax.dot_general(db[:, f], wu[o, f], NT, preferred_element_type=F32))
            dxp[:, o] = part if j == 0 else dxp[:, o] + part
    outs.append(pltpu.make_async_copy(da, da_out, o_sem.at[3]))
    outs.append(pltpu.make_async_copy(db, db_out, o_sem.at[4]))
    outs[3].start()
    outs[4].start()
    for i in range(8):
        r = ((i % 2) * 4 + i // 2) * rows
        p_out[i, :, :d_half] = dxp[r:r + rows, :]
        if NY < nd:
            p_out[i, :, d_half:] = yp[r:r + rows, NY * DC:]
    for q in range(2):
        i = t * 2 + q
        r = pl.ds(pl.multiple_of((q * 4 + t) * rows, rows), rows)
        p_out[i, :, :d_half] += gc[r, :].astype(F32)
        if NY < nd:
            p_out[i, :, d_half:] += xc[r, NY * DC:].astype(F32)

    for cp in sy:
        cp.wait_recv()
    wy = NY * DC
    for kc in range(2 if NY else 0):
        cols = pl.ds(col_of(kc), wy)
        if kc == 0:
            tot = yp[pl.ds(row_of(0), rows), :wy] + yr[2, :, :wy] + yr[4, :, :wy] + yr[6, :, :wy]
        else:
            tot = yr[1, :, :wy] + yr[3, :, :wy] + yr[5, :, :wy] + yr[7, :, :wy]
        y_ref[:, cols] = (x_v[:, cols].astype(F32) + tot).astype(BF16)

    for cp in sg + sy + eg:
        cp.wait_send()
    for ea, eb in ex:
        ea.wait_send()
        eb.wait_send()
    for o in outs:
        o.wait()


def _finish(y_part, p, y_ref, dx_ref):
    d_half = y_ref.shape[1] // 2
    wy = NY * DC
    for q in range(2):
        o = q * d_half
        tot = p[q] + p[q + 2] + p[q + 4] + p[q + 6]
        dx_ref[:, o:o + d_half] = tot[:, :d_half].astype(BF16)
        if NY:
            y_ref[:, o:o + wy] = y_part[:, o:o + wy]
        if wy < d_half:
            y_ref[:, o + wy:o + d_half] = tot[:, d_half:].astype(BF16)


def _grads(h, da, db, xc_hbm, gc, dwd_hbm, dwg_hbm, dwu_hbm, buf_d, buf_g, xc, sem_d, sem_g, sem_x):
    ff = h.shape[1]
    d_half = xc.shape[1]
    nb_d, tr_d = buf_d.shape[:2]
    nb_g, tr_g = buf_g.shape[:2]
    cx = pltpu.make_async_copy(xc_hbm, xc, sem_x)
    cx.start()

    def run(lhs, rhs, out, buf, sem, n, tr, nb, start, prev_out):
        def step(i, carry):
            slot = lax.rem(i + start, nb)
            r = pl.multiple_of(i * tr, tr)

            def drain():
                pltpu.make_async_copy(buf.at[slot], prev_out.at[pl.ds(0, tr), :], sem.at[slot]).wait()

            if start >= nb:
                drain()
            else:
                pl.when(i + start >= nb)(drain)
            buf[slot] = lax.dot_general(lhs[:, pl.ds(r, tr)], rhs[...], TN, preferred_element_type=F32)
            pltpu.make_async_copy(buf.at[slot], out.at[pl.ds(r, tr), :], sem.at[slot]).start()
            return carry

        lax.fori_loop(0, n, step, 0)

    n_d = ff // tr_d
    n_g = d_half // tr_g
    run(h, gc, dwd_hbm, buf_d, sem_d, n_d, tr_d, nb_d, 0, dwd_hbm)
    cx.wait()
    run(xc, da, dwg_hbm, buf_g, sem_g, n_g, tr_g, nb_g, 0, dwg_hbm)
    run(xc, db, dwu_hbm, buf_g, sem_g, n_g, tr_g, nb_g, n_g, dwu_hbm)
    for s in range(nb_d):
        pltpu.make_async_copy(buf_d.at[s], dwd_hbm.at[pl.ds(0, tr_d), :], sem_d.at[s]).wait()
    for s in range(nb_g):
        pltpu.make_async_copy(buf_g.at[s], dwu_hbm.at[pl.ds(0, tr_g), :], sem_g.at[s]).wait()


def solution(mesh):
    def local_step(x, wg, wu, wd, gy):
        rows, d_full = x.shape
        d_half, ff = wg.shape
        tok = rows * 8
        nf = ff // FC
        nd = d_half // DC
        any_ = pl.BlockSpec(memory_space=pl.ANY)
        hbm = pl.BlockSpec(memory_space=pltpu.HBM)
        vm = pl.BlockSpec(memory_space=pltpu.VMEM)
        S = jax.ShapeDtypeStruct
        dma = pltpu.SemaphoreType.DMA
        part = pltpu.VMEM((nf, tok, FC), F32)
        y, xc, gc, h, da, db, parts = pl.pallas_call(
            _front,
            name="front",
            out_shape=(S((rows, d_full), BF16),
                       pltpu.HBM((tok, d_half), BF16), S((tok, d_half), BF16),
                       S((tok, ff), BF16), S((tok, ff), BF16), S((tok, ff), BF16))
            + (S((8, rows, 2 * d_half - NY * DC), F32),),
            in_specs=[hbm] * 5,
            out_specs=(vm, hbm, any_, any_, any_, any_, vm),
            scratch_shapes=[
                pltpu.VMEM((rows, d_full), BF16), pltpu.VMEM((rows, d_full), BF16),
                pltpu.VMEM((d_half, ff), BF16), pltpu.VMEM((d_half, ff), BF16), pltpu.VMEM((ff, d_half), BF16),
                pltpu.VMEM((tok, d_half), BF16), pltpu.VMEM((tok, d_half), BF16),
                part, part, part, part, part, part, part,
                pltpu.VMEM((tok, ff), BF16), pltpu.VMEM((tok, ff), BF16), pltpu.VMEM((tok, ff), BF16),
                pltpu.VMEM((tok, d_half), F32), pltpu.VMEM((8, rows, d_half), F32),
                pltpu.VMEM((tok, d_half), F32),
                dma((5,)), dma((5,)), dma((8,)), dma((8,)), dma((8,)), dma((8,)),
                dma((3 * nf,)), dma((3 * nf,)),
                dma((8 * nd,)), dma((8 * nd,)),
            ],
            compiler_params=pltpu.CompilerParams(collective_id=0, has_side_effects=True,
                                                 vmem_limit_bytes=50 * 1024 * 1024),
        )(*(pltpu.with_memory_space_constraint(v, pltpu.HBM) for v in (x, wg, wu, wd, gy)))
        parts = lax.all_to_all(parts, ("tp", "dp"), 0, 0, tiled=True)

        tr = 256
        dwd, dwg, dwu = pl.pallas_call(
            _grads,
            name="grads",
            out_shape=(S((ff, d_half), F32), S((d_half, ff), F32), S((d_half, ff), F32)),
            in_specs=[vm, vm, vm, hbm, vm],
            out_specs=(any_, any_, any_),
            scratch_shapes=[pltpu.VMEM((8, tr, d_half), F32), pltpu.VMEM((6, tr, ff), F32),
                            pltpu.VMEM((tok, d_half), BF16), dma((8,)), dma((6,)), dma(())],
            cost_estimate=pl.CostEstimate(flops=6 * tok * d_half * ff, bytes_accessed=12 * d_half * ff,
                                          transcendentals=0),
            compiler_params=pltpu.CompilerParams(vmem_limit_bytes=34 * 1024 * 1024),
        )(h, da, db, pltpu.with_memory_space_constraint(xc, pltpu.HBM), gc)
        y, dx = pl.pallas_call(
            _finish,
            name="finish",
            out_shape=(S((rows, d_full), BF16), S((rows, d_full), BF16)),
            in_specs=[vm] * 2,
            out_specs=(vm, vm),
            compiler_params=pltpu.CompilerParams(vmem_limit_bytes=6 * 1024 * 1024),
        )(y, parts)
        return y, dx, dwg, dwu, dwd

    row_spec = P(("dp", "tp"), None)
    up_spec = P("dp", "tp")
    down_spec = P("tp", "dp")
    return jax.shard_map(local_step, mesh=mesh,
                         in_specs=(row_spec, up_spec, up_spec, down_spec, row_spec),
                         out_specs=(row_spec, row_spec, up_spec, up_spec, down_spec),
                         check_vma=False)
```

```python
import functools

import jax
import jax.numpy as jnp
from jax import lax
from jax.experimental import pallas as pl
from jax.experimental.pallas import tpu as pltpu
from jax.sharding import PartitionSpec as P

MESH = pl.DeviceIdType.MESH
F32 = jnp.float32
BF16 = jnp.bfloat16

NT = (((1,), (1,)), ((), ()))
TN = (((0,), (0,)), ((), ()))

FC = 512
DC = 512
RB = 32


def _front(x_hbm, wg_hbm, wu_hbm, wd_hbm, gy_hbm,
           y_ref, xc_out, gc_out, h_out, da_out, db_out, p_out,
           x_v, gy_v, wg, wu, wd, xc, gc,
           pa, pb, pg, ra, rb, rg, sd, h, da, db,
           yp, s1, r1, s2, r2, sc, rc, yk, dxp,
           w_sem, o_sem, xs, xrs, gs, grs, es, ers, ys, yrs):
    rows, d_full = x_v.shape
    tok, d_half = xc.shape
    half = tok // 2
    nf = wg.shape[1] // FC
    nd = d_half // DC
    t = lax.axis_index("tp")
    c = lax.axis_index("dp")
    ty, tx = t // 2, t % 2
    tx_n = ty * 2 + 1 - tx
    ty_n = (1 - ty) * 2 + tx
    t_d = 3 - t
    t1 = (1 - c) * tx_n + c * ty_n
    t2 = (1 - c) * ty_n + c * tx_n
    order = ((t_d, c), (t_d, 1 - c), (tx_n, c), (tx_n, 1 - c), (ty_n, c), (ty_n, 1 - c), (t, 1 - c))

    def rows_of(q, chip):
        return pl.ds(pl.multiple_of((q * 4 + chip) * rows, rows), rows)

    def cols_of(q):
        return pl.ds(pl.multiple_of(q * d_half, d_half), d_half)

    cx = pltpu.make_async_copy(x_hbm, x_v, w_sem.at[0])
    cg = pltpu.make_async_copy(gy_hbm, gy_v, w_sem.at[1])
    cw = [pltpu.make_async_copy(a, b, w_sem.at[2 + i])
          for i, (a, b) in enumerate(((wg_hbm, wg), (wu_hbm, wu), (wd_hbm, wd)))]
    cx.start()
    cg.start()

    barrier = pltpu.get_barrier_semaphore()
    for chip, q in order:
        pl.semaphore_signal(barrier, inc=1, device_id={"tp": chip, "dp": q}, device_id_type=MESH)
    pl.semaphore_wait(barrier, 7)

    def remote(src, dst, ssem, rsem, chip, q):
        cp = pltpu.make_async_remote_copy(src_ref=src, dst_ref=dst, send_sem=ssem, recv_sem=rsem,
                                          device_id={"tp": chip, "dp": q}, device_id_type=MESH)
        cp.start()
        return cp

    def swap(src, dst, i):
        return remote(src, dst, es.at[i], ers.at[i], t, 1 - c)

    def spread(own, cols, ssem, rsem):
        return [remote(own.at[:, cols_of(q)], cols.at[rows_of(c, t), :], ssem.at[k], rsem.at[k], chip, q)
                for k, (chip, q) in enumerate(order)]

    cx.wait()
    sx = spread(x_v, xc, xs, xrs)
    for w in cw:
        w.start()
    xc[rows_of(c, t), :] = x_v[:, cols_of(c)]
    cg.wait()
    for cp in sx:
        cp.wait_send()
    sg = spread(gy_v, gc, gs, grs)
    gc[rows_of(c, t), :] = gy_v[:, cols_of(c)]

    mine = pl.multiple_of(c * half, half)
    theirs = pl.ds(pl.multiple_of((1 - c) * half, half), half)
    cw[0].wait()
    cw[1].wait()
    for cp in sx:
        cp.wait_recv()
    out_x = pltpu.make_async_copy(xc, xc_out, o_sem.at[0])
    out_x.start()
    cps = {}
    for j in range(nf):
        f = slice(j * FC, (j + 1) * FC)
        pa[j] = jnp.dot(xc[...], wg[:, f], preferred_element_type=F32)
        cps["a", j] = swap(pa.at[j, theirs, :], ra.at[j], 6 * j)
        pb[j] = jnp.dot(xc[...], wu[:, f], preferred_element_type=F32)
        cps["b", j] = swap(pb.at[j, theirs, :], rb.at[j], 6 * j + 1)

    def blocks():
        for i in range(0, half, RB):
            yield pl.ds(pl.multiple_of(mine + i, RB), RB), slice(i, i + RB)

    for j in range(nf):
        f = slice(j * FC, (j + 1) * FC)
        cps["a", j].wait_recv()
        cps["b", j].wait_recv()
        for r, i in blocks():
            a = pa[j, r, :] + ra[j, i, :]
            b = pb[j, r, :] + rb[j, i, :]
            s = jax.nn.sigmoid(a)
            u = a * s
            h[r, f] = (u * b).astype(BF16)
            sd[j, i, :] = s * (1.0 + a * (1.0 - s))
            ra[j, i, :] = u
            rb[j, i, :] = b
        own = h.at[pl.ds(mine, half), f]
        cps["h", j] = swap(own, own, 6 * j + 3)
    for j in range(nf):
        cps["h", j].wait_recv()

    def y_part(n):
        o = slice(n * DC, (n + 1) * DC)
        yp[:, o] = jnp.dot(h[...], wd[:, o], preferred_element_type=F32)
        for q in range(2):
            for e, chip in enumerate((t1, t_d)):
                s1[n, (q * 2 + e) * rows:(q * 2 + e + 1) * rows, :] = yp[rows_of(q, chip), o]
        cps["1", n] = remote(s1.at[n], r1.at[n], ys.at[4 * n], yrs.at[4 * n], t1, c)

    def y_step(n):
        o = slice(n * DC, (n + 1) * DC)
        cps["1", n].wait_recv()

        def got(q, e):
            return r1[n, pl.ds(pl.multiple_of((q * 2 + e) * rows, rows), rows), :]

        s2[n, 0] = yp[rows_of(c, t2), o] + got(c, 1)
        s2[n, 1] = yp[rows_of(1 - c, t2), o] + got(1 - c, 1)
        cps["2", n] = remote(s2.at[n, 0], r2.at[n, 0], ys.at[4 * n + 1], yrs.at[4 * n + 1], t2, c)
        cps["3", n] = remote(s2.at[n, 1], r2.at[n, 1], ys.at[4 * n + 2], yrs.at[4 * n + 2], t2, 1 - c)
        sc[n] = yp[rows_of(1 - c, t), o] + got(1 - c, 0)
        cps["4", n] = remote(sc.at[n], rc.at[n], ys.at[4 * n + 3], yrs.at[4 * n + 3], t, 1 - c)
        yk[n] = yp[rows_of(c, t), o] + got(c, 0)

    def y_done(n):
        for k in "234":
            cps[k, n].wait_recv()
        for q, tot in ((c, yk[n] + r2[n, 0]), (1 - c, rc[n] + r2[n, 1])):
            cols = pl.ds(pl.multiple_of(q * d_half + n * DC, DC), DC)
            y_ref[:, cols] = (x_v[:, cols].astype(F32) + tot).astype(BF16)

    def g_part(j):
        pg[j] = lax.dot_general(gc[...], wd[j * FC:(j + 1) * FC, :], NT, preferred_element_type=F32)
        cps["g", j] = swap(pg.at[j, theirs, :], rg.at[j], 6 * j + 2)

    def grad(j):
        f = slice(j * FC, (j + 1) * FC)
        cps["g", j].wait_recv()
        for r, i in blocks():
            g = pg[j, r, :] + rg[j, i, :]
            da[r, f] = (g * rb[j, i, :] * sd[j, i, :]).astype(BF16)
            db[r, f] = (g * ra[j, i, :]).astype(BF16)
        own = da.at[pl.ds(mine, half), f]
        cps["da", j] = swap(own, own, 6 * j + 4)
        own = db.at[pl.ds(mine, half), f]
        cps["db", j] = swap(own, own, 6 * j + 5)

    def dx_part(j):
        f = slice(j * FC, (j + 1) * FC)
        cps["da", j].wait_recv()
        cps["db", j].wait_recv()
        for n in range(nd):
            o = slice(n * DC, (n + 1) * DC)
            part = (lax.dot_general(da[:, f], wg[o, f], NT, preferred_element_type=F32)
                    + lax.dot_general(db[:, f], wu[o, f], NT, preferred_element_type=F32))
            dxp[:, o] = part if j == 0 else dxp[:, o] + part

    cw[2].wait()
    y_part(0)
    y_part(1)
    for cp in sg:
        cp.wait_recv()
    g_part(0)
    g_part(1)
    g_part(2)
    grad(0)
    g_part(3)
    grad(1)
    y_part(2)
    y_step(0)
    grad(2)
    dx_part(0)
    grad(3)
    dx_part(1)
    y_step(1)
    dx_part(2)
    y_step(2)
    dx_part(3)

    for i in range(8):
        r = ((i % 2) * 4 + i // 2) * rows
        p_out[i] = dxp[r:r + rows, :]
    for q in range(2):
        p_out[t * 2 + q] += gc[rows_of(q, t), :].astype(F32)
    gc_out[...] = gc[...]
    h_out[...] = h[...]
    da_out[...] = da[...]
    db_out[...] = db[...]
    for n in range(nd):
        y_done(n)

    for cp in sg:
        cp.wait_send()
    for cp in cps.values():
        cp.wait_send()
    out_x.wait()


def _finish(y_in, p, y_ref, dx_ref):
    d_half = p.shape[2]
    y_ref[...] = y_in[...]
    for q in range(2):
        dx_ref[:, q * d_half:(q + 1) * d_half] = (p[q] + p[q + 2] + p[q + 4] + p[q + 6]).astype(BF16)


def _grads(h, da, db, xc_hbm, gc, dwd_hbm, dwg_hbm, dwu_hbm, buf_d, buf_g, xc, sem_d, sem_g, sem_x):
    ff = h.shape[1]
    d_half = xc.shape[1]
    nb_d, tr_d = buf_d.shape[:2]
    nb_g, tr_g = buf_g.shape[:2]
    cx = pltpu.make_async_copy(xc_hbm, xc, sem_x)
    cx.start()

    def run(lhs, rhs, out, buf, sem, n, tr, nb, start, prev_out):
        def step(i, carry):
            slot = lax.rem(i + start, nb)
            r = pl.multiple_of(i * tr, tr)

            def drain():
                pltpu.make_async_copy(buf.at[slot], prev_out.at[pl.ds(0, tr), :], sem.at[slot]).wait()

            if start >= nb:
                drain()
            else:
                pl.when(i + start >= nb)(drain)
            buf[slot] = lax.dot_general(lhs[:, pl.ds(r, tr)], rhs[...], TN, preferred_element_type=F32)
            pltpu.make_async_copy(buf.at[slot], out.at[pl.ds(r, tr), :], sem.at[slot]).start()
            return carry

        lax.fori_loop(0, n, step, 0)

    n_d = ff // tr_d
    n_g = d_half // tr_g
    run(h, gc, dwd_hbm, buf_d, sem_d, n_d, tr_d, nb_d, 0, dwd_hbm)
    cx.wait()
    run(xc, da, dwg_hbm, buf_g, sem_g, n_g, tr_g, nb_g, 0, dwg_hbm)
    run(xc, db, dwu_hbm, buf_g, sem_g, n_g, tr_g, nb_g, n_g, dwu_hbm)
    for s in range(nb_d):
        pltpu.make_async_copy(buf_d.at[s], dwd_hbm.at[pl.ds(0, tr_d), :], sem_d.at[s]).wait()
    for s in range(nb_g):
        pltpu.make_async_copy(buf_g.at[s], dwu_hbm.at[pl.ds(0, tr_g), :], sem_g.at[s]).wait()


def solution(mesh):
    def local_step(x, wg, wu, wd, gy):
        rows, d_full = x.shape
        d_half, ff = wg.shape
        tok = rows * 8
        nf = ff // FC
        nd = d_half // DC
        any_ = pl.BlockSpec(memory_space=pl.ANY)
        hbm = pl.BlockSpec(memory_space=pltpu.HBM)
        vm = pl.BlockSpec(memory_space=pltpu.VMEM)
        S = jax.ShapeDtypeStruct
        dma = pltpu.SemaphoreType.DMA
        full = pltpu.VMEM((nf, tok, FC), F32)
        part = pltpu.VMEM((nf, tok // 2, FC), F32)
        block = pltpu.VMEM((nd, rows, DC), F32)
        y, xc, gc, h, da, db, parts = pl.pallas_call(
            _front,
            name="front",
            out_shape=(S((rows, d_full), BF16),
                       pltpu.HBM((tok, d_half), BF16), S((tok, d_half), BF16),
                       S((tok, ff), BF16), S((tok, ff), BF16), S((tok, ff), BF16))
            + (S((8, rows, d_half), F32),),
            in_specs=[hbm] * 5,
            out_specs=(vm, hbm, vm, vm, vm, vm, vm),
            scratch_shapes=[
                pltpu.VMEM((rows, d_full), BF16), pltpu.VMEM((rows, d_full), BF16),
                pltpu.VMEM((d_half, ff), BF16), pltpu.VMEM((d_half, ff), BF16), pltpu.VMEM((ff, d_half), BF16),
                pltpu.VMEM((tok, d_half), BF16), pltpu.VMEM((tok, d_half), BF16),
                full, full, full, part, part, part, part,
                pltpu.VMEM((tok, ff), BF16), pltpu.VMEM((tok, ff), BF16), pltpu.VMEM((tok, ff), BF16),
                pltpu.VMEM((tok, d_half), F32),
                pltpu.VMEM((nd, 4 * rows, DC), F32), pltpu.VMEM((nd, 4 * rows, DC), F32),
                pltpu.VMEM((nd, 2, rows, DC), F32), pltpu.VMEM((nd, 2, rows, DC), F32),
                block, block, block,
                pltpu.VMEM((tok, d_half), F32),
                dma((5,)), dma((1,)), dma((7,)), dma((7,)), dma((7,)), dma((7,)),
                dma((6 * nf,)), dma((6 * nf,)), dma((4 * nd,)), dma((4 * nd,)),
            ],
            compiler_params=pltpu.CompilerParams(collective_id=0, has_side_effects=True,
                                                 vmem_limit_bytes=50 * 1024 * 1024),
        )(*(pltpu.with_memory_space_constraint(v, pltpu.HBM) for v in (x, wg, wu, wd, gy)))
        parts = lax.all_to_all(parts, ("tp", "dp"), 0, 0, tiled=True)

        tr = 256
        dwd, dwg, dwu = pl.pallas_call(
            _grads,
            name="grads",
            out_shape=(S((ff, d_half), F32), S((d_half, ff), F32), S((d_half, ff), F32)),
            in_specs=[vm, vm, vm, hbm, vm],
            out_specs=(any_, any_, any_),
            scratch_shapes=[pltpu.VMEM((8, tr, d_half), F32), pltpu.VMEM((6, tr, ff), F32),
                            pltpu.VMEM((tok, d_half), BF16), dma((8,)), dma((6,)), dma(())],
            cost_estimate=pl.CostEstimate(flops=6 * tok * d_half * ff, bytes_accessed=12 * d_half * ff,
                                          transcendentals=0),
            compiler_params=pltpu.CompilerParams(vmem_limit_bytes=34 * 1024 * 1024),
        )(h, da, db, pltpu.with_memory_space_constraint(xc, pltpu.HBM), gc)
        y, dx = pl.pallas_call(
            _finish,
            name="finish",
            out_shape=(S((rows, d_full), BF16), S((rows, d_full), BF16)),
            in_specs=[vm] * 2,
            out_specs=(vm, vm),
            compiler_params=pltpu.CompilerParams(vmem_limit_bytes=6 * 1024 * 1024),
        )(y, parts)
        return y, dx, dwg, dwu, dwd

    row_spec = P(("dp", "tp"), None)
    up_spec = P("dp", "tp")
    down_spec = P("tp", "dp")
    return jax.shard_map(local_step, mesh=mesh,
                         in_specs=(row_spec, up_spec, up_spec, down_spec, row_spec),
                         out_specs=(row_spec, row_spec, up_spec, up_spec, down_spec),
                         check_vma=False)
```

```python
import functools

import jax
import jax.numpy as jnp
from jax import lax
from jax.experimental import pallas as pl
from jax.experimental.pallas import tpu as pltpu
from jax.sharding import PartitionSpec as P

MESH = pl.DeviceIdType.MESH
F32 = jnp.float32
BF16 = jnp.bfloat16

NT = (((1,), (1,)), ((), ()))
TN = (((0,), (0,)), ((), ()))

FC = 512
DC = 512
RB = 32


def _front(x_hbm, wg_hbm, wu_hbm, wd_hbm, gy_hbm,
           y_ref, xc_out, gc_out, h_out, da_out, db_out, p_out,
           x_v, gy_v, wg, wu, wd, xc, gc,
           pa, pb, pg, ra, rb, rg, sd, h, da, db,
           yp, s1, r1, s2, r2, sc, rc, yk, dxp,
           w_sem, o_sem, xs, xrs, gs, grs, es, ers, ys, yrs):
    rows, d_full = x_v.shape
    tok, d_half = xc.shape
    half = tok // 2
    nf = wg.shape[1] // FC
    nd = d_half // DC
    t = lax.axis_index("tp")
    c = lax.axis_index("dp")
    ty, tx = t // 2, t % 2
    tx_n = ty * 2 + 1 - tx
    ty_n = (1 - ty) * 2 + tx
    t_d = 3 - t
    t1 = (1 - c) * tx_n + c * ty_n
    t2 = (1 - c) * ty_n + c * tx_n
    order = ((t_d, c), (t_d, 1 - c), (tx_n, c), (tx_n, 1 - c), (ty_n, c), (ty_n, 1 - c), (t, 1 - c))

    def rows_of(q, chip):
        return pl.ds(pl.multiple_of((q * 4 + chip) * rows, rows), rows)

    def cols_of(q):
        return pl.ds(pl.multiple_of(q * d_half, d_half), d_half)

    cx = pltpu.make_async_copy(x_hbm, x_v, w_sem.at[0])
    cg = pltpu.make_async_copy(gy_hbm, gy_v, w_sem.at[1])
    cw = [pltpu.make_async_copy(a, b, w_sem.at[2 + i])
          for i, (a, b) in enumerate(((wg_hbm, wg), (wu_hbm, wu), (wd_hbm, wd)))]
    cx.start()
    cg.start()
    for w in cw:
        w.start()

    barrier = pltpu.get_barrier_semaphore()
    for chip, q in order:
        pl.semaphore_signal(barrier, inc=1, device_id={"tp": chip, "dp": q}, device_id_type=MESH)
    pl.semaphore_wait(barrier, 7)

    def remote(src, dst, ssem, rsem, chip, q):
        cp = pltpu.make_async_remote_copy(src_ref=src, dst_ref=dst, send_sem=ssem, recv_sem=rsem,
                                          device_id={"tp": chip, "dp": q}, device_id_type=MESH)
        cp.start()
        return cp

    def swap(src, dst, i):
        return remote(src, dst, es.at[i], ers.at[i], t, 1 - c)

    def spread(own, cols, ssem, rsem):
        return [remote(own.at[:, cols_of(q)], cols.at[rows_of(c, t), :], ssem.at[k], rsem.at[k], chip, q)
                for k, (chip, q) in enumerate(order)]

    cx.wait()
    sx = spread(x_v, xc, xs, xrs)
    xc[rows_of(c, t), :] = x_v[:, cols_of(c)]
    cg.wait()
    for cp in sx:
        cp.wait_send()
    sg = spread(gy_v, gc, gs, grs)
    gc[rows_of(c, t), :] = gy_v[:, cols_of(c)]

    mine = pl.multiple_of(c * half, half)
    theirs = pl.ds(pl.multiple_of((1 - c) * half, half), half)
    cw[0].wait()
    cw[1].wait()
    for cp in sx:
        cp.wait_recv()
    out_x = pltpu.make_async_copy(xc, xc_out, o_sem.at[0])
    out_x.start()
    cps = {}
    for j in range(nf):
        f = slice(j * FC, (j + 1) * FC)
        pa[j] = jnp.dot(xc[...], wg[:, f], preferred_element_type=F32)
        cps["a", j] = swap(pa.at[j, theirs, :], ra.at[j], 6 * j)
        pb[j] = jnp.dot(xc[...], wu[:, f], preferred_element_type=F32)
        cps["b", j] = swap(pb.at[j, theirs, :], rb.at[j], 6 * j + 1)

    def blocks():
        for i in range(0, half, RB):
            yield pl.ds(pl.multiple_of(mine + i, RB), RB), slice(i, i + RB)

    for j in range(nf):
        f = slice(j * FC, (j + 1) * FC)
        cps["a", j].wait_recv()
        cps["b", j].wait_recv()
        for r, i in blocks():
            a = pa[j, r, :] + ra[j, i, :]
            b = pb[j, r, :] + rb[j, i, :]
            s = jax.nn.sigmoid(a)
            u = a * s
            h[r, f] = (u * b).astype(BF16)
            sd[j, i, :] = s * (1.0 + a * (1.0 - s))
            ra[j, i, :] = u
            rb[j, i, :] = b
        own = h.at[pl.ds(mine, half), f]
        cps["h", j] = swap(own, own, 6 * j + 3)
    def y_part(n):
        o = slice(n * DC, (n + 1) * DC)
        yp[:, o] = jnp.dot(h[...], wd[:, o], preferred_element_type=F32)
        for q in range(2):
            for e, chip in enumerate((t1, t_d)):
                s1[n, (q * 2 + e) * rows:(q * 2 + e + 1) * rows, :] = yp[rows_of(q, chip), o]
        cps["1", n] = remote(s1.at[n], r1.at[n], ys.at[4 * n], yrs.at[4 * n], t1, c)

    def y_step(n):
        o = slice(n * DC, (n + 1) * DC)
        cps["1", n].wait_recv()

        def got(q, e):
            return r1[n, pl.ds(pl.multiple_of((q * 2 + e) * rows, rows), rows), :]

        s2[n, 0] = yp[rows_of(c, t2), o] + got(c, 1)
        s2[n, 1] = yp[rows_of(1 - c, t2), o] + got(1 - c, 1)
        cps["2", n] = remote(s2.at[n, 0], r2.at[n, 0], ys.at[4 * n + 1], yrs.at[4 * n + 1], t2, c)
        cps["3", n] = remote(s2.at[n, 1], r2.at[n, 1], ys.at[4 * n + 2], yrs.at[4 * n + 2], t2, 1 - c)
        sc[n] = yp[rows_of(1 - c, t), o] + got(1 - c, 0)
        cps["4", n] = remote(sc.at[n], rc.at[n], ys.at[4 * n + 3], yrs.at[4 * n + 3], t, 1 - c)
        yk[n] = yp[rows_of(c, t), o] + got(c, 0)

    def y_done(n):
        for k in "234":
            cps[k, n].wait_recv()
        for q, tot in ((c, yk[n] + r2[n, 0]), (1 - c, rc[n] + r2[n, 1])):
            cols = pl.ds(pl.multiple_of(q * d_half + n * DC, DC), DC)
            y_ref[:, cols] = (x_v[:, cols].astype(F32) + tot).astype(BF16)

    def g_part(j):
        pg[j] = lax.dot_general(gc[...], wd[j * FC:(j + 1) * FC, :], NT, preferred_element_type=F32)
        cps["g", j] = swap(pg.at[j, theirs, :], rg.at[j], 6 * j + 2)

    def grad(j):
        f = slice(j * FC, (j + 1) * FC)
        cps["g", j].wait_recv()
        for r, i in blocks():
            g = pg[j, r, :] + rg[j, i, :]
            da[r, f] = (g * rb[j, i, :] * sd[j, i, :]).astype(BF16)
            db[r, f] = (g * ra[j, i, :]).astype(BF16)
        own = da.at[pl.ds(mine, half), f]
        cps["da", j] = swap(own, own, 6 * j + 4)
        own = db.at[pl.ds(mine, half), f]
        cps["db", j] = swap(own, own, 6 * j + 5)

    def dx_part(j):
        f = slice(j * FC, (j + 1) * FC)
        cps["da", j].wait_recv()
        cps["db", j].wait_recv()
        for n in range(nd):
            o = slice(n * DC, (n + 1) * DC)
            part = (lax.dot_general(da[:, f], wg[o, f], NT, preferred_element_type=F32)
                    + lax.dot_general(db[:, f], wu[o, f], NT, preferred_element_type=F32))
            dxp[:, o] = part if j == 0 else dxp[:, o] + part

    cw[2].wait()
    for cp in sg:
        cp.wait_recv()
    g_part(0)
    g_part(1)
    for j in range(nf):
        cps["h", j].wait_recv()
    y_part(0)
    y_part(1)
    y_part(2)
    g_part(2)
    grad(0)
    g_part(3)
    grad(1)
    grad(2)
    dx_part(0)
    grad(3)
    y_step(0)
    dx_part(1)
    y_step(1)
    dx_part(2)
    y_step(2)
    dx_part(3)

    for i in range(8):
        r = ((i % 2) * 4 + i // 2) * rows
        p_out[i] = dxp[r:r + rows, :]
    for q in range(2):
        p_out[t * 2 + q] += gc[rows_of(q, t), :].astype(F32)
    gc_out[...] = gc[...]
    h_out[...] = h[...]
    da_out[...] = da[...]
    db_out[...] = db[...]
    for n in range(nd):
        y_done(n)

    for cp in sg:
        cp.wait_send()
    for cp in cps.values():
        cp.wait_send()
    out_x.wait()


def _finish(y_in, p, y_ref, dx_ref):
    d_half = p.shape[2]
    y_ref[...] = y_in[...]
    for q in range(2):
        dx_ref[:, q * d_half:(q + 1) * d_half] = (p[q] + p[q + 2] + p[q + 4] + p[q + 6]).astype(BF16)


def _grads(h, da, db, xc_hbm, gc, dwd_hbm, dwg_hbm, dwu_hbm, buf_d, buf_g, xc, sem_d, sem_g, sem_x):
    ff = h.shape[1]
    d_half = xc.shape[1]
    nb_d, tr_d = buf_d.shape[:2]
    nb_g, tr_g = buf_g.shape[:2]
    cx = pltpu.make_async_copy(xc_hbm, xc, sem_x)
    cx.start()

    def run(lhs, rhs, out, buf, sem, n, tr, nb, start, prev_out):
        def step(i, carry):
            slot = lax.rem(i + start, nb)
            r = pl.multiple_of(i * tr, tr)

            def drain():
                pltpu.make_async_copy(buf.at[slot], prev_out.at[pl.ds(0, tr), :], sem.at[slot]).wait()

            if start >= nb:
                drain()
            else:
                pl.when(i + start >= nb)(drain)
            buf[slot] = lax.dot_general(lhs[:, pl.ds(r, tr)], rhs[...], TN, preferred_element_type=F32)
            pltpu.make_async_copy(buf.at[slot], out.at[pl.ds(r, tr), :], sem.at[slot]).start()
            return carry

        lax.fori_loop(0, n, step, 0)

    n_d = ff // tr_d
    n_g = d_half // tr_g
    run(h, gc, dwd_hbm, buf_d, sem_d, n_d, tr_d, nb_d, 0, dwd_hbm)
    cx.wait()
    run(xc, da, dwg_hbm, buf_g, sem_g, n_g, tr_g, nb_g, 0, dwg_hbm)
    run(xc, db, dwu_hbm, buf_g, sem_g, n_g, tr_g, nb_g, n_g, dwu_hbm)
    for s in range(nb_d):
        pltpu.make_async_copy(buf_d.at[s], dwd_hbm.at[pl.ds(0, tr_d), :], sem_d.at[s]).wait()
    for s in range(nb_g):
        pltpu.make_async_copy(buf_g.at[s], dwu_hbm.at[pl.ds(0, tr_g), :], sem_g.at[s]).wait()


def solution(mesh):
    def local_step(x, wg, wu, wd, gy):
        rows, d_full = x.shape
        d_half, ff = wg.shape
        tok = rows * 8
        nf = ff // FC
        nd = d_half // DC
        any_ = pl.BlockSpec(memory_space=pl.ANY)
        hbm = pl.BlockSpec(memory_space=pltpu.HBM)
        vm = pl.BlockSpec(memory_space=pltpu.VMEM)
        S = jax.ShapeDtypeStruct
        dma = pltpu.SemaphoreType.DMA
        full = pltpu.VMEM((nf, tok, FC), F32)
        part = pltpu.VMEM((nf, tok // 2, FC), F32)
        block = pltpu.VMEM((nd, rows, DC), F32)
        y, xc, gc, h, da, db, parts = pl.pallas_call(
            _front,
            name="front",
            out_shape=(S((rows, d_full), BF16),
                       pltpu.HBM((tok, d_half), BF16), S((tok, d_half), BF16),
                       S((tok, ff), BF16), S((tok, ff), BF16), S((tok, ff), BF16))
            + (S((8, rows, d_half), F32),),
            in_specs=[hbm] * 5,
            out_specs=(vm, hbm, vm, vm, vm, vm, vm),
            scratch_shapes=[
                pltpu.VMEM((rows, d_full), BF16), pltpu.VMEM((rows, d_full), BF16),
                pltpu.VMEM((d_half, ff), BF16), pltpu.VMEM((d_half, ff), BF16), pltpu.VMEM((ff, d_half), BF16),
                pltpu.VMEM((tok, d_half), BF16), pltpu.VMEM((tok, d_half), BF16),
                full, full, full, part, part, part, part,
                pltpu.VMEM((tok, ff), BF16), pltpu.VMEM((tok, ff), BF16), pltpu.VMEM((tok, ff), BF16),
                pltpu.VMEM((tok, d_half), F32),
                pltpu.VMEM((nd, 4 * rows, DC), F32), pltpu.VMEM((nd, 4 * rows, DC), F32),
                pltpu.VMEM((nd, 2, rows, DC), F32), pltpu.VMEM((nd, 2, rows, DC), F32),
                block, block, block,
                pltpu.VMEM((tok, d_half), F32),
                dma((5,)), dma((1,)), dma((7,)), dma((7,)), dma((7,)), dma((7,)),
                dma((6 * nf,)), dma((6 * nf,)), dma((4 * nd,)), dma((4 * nd,)),
            ],
            compiler_params=pltpu.CompilerParams(collective_id=0, has_side_effects=True,
                                                 vmem_limit_bytes=50 * 1024 * 1024),
        )(*(pltpu.with_memory_space_constraint(v, pltpu.HBM) for v in (x, wg, wu, wd, gy)))
        parts = lax.all_to_all(parts, ("tp", "dp"), 0, 0, tiled=True)

        tr = 256
        dwd, dwg, dwu = pl.pallas_call(
            _grads,
            name="grads",
            out_shape=(S((ff, d_half), F32), S((d_half, ff), F32), S((d_half, ff), F32)),
            in_specs=[vm, vm, vm, hbm, vm],
            out_specs=(any_, any_, any_),
            scratch_shapes=[pltpu.VMEM((8, tr, d_half), F32), pltpu.VMEM((6, tr, ff), F32),
                            pltpu.VMEM((tok, d_half), BF16), dma((8,)), dma((6,)), dma(())],
            cost_estimate=pl.CostEstimate(flops=6 * tok * d_half * ff, bytes_accessed=12 * d_half * ff,
                                          transcendentals=0),
            compiler_params=pltpu.CompilerParams(vmem_limit_bytes=34 * 1024 * 1024),
        )(h, da, db, pltpu.with_memory_space_constraint(xc, pltpu.HBM), gc)
        y, dx = pl.pallas_call(
            _finish,
            name="finish",
            out_shape=(S((rows, d_full), BF16), S((rows, d_full), BF16)),
            in_specs=[vm] * 2,
            out_specs=(vm, vm),
            compiler_params=pltpu.CompilerParams(vmem_limit_bytes=6 * 1024 * 1024),
        )(y, parts)
        return y, dx, dwg, dwu, dwd

    row_spec = P(("dp", "tp"), None)
    up_spec = P("dp", "tp")
    down_spec = P("tp", "dp")
    return jax.shard_map(local_step, mesh=mesh,
                         in_specs=(row_spec, up_spec, up_spec, down_spec, row_spec),
                         out_specs=(row_spec, row_spec, up_spec, up_spec, down_spec),
                         check_vma=False)
```

```python
import functools

import jax
import jax.numpy as jnp
from jax import lax
from jax.experimental import pallas as pl
from jax.experimental.pallas import tpu as pltpu
from jax.sharding import PartitionSpec as P

MESH = pl.DeviceIdType.MESH
F32 = jnp.float32
BF16 = jnp.bfloat16

NT = (((1,), (1,)), ((), ()))
TN = (((0,), (0,)), ((), ()))

FC = 512
DC = 512
SPLIT = 2
RB = 32


def _front(x_hbm, wg_hbm, wu_hbm, wd_hbm, gy_hbm,
           y_ref, xc_out, gc_out, h_out, da_out, db_out, p_out,
           x_v, gy_v, wg, wu, wd, xc, gc,
           pa, pb, pg, ra, rb, rg, sd, h, da, db,
           yp, s1, r1, s2, r2, sc, rc, yk, dxp,
           w_sem, o_sem, xs, xrs, gs, grs, es, ers, ys, yrs):
    rows, d_full = x_v.shape
    tok, d_half = xc.shape
    half = tok // 2
    nf = wg.shape[1] // FC
    nd = d_half // DC
    t = lax.axis_index("tp")
    c = lax.axis_index("dp")
    ty, tx = t // 2, t % 2
    tx_n = ty * 2 + 1 - tx
    ty_n = (1 - ty) * 2 + tx
    t_d = 3 - t
    t1 = (1 - c) * tx_n + c * ty_n
    t2 = (1 - c) * ty_n + c * tx_n
    order = ((t_d, c), (t_d, 1 - c), (tx_n, c), (tx_n, 1 - c), (ty_n, c), (ty_n, 1 - c), (t, 1 - c))

    def rows_of(q, chip):
        return pl.ds(pl.multiple_of((q * 4 + chip) * rows, rows), rows)

    def cols_of(q):
        return pl.ds(pl.multiple_of(q * d_half, d_half), d_half)

    cx = pltpu.make_async_copy(x_hbm, x_v, w_sem.at[0])
    cg = pltpu.make_async_copy(gy_hbm, gy_v, w_sem.at[1])
    cw = [pltpu.make_async_copy(a, b, w_sem.at[2 + i])
          for i, (a, b) in enumerate(((wg_hbm, wg), (wu_hbm, wu), (wd_hbm, wd)))]
    cx.start()
    cg.start()
    for w in cw:
        w.start()

    barrier = pltpu.get_barrier_semaphore()
    for chip, q in order:
        pl.semaphore_signal(barrier, inc=1, device_id={"tp": chip, "dp": q}, device_id_type=MESH)
    pl.semaphore_wait(barrier, 7)

    def remote(src, dst, ssem, rsem, chip, q):
        cp = pltpu.make_async_remote_copy(src_ref=src, dst_ref=dst, send_sem=ssem, recv_sem=rsem,
                                          device_id={"tp": chip, "dp": q}, device_id_type=MESH)
        cp.start()
        return cp

    def swap(src, dst, i):
        return remote(src, dst, es.at[i], ers.at[i], t, 1 - c)

    def spread(own, cols, ssem, rsem):
        return [remote(own.at[:, cols_of(q)], cols.at[rows_of(c, t), :], ssem.at[k], rsem.at[k], chip, q)
                for k, (chip, q) in enumerate(order)]

    cx.wait()
    sx = spread(x_v, xc, xs, xrs)
    xc[rows_of(c, t), :] = x_v[:, cols_of(c)]
    cg.wait()
    for cp in sx:
        cp.wait_send()
    sg = spread(gy_v, gc, gs, grs)
    gc[rows_of(c, t), :] = gy_v[:, cols_of(c)]

    mine = pl.multiple_of(c * half, half)
    theirs = pl.ds(pl.multiple_of((1 - c) * half, half), half)
    cw[0].wait()
    cw[1].wait()
    for cp in sx:
        cp.wait_recv()
    out_x = pltpu.make_async_copy(xc, xc_out, o_sem.at[0])
    out_x.start()
    cps = {}

    def swap_part(part, got, j, i):
        if j < SPLIT:
            return swap(part.at[j, theirs, :], got.at[j, pl.ds(0, half), :], i)
        return swap(part.at[j], got.at[j], i)

    for j in range(nf):
        f = slice(j * FC, (j + 1) * FC)
        pa[j] = jnp.dot(xc[...], wg[:, f], preferred_element_type=F32)
        cps["a", j] = swap_part(pa, ra, j, 6 * j)
        pb[j] = jnp.dot(xc[...], wu[:, f], preferred_element_type=F32)
        cps["b", j] = swap_part(pb, rb, j, 6 * j + 1)

    def blocks(j):
        for i in range(0, half if j < SPLIT else tok, RB):
            yield pl.ds(pl.multiple_of(mine + i, RB), RB) if j < SPLIT else slice(i, i + RB), slice(i, i + RB)

    for j in range(nf):
        f = slice(j * FC, (j + 1) * FC)
        cps["a", j].wait_recv()
        cps["b", j].wait_recv()
        for r, i in blocks(j):
            a = pa[j, r, :] + ra[j, i, :]
            b = pb[j, r, :] + rb[j, i, :]
            s = jax.nn.sigmoid(a)
            u = a * s
            h[r, f] = (u * b).astype(BF16)
            sd[j, i, :] = s * (1.0 + a * (1.0 - s))
            ra[j, i, :] = u
            rb[j, i, :] = b
        if j < SPLIT:
            own = h.at[pl.ds(mine, half), f]
            cps["h", j] = swap(own, own, 6 * j + 3)
    def y_part(n):
        o = slice(n * DC, (n + 1) * DC)
        yp[:, o] = jnp.dot(h[...], wd[:, o], preferred_element_type=F32)
        for q in range(2):
            for e, chip in enumerate((t1, t_d)):
                s1[n, (q * 2 + e) * rows:(q * 2 + e + 1) * rows, :] = yp[rows_of(q, chip), o]
        cps["1", n] = remote(s1.at[n], r1.at[n], ys.at[4 * n], yrs.at[4 * n], t1, c)

    def y_step(n):
        o = slice(n * DC, (n + 1) * DC)
        cps["1", n].wait_recv()

        def got(q, e):
            return r1[n, pl.ds(pl.multiple_of((q * 2 + e) * rows, rows), rows), :]

        s2[n, 0] = yp[rows_of(c, t2), o] + got(c, 1)
        s2[n, 1] = yp[rows_of(1 - c, t2), o] + got(1 - c, 1)
        cps["2", n] = remote(s2.at[n, 0], r2.at[n, 0], ys.at[4 * n + 1], yrs.at[4 * n + 1], t2, c)
        cps["3", n] = remote(s2.at[n, 1], r2.at[n, 1], ys.at[4 * n + 2], yrs.at[4 * n + 2], t2, 1 - c)
        sc[n] = yp[rows_of(1 - c, t), o] + got(1 - c, 0)
        cps["4", n] = remote(sc.at[n], rc.at[n], ys.at[4 * n + 3], yrs.at[4 * n + 3], t, 1 - c)
        yk[n] = yp[rows_of(c, t), o] + got(c, 0)

    def y_done(n):
        for k in "234":
            cps[k, n].wait_recv()
        for q, tot in ((c, yk[n] + r2[n, 0]), (1 - c, rc[n] + r2[n, 1])):
            cols = pl.ds(pl.multiple_of(q * d_half + n * DC, DC), DC)
            y_ref[:, cols] = (x_v[:, cols].astype(F32) + tot).astype(BF16)

    def g_part(j):
        pg[j] = lax.dot_general(gc[...], wd[j * FC:(j + 1) * FC, :], NT, preferred_element_type=F32)
        cps["g", j] = swap_part(pg, rg, j, 6 * j + 2)

    def grad(j):
        f = slice(j * FC, (j + 1) * FC)
        cps["g", j].wait_recv()
        for r, i in blocks(j):
            g = pg[j, r, :] + rg[j, i, :]
            da[r, f] = (g * rb[j, i, :] * sd[j, i, :]).astype(BF16)
            db[r, f] = (g * ra[j, i, :]).astype(BF16)
        if j < SPLIT:
            own = da.at[pl.ds(mine, half), f]
            cps["da", j] = swap(own, own, 6 * j + 4)
            own = db.at[pl.ds(mine, half), f]
            cps["db", j] = swap(own, own, 6 * j + 5)

    def dx_part(j):
        f = slice(j * FC, (j + 1) * FC)
        if j < SPLIT:
            cps["da", j].wait_recv()
            cps["db", j].wait_recv()
        for n in range(nd):
            o = slice(n * DC, (n + 1) * DC)
            part = (lax.dot_general(da[:, f], wg[o, f], NT, preferred_element_type=F32)
                    + lax.dot_general(db[:, f], wu[o, f], NT, preferred_element_type=F32))
            dxp[:, o] = part if j == 0 else dxp[:, o] + part

    cw[2].wait()
    for j in range(SPLIT):
        cps["h", j].wait_recv()
    y_part(0)
    y_part(1)
    y_part(2)
    for cp in sg:
        cp.wait_recv()
    g_part(0)
    g_part(1)
    g_part(2)
    grad(0)
    g_part(3)
    grad(1)
    dx_part(0)
    y_step(0)
    grad(2)
    dx_part(1)
    grad(3)
    y_step(1)
    dx_part(2)
    y_step(2)
    dx_part(3)

    for i in range(8):
        r = ((i % 2) * 4 + i // 2) * rows
        p_out[i] = dxp[r:r + rows, :]
    for q in range(2):
        p_out[t * 2 + q] += gc[rows_of(q, t), :].astype(F32)
    gc_out[...] = gc[...]
    h_out[...] = h[...]
    da_out[...] = da[...]
    db_out[...] = db[...]
    for n in range(nd):
        y_done(n)

    for cp in sg:
        cp.wait_send()
    for cp in cps.values():
        cp.wait_send()
    out_x.wait()


def _finish(y_in, p, y_ref, dx_ref):
    d_half = p.shape[2]
    y_ref[...] = y_in[...]
    for q in range(2):
        dx_ref[:, q * d_half:(q + 1) * d_half] = (p[q] + p[q + 2] + p[q + 4] + p[q + 6]).astype(BF16)


def _grads(h, da, db, xc_hbm, gc, dwd_hbm, dwg_hbm, dwu_hbm, buf_d, buf_g, xc, sem_d, sem_g, sem_x):
    ff = h.shape[1]
    d_half = xc.shape[1]
    nb_d, tr_d = buf_d.shape[:2]
    nb_g, tr_g = buf_g.shape[:2]
    cx = pltpu.make_async_copy(xc_hbm, xc, sem_x)
    cx.start()

    def run(lhs, rhs, out, buf, sem, n, tr, nb, start, prev_out):
        def step(i, carry):
            slot = lax.rem(i + start, nb)
            r = pl.multiple_of(i * tr, tr)

            def drain():
                pltpu.make_async_copy(buf.at[slot], prev_out.at[pl.ds(0, tr), :], sem.at[slot]).wait()

            if start >= nb:
                drain()
            else:
                pl.when(i + start >= nb)(drain)
            buf[slot] = lax.dot_general(lhs[:, pl.ds(r, tr)], rhs[...], TN, preferred_element_type=F32)
            pltpu.make_async_copy(buf.at[slot], out.at[pl.ds(r, tr), :], sem.at[slot]).start()
            return carry

        lax.fori_loop(0, n, step, 0)

    n_d = ff // tr_d
    n_g = d_half // tr_g
    run(h, gc, dwd_hbm, buf_d, sem_d, n_d, tr_d, nb_d, 0, dwd_hbm)
    cx.wait()
    run(xc, da, dwg_hbm, buf_g, sem_g, n_g, tr_g, nb_g, 0, dwg_hbm)
    run(xc, db, dwu_hbm, buf_g, sem_g, n_g, tr_g, nb_g, n_g, dwu_hbm)
    for s in range(nb_d):
        pltpu.make_async_copy(buf_d.at[s], dwd_hbm.at[pl.ds(0, tr_d), :], sem_d.at[s]).wait()
    for s in range(nb_g):
        pltpu.make_async_copy(buf_g.at[s], dwu_hbm.at[pl.ds(0, tr_g), :], sem_g.at[s]).wait()


def solution(mesh):
    def local_step(x, wg, wu, wd, gy):
        rows, d_full = x.shape
        d_half, ff = wg.shape
        tok = rows * 8
        nf = ff // FC
        nd = d_half // DC
        any_ = pl.BlockSpec(memory_space=pl.ANY)
        hbm = pl.BlockSpec(memory_space=pltpu.HBM)
        vm = pl.BlockSpec(memory_space=pltpu.VMEM)
        S = jax.ShapeDtypeStruct
        dma = pltpu.SemaphoreType.DMA
        full = pltpu.VMEM((nf, tok, FC), F32)
        block = pltpu.VMEM((nd, rows, DC), F32)
        y, xc, gc, h, da, db, parts = pl.pallas_call(
            _front,
            name="front",
            out_shape=(S((rows, d_full), BF16),
                       pltpu.HBM((tok, d_half), BF16), S((tok, d_half), BF16),
                       S((tok, ff), BF16), S((tok, ff), BF16), S((tok, ff), BF16))
            + (S((8, rows, d_half), F32),),
            in_specs=[hbm] * 5,
            out_specs=(vm, hbm, vm, vm, vm, vm, vm),
            scratch_shapes=[
                pltpu.VMEM((rows, d_full), BF16), pltpu.VMEM((rows, d_full), BF16),
                pltpu.VMEM((d_half, ff), BF16), pltpu.VMEM((d_half, ff), BF16), pltpu.VMEM((ff, d_half), BF16),
                pltpu.VMEM((tok, d_half), BF16), pltpu.VMEM((tok, d_half), BF16),
                full, full, full, full, full, full, full,
                pltpu.VMEM((tok, ff), BF16), pltpu.VMEM((tok, ff), BF16), pltpu.VMEM((tok, ff), BF16),
                pltpu.VMEM((tok, d_half), F32),
                pltpu.VMEM((nd, 4 * rows, DC), F32), pltpu.VMEM((nd, 4 * rows, DC), F32),
                pltpu.VMEM((nd, 2, rows, DC), F32), pltpu.VMEM((nd, 2, rows, DC), F32),
                block, block, block,
                pltpu.VMEM((tok, d_half), F32),
                dma((5,)), dma((1,)), dma((7,)), dma((7,)), dma((7,)), dma((7,)),
                dma((6 * nf,)), dma((6 * nf,)), dma((4 * nd,)), dma((4 * nd,)),
            ],
            compiler_params=pltpu.CompilerParams(collective_id=0, has_side_effects=True,
                                                 vmem_limit_bytes=50 * 1024 * 1024),
        )(*(pltpu.with_memory_space_constraint(v, pltpu.HBM) for v in (x, wg, wu, wd, gy)))
        parts = lax.all_to_all(parts, ("tp", "dp"), 0, 0, tiled=True)

        tr = 256
        dwd, dwg, dwu = pl.pallas_call(
            _grads,
            name="grads",
            out_shape=(S((ff, d_half), F32), S((d_half, ff), F32), S((d_half, ff), F32)),
            in_specs=[vm, vm, vm, hbm, vm],
            out_specs=(any_, any_, any_),
            scratch_shapes=[pltpu.VMEM((8, tr, d_half), F32), pltpu.VMEM((6, tr, ff), F32),
                            pltpu.VMEM((tok, d_half), BF16), dma((8,)), dma((6,)), dma(())],
            cost_estimate=pl.CostEstimate(flops=6 * tok * d_half * ff, bytes_accessed=12 * d_half * ff,
                                          transcendentals=0),
            compiler_params=pltpu.CompilerParams(vmem_limit_bytes=34 * 1024 * 1024),
        )(h, da, db, pltpu.with_memory_space_constraint(xc, pltpu.HBM), gc)
        y, dx = pl.pallas_call(
            _finish,
            name="finish",
            out_shape=(S((rows, d_full), BF16), S((rows, d_full), BF16)),
            in_specs=[vm] * 2,
            out_specs=(vm, vm),
            compiler_params=pltpu.CompilerParams(vmem_limit_bytes=6 * 1024 * 1024),
        )(y, parts)
        return y, dx, dwg, dwu, dwd

    row_spec = P(("dp", "tp"), None)
    up_spec = P("dp", "tp")
    down_spec = P("tp", "dp")
    return jax.shard_map(local_step, mesh=mesh,
                         in_specs=(row_spec, up_spec, up_spec, down_spec, row_spec),
                         out_specs=(row_spec, row_spec, up_spec, up_spec, down_spec),
                         check_vma=False)
```

```python
import functools

import jax
import jax.numpy as jnp
from jax import lax
from jax.experimental import pallas as pl
from jax.experimental.pallas import tpu as pltpu
from jax.sharding import PartitionSpec as P

MESH = pl.DeviceIdType.MESH
F32 = jnp.float32
BF16 = jnp.bfloat16

NT = (((1,), (1,)), ((), ()))
TN = (((0,), (0,)), ((), ()))

FC = 512
DC = 512
SPLIT = 2
RB = 32


def _front(x_hbm, wg_hbm, wu_hbm, wd_hbm, gy_hbm,
           y_ref, xc_out, gc_out, h_out, da_out, db_out, p_out,
           x_v, gy_v, wg, wu, wd, xc, gc,
           pa, pb, pg, ra, rb, rg, sd, h, da, db,
           yp, s1, r1, s2, r2, sc, rc, yk, dxp,
           w_sem, o_sem, xs, xrs, gs, grs, es, ers, ys, yrs):
    rows, d_full = x_v.shape
    tok, d_half = xc.shape
    half = tok // 2
    nf = wg.shape[1] // FC
    nd = d_half // DC
    t = lax.axis_index("tp")
    c = lax.axis_index("dp")
    ty, tx = t // 2, t % 2
    tx_n = ty * 2 + 1 - tx
    ty_n = (1 - ty) * 2 + tx
    t_d = 3 - t
    t1 = (1 - c) * tx_n + c * ty_n
    t2 = (1 - c) * ty_n + c * tx_n
    order = ((t_d, c), (t_d, 1 - c), (tx_n, c), (tx_n, 1 - c), (ty_n, c), (ty_n, 1 - c), (t, 1 - c))

    def rows_of(q, chip):
        return pl.ds(pl.multiple_of((q * 4 + chip) * rows, rows), rows)

    def cols_of(q):
        return pl.ds(pl.multiple_of(q * d_half, d_half), d_half)

    cx = pltpu.make_async_copy(x_hbm, x_v, w_sem.at[0])
    cg = pltpu.make_async_copy(gy_hbm, gy_v, w_sem.at[1])
    cw = [pltpu.make_async_copy(a, b, w_sem.at[2 + i])
          for i, (a, b) in enumerate(((wg_hbm, wg), (wu_hbm, wu), (wd_hbm, wd)))]
    cx.start()
    cg.start()
    for w in cw:
        w.start()

    barrier = pltpu.get_barrier_semaphore()
    for chip, q in order:
        pl.semaphore_signal(barrier, inc=1, device_id={"tp": chip, "dp": q}, device_id_type=MESH)
    pl.semaphore_wait(barrier, 7)

    def remote(src, dst, ssem, rsem, chip, q):
        cp = pltpu.make_async_remote_copy(src_ref=src, dst_ref=dst, send_sem=ssem, recv_sem=rsem,
                                          device_id={"tp": chip, "dp": q}, device_id_type=MESH)
        cp.start()
        return cp

    def swap(src, dst, i):
        return remote(src, dst, es.at[i], ers.at[i], t, 1 - c)

    def spread(own, cols, ssem, rsem):
        return [remote(own.at[:, cols_of(q)], cols.at[rows_of(c, t), :], ssem.at[k], rsem.at[k], chip, q)
                for k, (chip, q) in enumerate(order)]

    cx.wait()
    sx = spread(x_v, xc, xs, xrs)
    xc[rows_of(c, t), :] = x_v[:, cols_of(c)]
    cg.wait()
    for cp in sx:
        cp.wait_send()
    sg = spread(gy_v, gc, gs, grs)
    gc[rows_of(c, t), :] = gy_v[:, cols_of(c)]

    mine = pl.multiple_of(c * half, half)
    theirs = pl.ds(pl.multiple_of((1 - c) * half, half), half)
    cw[0].wait()
    cw[1].wait()
    for cp in sx:
        cp.wait_recv()
    out_x = pltpu.make_async_copy(xc, xc_out, o_sem.at[0])
    out_x.start()
    cps = {}

    def swap_part(part, got, j, i):
        if j < SPLIT:
            return swap(part.at[j, theirs, :], got.at[j, pl.ds(0, half), :], i)
        return swap(part.at[j], got.at[j], i)

    for j in range(nf):
        f = slice(j * FC, (j + 1) * FC)
        pa[j] = jnp.dot(xc[...], wg[:, f], preferred_element_type=F32)
        cps["a", j] = swap_part(pa, ra, j, 6 * j)
        pb[j] = jnp.dot(xc[...], wu[:, f], preferred_element_type=F32)
        cps["b", j] = swap_part(pb, rb, j, 6 * j + 1)

    def blocks(j):
        for i in range(0, half if j < SPLIT else tok, RB):
            yield pl.ds(pl.multiple_of(mine + i, RB), RB) if j < SPLIT else slice(i, i + RB), slice(i, i + RB)

    for j in range(nf):
        f = slice(j * FC, (j + 1) * FC)
        cps["a", j].wait_recv()
        cps["b", j].wait_recv()
        for r, i in blocks(j):
            a = pa[j, r, :] + ra[j, i, :]
            b = pb[j, r, :] + rb[j, i, :]
            s = jax.nn.sigmoid(a)
            u = a * s
            h[r, f] = (u * b).astype(BF16)
            sd[j, i, :] = s * (1.0 + a * (1.0 - s))
            ra[j, i, :] = u
            rb[j, i, :] = b
        if j < SPLIT:
            own = h.at[pl.ds(mine, half), f]
            cps["h", j] = swap(own, own, 6 * j + 3)
    def y_part(n):
        o = slice(n * DC, (n + 1) * DC)
        yp[:, o] = jnp.dot(h[...], wd[:, o], preferred_element_type=F32)
        for q in range(2):
            for e, chip in enumerate((t1, t_d)):
                s1[n, (q * 2 + e) * rows:(q * 2 + e + 1) * rows, :] = yp[rows_of(q, chip), o]
        cps["1", n] = remote(s1.at[n], r1.at[n], ys.at[4 * n], yrs.at[4 * n], t1, c)

    def y_step(n):
        o = slice(n * DC, (n + 1) * DC)
        cps["1", n].wait_recv()

        def got(q, e):
            return r1[n, pl.ds(pl.multiple_of((q * 2 + e) * rows, rows), rows), :]

        s2[n, 0] = yp[rows_of(c, t2), o] + got(c, 1)
        s2[n, 1] = yp[rows_of(1 - c, t2), o] + got(1 - c, 1)
        cps["2", n] = remote(s2.at[n, 0], r2.at[n, 0], ys.at[4 * n + 1], yrs.at[4 * n + 1], t2, c)
        cps["3", n] = remote(s2.at[n, 1], r2.at[n, 1], ys.at[4 * n + 2], yrs.at[4 * n + 2], t2, 1 - c)
        sc[n] = yp[rows_of(1 - c, t), o] + got(1 - c, 0)
        cps["4", n] = remote(sc.at[n], rc.at[n], ys.at[4 * n + 3], yrs.at[4 * n + 3], t, 1 - c)
        yk[n] = yp[rows_of(c, t), o] + got(c, 0)

    def y_done(n):
        for k in "234":
            cps[k, n].wait_recv()
        for q, tot in ((c, yk[n] + r2[n, 0]), (1 - c, rc[n] + r2[n, 1])):
            cols = pl.ds(pl.multiple_of(q * d_half + n * DC, DC), DC)
            y_ref[:, cols] = (x_v[:, cols].astype(F32) + tot).astype(BF16)

    def g_part(j):
        pg[j] = lax.dot_general(gc[...], wd[j * FC:(j + 1) * FC, :], NT, preferred_element_type=F32)
        cps["g", j] = swap_part(pg, rg, j, 6 * j + 2)

    def grad(j):
        f = slice(j * FC, (j + 1) * FC)
        cps["g", j].wait_recv()
        for r, i in blocks(j):
            g = pg[j, r, :] + rg[j, i, :]
            da[r, f] = (g * rb[j, i, :] * sd[j, i, :]).astype(BF16)
            db[r, f] = (g * ra[j, i, :]).astype(BF16)
        if j < SPLIT:
            own = da.at[pl.ds(mine, half), f]
            cps["da", j] = swap(own, own, 6 * j + 4)
            own = db.at[pl.ds(mine, half), f]
            cps["db", j] = swap(own, own, 6 * j + 5)

    def dx_part(j):
        f = slice(j * FC, (j + 1) * FC)
        if j < SPLIT:
            cps["da", j].wait_recv()
            cps["db", j].wait_recv()
        for n in range(nd):
            o = slice(n * DC, (n + 1) * DC)
            part = (lax.dot_general(da[:, f], wg[o, f], NT, preferred_element_type=F32)
                    + lax.dot_general(db[:, f], wu[o, f], NT, preferred_element_type=F32))
            dxp[:, o] = part if j == 0 else dxp[:, o] + part

    cw[2].wait()
    for j in range(SPLIT):
        cps["h", j].wait_recv()
    y_part(0)
    y_part(1)
    y_part(2)
    for cp in sg:
        cp.wait_recv()
    g_part(0)
    g_part(1)
    g_part(2)
    grad(0)
    g_part(3)
    grad(1)
    y_step(0)
    dx_part(0)
    grad(2)
    y_step(1)
    dx_part(1)
    grad(3)
    y_step(2)
    dx_part(2)
    dx_part(3)

    for i in range(8):
        r = ((i % 2) * 4 + i // 2) * rows
        p_out[i] = dxp[r:r + rows, :]
    for q in range(2):
        p_out[t * 2 + q] += gc[rows_of(q, t), :].astype(F32)
    gc_out[...] = gc[...]
    h_out[...] = h[...]
    da_out[...] = da[...]
    db_out[...] = db[...]
    for n in range(nd):
        y_done(n)

    for cp in sg:
        cp.wait_send()
    for cp in cps.values():
        cp.wait_send()
    out_x.wait()


def _finish(y_in, p, y_ref, dx_ref):
    d_half = p.shape[2]
    y_ref[...] = y_in[...]
    for q in range(2):
        dx_ref[:, q * d_half:(q + 1) * d_half] = (p[q] + p[q + 2] + p[q + 4] + p[q + 6]).astype(BF16)


def _grads(h, da, db, xc_hbm, gc, dwd_hbm, dwg_hbm, dwu_hbm, buf_d, buf_g, xc, sem_d, sem_g, sem_x):
    ff = h.shape[1]
    d_half = xc.shape[1]
    nb_d, tr_d = buf_d.shape[:2]
    nb_g, tr_g = buf_g.shape[:2]
    cx = pltpu.make_async_copy(xc_hbm, xc, sem_x)
    cx.start()

    def run(lhs, rhs, out, buf, sem, n, tr, nb, start, prev_out):
        def step(i, carry):
            slot = lax.rem(i + start, nb)
            r = pl.multiple_of(i * tr, tr)

            def drain():
                pltpu.make_async_copy(buf.at[slot], prev_out.at[pl.ds(0, tr), :], sem.at[slot]).wait()

            if start >= nb:
                drain()
            else:
                pl.when(i + start >= nb)(drain)
            buf[slot] = lax.dot_general(lhs[:, pl.ds(r, tr)], rhs[...], TN, preferred_element_type=F32)
            pltpu.make_async_copy(buf.at[slot], out.at[pl.ds(r, tr), :], sem.at[slot]).start()
            return carry

        lax.fori_loop(0, n, step, 0)

    n_d = ff // tr_d
    n_g = d_half // tr_g
    run(h, gc, dwd_hbm, buf_d, sem_d, n_d, tr_d, nb_d, 0, dwd_hbm)
    cx.wait()
    run(xc, da, dwg_hbm, buf_g, sem_g, n_g, tr_g, nb_g, 0, dwg_hbm)
    run(xc, db, dwu_hbm, buf_g, sem_g, n_g, tr_g, nb_g, n_g, dwu_hbm)
    for s in range(nb_d):
        pltpu.make_async_copy(buf_d.at[s], dwd_hbm.at[pl.ds(0, tr_d), :], sem_d.at[s]).wait()
    for s in range(nb_g):
        pltpu.make_async_copy(buf_g.at[s], dwu_hbm.at[pl.ds(0, tr_g), :], sem_g.at[s]).wait()


def solution(mesh):
    def local_step(x, wg, wu, wd, gy):
        rows, d_full = x.shape
        d_half, ff = wg.shape
        tok = rows * 8
        nf = ff // FC
        nd = d_half // DC
        any_ = pl.BlockSpec(memory_space=pl.ANY)
        hbm = pl.BlockSpec(memory_space=pltpu.HBM)
        vm = pl.BlockSpec(memory_space=pltpu.VMEM)
        S = jax.ShapeDtypeStruct
        dma = pltpu.SemaphoreType.DMA
        full = pltpu.VMEM((nf, tok, FC), F32)
        block = pltpu.VMEM((nd, rows, DC), F32)
        y, xc, gc, h, da, db, parts = pl.pallas_call(
            _front,
            name="front",
            out_shape=(S((rows, d_full), BF16),
                       pltpu.HBM((tok, d_half), BF16), S((tok, d_half), BF16),
                       S((tok, ff), BF16), S((tok, ff), BF16), S((tok, ff), BF16))
            + (S((8, rows, d_half), F32),),
            in_specs=[hbm] * 5,
            out_specs=(vm, hbm, vm, vm, vm, vm, vm),
            scratch_shapes=[
                pltpu.VMEM((rows, d_full), BF16), pltpu.VMEM((rows, d_full), BF16),
                pltpu.VMEM((d_half, ff), BF16), pltpu.VMEM((d_half, ff), BF16), pltpu.VMEM((ff, d_half), BF16),
                pltpu.VMEM((tok, d_half), BF16), pltpu.VMEM((tok, d_half), BF16),
                full, full, full, full, full, full, full,
                pltpu.VMEM((tok, ff), BF16), pltpu.VMEM((tok, ff), BF16), pltpu.VMEM((tok, ff), BF16),
                pltpu.VMEM((tok, d_half), F32),
                pltpu.VMEM((nd, 4 * rows, DC), F32), pltpu.VMEM((nd, 4 * rows, DC), F32),
                pltpu.VMEM((nd, 2, rows, DC), F32), pltpu.VMEM((nd, 2, rows, DC), F32),
                block, block, block,
                pltpu.VMEM((tok, d_half), F32),
                dma((5,)), dma((1,)), dma((7,)), dma((7,)), dma((7,)), dma((7,)),
                dma((6 * nf,)), dma((6 * nf,)), dma((4 * nd,)), dma((4 * nd,)),
            ],
            compiler_params=pltpu.CompilerParams(collective_id=0, has_side_effects=True,
                                                 vmem_limit_bytes=50 * 1024 * 1024),
        )(*(pltpu.with_memory_space_constraint(v, pltpu.HBM) for v in (x, wg, wu, wd, gy)))
        parts = lax.all_to_all(parts, ("tp", "dp"), 0, 0, tiled=True)

        tr = 128
        dwd, dwg, dwu = pl.pallas_call(
            _grads,
            name="grads",
            out_shape=(S((ff, d_half), F32), S((d_half, ff), F32), S((d_half, ff), F32)),
            in_specs=[vm, vm, vm, hbm, vm],
            out_specs=(any_, any_, any_),
            scratch_shapes=[pltpu.VMEM((16, tr, d_half), F32), pltpu.VMEM((12, tr, ff), F32),
                            pltpu.VMEM((tok, d_half), BF16), dma((16,)), dma((12,)), dma(())],
            cost_estimate=pl.CostEstimate(flops=6 * tok * d_half * ff, bytes_accessed=12 * d_half * ff,
                                          transcendentals=0),
            compiler_params=pltpu.CompilerParams(vmem_limit_bytes=34 * 1024 * 1024),
        )(h, da, db, pltpu.with_memory_space_constraint(xc, pltpu.HBM), gc)
        y, dx = pl.pallas_call(
            _finish,
            name="finish",
            out_shape=(S((rows, d_full), BF16), S((rows, d_full), BF16)),
            in_specs=[vm] * 2,
            out_specs=(vm, vm),
            compiler_params=pltpu.CompilerParams(vmem_limit_bytes=6 * 1024 * 1024),
        )(y, parts)
        return y, dx, dwg, dwu, dwd

    row_spec = P(("dp", "tp"), None)
    up_spec = P("dp", "tp")
    down_spec = P("tp", "dp")
    return jax.shard_map(local_step, mesh=mesh,
                         in_specs=(row_spec, up_spec, up_spec, down_spec, row_spec),
                         out_specs=(row_spec, row_spec, up_spec, up_spec, down_spec),
                         check_vma=False)
```

```python
import functools

import jax
import jax.numpy as jnp
from jax import lax
from jax.experimental import pallas as pl
from jax.experimental.pallas import tpu as pltpu
from jax.sharding import PartitionSpec as P

MESH = pl.DeviceIdType.MESH
F32 = jnp.float32
BF16 = jnp.bfloat16

NT = (((1,), (1,)), ((), ()))
TN = (((0,), (0,)), ((), ()))

FC = 512
DC = 512
SPLIT = 3
RB = 32


def _front(x_hbm, wg_hbm, wu_hbm, wd_hbm, gy_hbm,
           y_ref, xc_out, gc_out, h_out, da_out, db_out, p_out,
           x_v, gy_v, wg, wu, wd, xc, gc,
           pa, pb, pg, ra, rb, rg, sd, h, da, db,
           yp, s1, r1, s2, r2, sc, rc, yk, dxp,
           w_sem, o_sem, xs, xrs, gs, grs, es, ers, ys, yrs):
    rows, d_full = x_v.shape
    tok, d_half = xc.shape
    half = tok // 2
    nf = wg.shape[1] // FC
    nd = d_half // DC
    t = lax.axis_index("tp")
    c = lax.axis_index("dp")
    ty, tx = t // 2, t % 2
    tx_n = ty * 2 + 1 - tx
    ty_n = (1 - ty) * 2 + tx
    t_d = 3 - t
    t1 = (1 - c) * tx_n + c * ty_n
    t2 = (1 - c) * ty_n + c * tx_n
    order = ((t_d, c), (t_d, 1 - c), (tx_n, c), (tx_n, 1 - c), (ty_n, c), (ty_n, 1 - c), (t, 1 - c))

    def rows_of(q, chip):
        return pl.ds(pl.multiple_of((q * 4 + chip) * rows, rows), rows)

    def cols_of(q):
        return pl.ds(pl.multiple_of(q * d_half, d_half), d_half)

    cx = pltpu.make_async_copy(x_hbm, x_v, w_sem.at[0])
    cg = pltpu.make_async_copy(gy_hbm, gy_v, w_sem.at[1])
    cw = [pltpu.make_async_copy(a, b, w_sem.at[2 + i])
          for i, (a, b) in enumerate(((wg_hbm, wg), (wu_hbm, wu), (wd_hbm, wd)))]
    cx.start()
    cg.start()
    for w in cw:
        w.start()

    barrier = pltpu.get_barrier_semaphore()
    for chip, q in order:
        pl.semaphore_signal(barrier, inc=1, device_id={"tp": chip, "dp": q}, device_id_type=MESH)
    pl.semaphore_wait(barrier, 7)

    def remote(src, dst, ssem, rsem, chip, q):
        cp = pltpu.make_async_remote_copy(src_ref=src, dst_ref=dst, send_sem=ssem, recv_sem=rsem,
                                          device_id={"tp": chip, "dp": q}, device_id_type=MESH)
        cp.start()
        return cp

    def swap(src, dst, i):
        return remote(src, dst, es.at[i], ers.at[i], t, 1 - c)

    def spread(own, cols, ssem, rsem):
        return [remote(own.at[:, cols_of(q)], cols.at[rows_of(c, t), :], ssem.at[k], rsem.at[k], chip, q)
                for k, (chip, q) in enumerate(order)]

    cx.wait()
    sx = spread(x_v, xc, xs, xrs)
    xc[rows_of(c, t), :] = x_v[:, cols_of(c)]
    cg.wait()
    for cp in sx:
        cp.wait_send()
    sg = spread(gy_v, gc, gs, grs)
    gc[rows_of(c, t), :] = gy_v[:, cols_of(c)]

    mine = pl.multiple_of(c * half, half)
    theirs = pl.ds(pl.multiple_of((1 - c) * half, half), half)
    cw[0].wait()
    cw[1].wait()
    for cp in sx:
        cp.wait_recv()
    out_x = pltpu.make_async_copy(xc, xc_out, o_sem.at[0])
    out_x.start()
    cps = {}

    def swap_part(part, got, j, i):
        if j < SPLIT:
            return swap(part.at[j, theirs, :], got.at[j, pl.ds(0, half), :], i)
        return swap(part.at[j], got.at[j], i)

    for j in range(nf):
        f = slice(j * FC, (j + 1) * FC)
        pa[j] = jnp.dot(xc[...], wg[:, f], preferred_element_type=F32)
        cps["a", j] = swap_part(pa, ra, j, 6 * j)
        pb[j] = jnp.dot(xc[...], wu[:, f], preferred_element_type=F32)
        cps["b", j] = swap_part(pb, rb, j, 6 * j + 1)

    def blocks(j):
        for i in range(0, half if j < SPLIT else tok, RB):
            yield pl.ds(pl.multiple_of(mine + i, RB), RB) if j < SPLIT else slice(i, i + RB), slice(i, i + RB)

    for j in range(nf):
        f = slice(j * FC, (j + 1) * FC)
        cps["a", j].wait_recv()
        cps["b", j].wait_recv()
        for r, i in blocks(j):
            a = pa[j, r, :] + ra[j, i, :]
            b = pb[j, r, :] + rb[j, i, :]
            s = jax.nn.sigmoid(a)
            u = a * s
            h[r, f] = (u * b).astype(BF16)
            sd[j, i, :] = s * (1.0 + a * (1.0 - s))
            ra[j, i, :] = u
            rb[j, i, :] = b
        if j < SPLIT:
            own = h.at[pl.ds(mine, half), f]
            cps["h", j] = swap(own, own, 6 * j + 3)
    def y_part(n):
        o = slice(n * DC, (n + 1) * DC)
        yp[:, o] = jnp.dot(h[...], wd[:, o], preferred_element_type=F32)
        for q in range(2):
            for e, chip in enumerate((t1, t_d)):
                s1[n, (q * 2 + e) * rows:(q * 2 + e + 1) * rows, :] = yp[rows_of(q, chip), o]
        cps["1", n] = remote(s1.at[n], r1.at[n], ys.at[4 * n], yrs.at[4 * n], t1, c)

    def y_step(n):
        o = slice(n * DC, (n + 1) * DC)
        cps["1", n].wait_recv()

        def got(q, e):
            return r1[n, pl.ds(pl.multiple_of((q * 2 + e) * rows, rows), rows), :]

        s2[n, 0] = yp[rows_of(c, t2), o] + got(c, 1)
        s2[n, 1] = yp[rows_of(1 - c, t2), o] + got(1 - c, 1)
        cps["2", n] = remote(s2.at[n, 0], r2.at[n, 0], ys.at[4 * n + 1], yrs.at[4 * n + 1], t2, c)
        cps["3", n] = remote(s2.at[n, 1], r2.at[n, 1], ys.at[4 * n + 2], yrs.at[4 * n + 2], t2, 1 - c)
        sc[n] = yp[rows_of(1 - c, t), o] + got(1 - c, 0)
        cps["4", n] = remote(sc.at[n], rc.at[n], ys.at[4 * n + 3], yrs.at[4 * n + 3], t, 1 - c)
        yk[n] = yp[rows_of(c, t), o] + got(c, 0)

    def y_done(n):
        for k in "234":
            cps[k, n].wait_recv()
        for q, tot in ((c, yk[n] + r2[n, 0]), (1 - c, rc[n] + r2[n, 1])):
            cols = pl.ds(pl.multiple_of(q * d_half + n * DC, DC), DC)
            y_ref[:, cols] = (x_v[:, cols].astype(F32) + tot).astype(BF16)

    def g_part(j):
        pg[j] = lax.dot_general(gc[...], wd[j * FC:(j + 1) * FC, :], NT, preferred_element_type=F32)
        cps["g", j] = swap_part(pg, rg, j, 6 * j + 2)

    def grad(j):
        f = slice(j * FC, (j + 1) * FC)
        cps["g", j].wait_recv()
        for r, i in blocks(j):
            g = pg[j, r, :] + rg[j, i, :]
            da[r, f] = (g * rb[j, i, :] * sd[j, i, :]).astype(BF16)
            db[r, f] = (g * ra[j, i, :]).astype(BF16)
        if j < SPLIT:
            own = da.at[pl.ds(mine, half), f]
            cps["da", j] = swap(own, own, 6 * j + 4)
            own = db.at[pl.ds(mine, half), f]
            cps["db", j] = swap(own, own, 6 * j + 5)

    def dx_part(j):
        f = slice(j * FC, (j + 1) * FC)
        if j < SPLIT:
            cps["da", j].wait_recv()
            cps["db", j].wait_recv()
        for n in range(nd):
            o = slice(n * DC, (n + 1) * DC)
            part = (lax.dot_general(da[:, f], wg[o, f], NT, preferred_element_type=F32)
                    + lax.dot_general(db[:, f], wu[o, f], NT, preferred_element_type=F32))
            dxp[:, o] = part if j == 0 else dxp[:, o] + part

    cw[2].wait()
    for j in range(SPLIT):
        cps["h", j].wait_recv()
    y_part(0)
    y_part(1)
    y_part(2)
    for cp in sg:
        cp.wait_recv()
    g_part(0)
    g_part(1)
    g_part(2)
    grad(0)
    g_part(3)
    grad(1)
    y_step(0)
    dx_part(0)
    grad(2)
    y_step(1)
    dx_part(1)
    grad(3)
    y_step(2)
    dx_part(2)
    dx_part(3)

    for i in range(8):
        r = ((i % 2) * 4 + i // 2) * rows
        p_out[i] = dxp[r:r + rows, :]
    for q in range(2):
        p_out[t * 2 + q] += gc[rows_of(q, t), :].astype(F32)
    gc_out[...] = gc[...]
    h_out[...] = h[...]
    da_out[...] = da[...]
    db_out[...] = db[...]
    for n in range(nd):
        y_done(n)

    for cp in sg:
        cp.wait_send()
    for cp in cps.values():
        cp.wait_send()
    out_x.wait()


def _finish(y_in, p, y_ref, dx_ref):
    d_half = p.shape[2]
    y_ref[...] = y_in[...]
    for q in range(2):
        dx_ref[:, q * d_half:(q + 1) * d_half] = (p[q] + p[q + 2] + p[q + 4] + p[q + 6]).astype(BF16)


def _grads(h, da, db, xc_hbm, gc, dwd_hbm, dwg_hbm, dwu_hbm, buf_d, buf_g, xc, sem_d, sem_g, sem_x):
    ff = h.shape[1]
    d_half = xc.shape[1]
    nb_d, tr_d = buf_d.shape[:2]
    nb_g, tr_g = buf_g.shape[:2]
    cx = pltpu.make_async_copy(xc_hbm, xc, sem_x)
    cx.start()

    def run(lhs, rhs, out, buf, sem, n, tr, nb, start, prev_out):
        def step(i, carry):
            slot = lax.rem(i + start, nb)
            r = pl.multiple_of(i * tr, tr)

            def drain():
                pltpu.make_async_copy(buf.at[slot], prev_out.at[pl.ds(0, tr), :], sem.at[slot]).wait()

            if start >= nb:
                drain()
            else:
                pl.when(i + start >= nb)(drain)
            buf[slot] = lax.dot_general(lhs[:, pl.ds(r, tr)], rhs[...], TN, preferred_element_type=F32)
            pltpu.make_async_copy(buf.at[slot], out.at[pl.ds(r, tr), :], sem.at[slot]).start()
            return carry

        lax.fori_loop(0, n, step, 0)

    n_d = ff // tr_d
    n_g = d_half // tr_g
    run(h, gc, dwd_hbm, buf_d, sem_d, n_d, tr_d, nb_d, 0, dwd_hbm)
    cx.wait()
    run(xc, da, dwg_hbm, buf_g, sem_g, n_g, tr_g, nb_g, 0, dwg_hbm)
    run(xc, db, dwu_hbm, buf_g, sem_g, n_g, tr_g, nb_g, n_g, dwu_hbm)
    for s in range(nb_d):
        pltpu.make_async_copy(buf_d.at[s], dwd_hbm.at[pl.ds(0, tr_d), :], sem_d.at[s]).wait()
    for s in range(nb_g):
        pltpu.make_async_copy(buf_g.at[s], dwu_hbm.at[pl.ds(0, tr_g), :], sem_g.at[s]).wait()


def solution(mesh):
    def local_step(x, wg, wu, wd, gy):
        rows, d_full = x.shape
        d_half, ff = wg.shape
        tok = rows * 8
        nf = ff // FC
        nd = d_half // DC
        any_ = pl.BlockSpec(memory_space=pl.ANY)
        hbm = pl.BlockSpec(memory_space=pltpu.HBM)
        vm = pl.BlockSpec(memory_space=pltpu.VMEM)
        S = jax.ShapeDtypeStruct
        dma = pltpu.SemaphoreType.DMA
        full = pltpu.VMEM((nf, tok, FC), F32)
        block = pltpu.VMEM((nd, rows, DC), F32)
        y, xc, gc, h, da, db, parts = pl.pallas_call(
            _front,
            name="front",
            out_shape=(S((rows, d_full), BF16),
                       pltpu.HBM((tok, d_half), BF16), S((tok, d_half), BF16),
                       S((tok, ff), BF16), S((tok, ff), BF16), S((tok, ff), BF16))
            + (S((8, rows, d_half), F32),),
            in_specs=[hbm] * 5,
            out_specs=(vm, hbm, vm, vm, vm, vm, vm),
            scratch_shapes=[
                pltpu.VMEM((rows, d_full), BF16), pltpu.VMEM((rows, d_full), BF16),
                pltpu.VMEM((d_half, ff), BF16), pltpu.VMEM((d_half, ff), BF16), pltpu.VMEM((ff, d_half), BF16),
                pltpu.VMEM((tok, d_half), BF16), pltpu.VMEM((tok, d_half), BF16),
                full, full, full, full, full, full, full,
                pltpu.VMEM((tok, ff), BF16), pltpu.VMEM((tok, ff), BF16), pltpu.VMEM((tok, ff), BF16),
                pltpu.VMEM((tok, d_half), F32),
                pltpu.VMEM((nd, 4 * rows, DC), F32), pltpu.VMEM((nd, 4 * rows, DC), F32),
                pltpu.VMEM((nd, 2, rows, DC), F32), pltpu.VMEM((nd, 2, rows, DC), F32),
                block, block, block,
                pltpu.VMEM((tok, d_half), F32),
                dma((5,)), dma((1,)), dma((7,)), dma((7,)), dma((7,)), dma((7,)),
                dma((6 * nf,)), dma((6 * nf,)), dma((4 * nd,)), dma((4 * nd,)),
            ],
            compiler_params=pltpu.CompilerParams(collective_id=0, has_side_effects=True,
                                                 vmem_limit_bytes=50 * 1024 * 1024),
        )(*(pltpu.with_memory_space_constraint(v, pltpu.HBM) for v in (x, wg, wu, wd, gy)))
        parts = lax.all_to_all(parts, ("tp", "dp"), 0, 0, tiled=True)

        tr = 512
        dwd, dwg, dwu = pl.pallas_call(
            _grads,
            name="grads",
            out_shape=(S((ff, d_half), F32), S((d_half, ff), F32), S((d_half, ff), F32)),
            in_specs=[vm, vm, vm, hbm, vm],
            out_specs=(any_, any_, any_),
            scratch_shapes=[pltpu.VMEM((4, tr, d_half), F32), pltpu.VMEM((6, tr, ff), F32),
                            pltpu.VMEM((tok, d_half), BF16), dma((4,)), dma((6,)), dma(())],
            cost_estimate=pl.CostEstimate(flops=6 * tok * d_half * ff, bytes_accessed=12 * d_half * ff,
                                          transcendentals=0),
            compiler_params=pltpu.CompilerParams(vmem_limit_bytes=50 * 1024 * 1024),
        )(h, da, db, pltpu.with_memory_space_constraint(xc, pltpu.HBM), gc)
        y, dx = pl.pallas_call(
            _finish,
            name="finish",
            out_shape=(S((rows, d_full), BF16), S((rows, d_full), BF16)),
            in_specs=[vm] * 2,
            out_specs=(vm, vm),
            compiler_params=pltpu.CompilerParams(vmem_limit_bytes=6 * 1024 * 1024),
        )(y, parts)
        return y, dx, dwg, dwu, dwd

    row_spec = P(("dp", "tp"), None)
    up_spec = P("dp", "tp")
    down_spec = P("tp", "dp")
    return jax.shard_map(local_step, mesh=mesh,
                         in_specs=(row_spec, up_spec, up_spec, down_spec, row_spec),
                         out_specs=(row_spec, row_spec, up_spec, up_spec, down_spec),
                         check_vma=False)
```

```python
import functools

import jax
import jax.numpy as jnp
from jax import lax
from jax.experimental import pallas as pl
from jax.experimental.pallas import tpu as pltpu
from jax.sharding import PartitionSpec as P

MESH = pl.DeviceIdType.MESH
F32 = jnp.float32
BF16 = jnp.bfloat16

NT = (((1,), (1,)), ((), ()))
TN = (((0,), (0,)), ((), ()))

FC = 512
DC = 512
PIECES = ((0, 512), (512, 512), (1024, 256), (1280, 128))
FRONT = 1408
SPLIT = 2
RB = 32


def _front(x_hbm, wg_hbm, wu_hbm, wd_hbm, gy_hbm,
           y_ref, xc_out, gc_out, h_out, da_out, db_out, p_out,
           x_v, gy_v, wg, wu, wd, xc, gc,
           pa, pb, pg, ra, rb, rg, sd, h, da, db,
           yp, s1, r1, s2, r2, sc, rc, yk, dxp,
           w_sem, o_sem, xs, xrs, gs, grs, es, ers, ys, yrs):
    rows, d_full = x_v.shape
    tok, d_half = xc.shape
    half = tok // 2
    nf = wg.shape[1] // FC
    nd = d_half // DC
    t = lax.axis_index("tp")
    c = lax.axis_index("dp")
    ty, tx = t // 2, t % 2
    tx_n = ty * 2 + 1 - tx
    ty_n = (1 - ty) * 2 + tx
    t_d = 3 - t
    t1 = (1 - c) * tx_n + c * ty_n
    t2 = (1 - c) * ty_n + c * tx_n
    order = ((t_d, c), (t_d, 1 - c), (tx_n, c), (tx_n, 1 - c), (ty_n, c), (ty_n, 1 - c), (t, 1 - c))

    def rows_of(q, chip):
        return pl.ds(pl.multiple_of((q * 4 + chip) * rows, rows), rows)

    def cols_of(q):
        return pl.ds(pl.multiple_of(q * d_half, d_half), d_half)

    cx = pltpu.make_async_copy(x_hbm, x_v, w_sem.at[0])
    cg = pltpu.make_async_copy(gy_hbm, gy_v, w_sem.at[1])
    cw = [pltpu.make_async_copy(a, b, w_sem.at[2 + i])
          for i, (a, b) in enumerate(((wg_hbm, wg), (wu_hbm, wu), (wd_hbm, wd)))]
    cx.start()
    cg.start()
    for w in cw:
        w.start()

    barrier = pltpu.get_barrier_semaphore()
    for chip, q in order:
        pl.semaphore_signal(barrier, inc=1, device_id={"tp": chip, "dp": q}, device_id_type=MESH)
    pl.semaphore_wait(barrier, 7)

    def remote(src, dst, ssem, rsem, chip, q):
        cp = pltpu.make_async_remote_copy(src_ref=src, dst_ref=dst, send_sem=ssem, recv_sem=rsem,
                                          device_id={"tp": chip, "dp": q}, device_id_type=MESH)
        cp.start()
        return cp

    def swap(src, dst, i):
        return remote(src, dst, es.at[i], ers.at[i], t, 1 - c)

    def spread(own, cols, ssem, rsem):
        return [remote(own.at[:, cols_of(q)], cols.at[rows_of(c, t), :], ssem.at[k], rsem.at[k], chip, q)
                for k, (chip, q) in enumerate(order)]

    cx.wait()
    sx = spread(x_v, xc, xs, xrs)
    xc[rows_of(c, t), :] = x_v[:, cols_of(c)]
    cg.wait()
    for cp in sx:
        cp.wait_send()
    sg = spread(gy_v, gc, gs, grs)
    gc[rows_of(c, t), :] = gy_v[:, cols_of(c)]

    mine = pl.multiple_of(c * half, half)
    theirs = pl.ds(pl.multiple_of((1 - c) * half, half), half)
    cw[0].wait()
    cw[1].wait()
    for cp in sx:
        cp.wait_recv()
    out_x = pltpu.make_async_copy(xc, xc_out, o_sem.at[0])
    out_x.start()
    cps = {}

    def swap_part(part, got, j, i):
        if j < SPLIT:
            return swap(part.at[j, theirs, :], got.at[j, pl.ds(0, half), :], i)
        return swap(part.at[j], got.at[j], i)

    for j in range(nf):
        f = slice(j * FC, (j + 1) * FC)
        pa[j] = jnp.dot(xc[...], wg[:, f], preferred_element_type=F32)
        cps["a", j] = swap_part(pa, ra, j, 6 * j)
        pb[j] = jnp.dot(xc[...], wu[:, f], preferred_element_type=F32)
        cps["b", j] = swap_part(pb, rb, j, 6 * j + 1)

    def blocks(j):
        for i in range(0, half if j < SPLIT else tok, RB):
            yield pl.ds(pl.multiple_of(mine + i, RB), RB) if j < SPLIT else slice(i, i + RB), slice(i, i + RB)

    for j in range(nf):
        f = slice(j * FC, (j + 1) * FC)
        cps["a", j].wait_recv()
        cps["b", j].wait_recv()
        for r, i in blocks(j):
            a = pa[j, r, :] + ra[j, i, :]
            b = pb[j, r, :] + rb[j, i, :]
            s = jax.nn.sigmoid(a)
            u = a * s
            h[r, f] = (u * b).astype(BF16)
            sd[j, i, :] = s * (1.0 + a * (1.0 - s))
            ra[j, i, :] = u
            rb[j, i, :] = b
        if j < SPLIT:
            own = h.at[pl.ds(mine, half), f]
            cps["h", j] = swap(own, own, 6 * j + 3)
    def y_part(n, pieces):
        o = slice(n * DC, (n + 1) * DC)
        yp[:, o] = jnp.dot(h[...], wd[:, o], preferred_element_type=F32)
        for p in pieces:
            o = slice(PIECES[p][0], sum(PIECES[p]))
            for q in range(2):
                for e, chip in enumerate((t1, t_d)):
                    s1[p][(q * 2 + e) * rows:(q * 2 + e + 1) * rows, :] = yp[rows_of(q, chip), o]
            cps["1", p] = remote(s1[p], r1[p], ys.at[4 * p], yrs.at[4 * p], t1, c)

    def y_step(p):
        o = slice(PIECES[p][0], sum(PIECES[p]))
        cps["1", p].wait_recv()

        def got(q, e):
            return r1[p][pl.ds(pl.multiple_of((q * 2 + e) * rows, rows), rows), :]

        s2[p][0] = yp[rows_of(c, t2), o] + got(c, 1)
        s2[p][1] = yp[rows_of(1 - c, t2), o] + got(1 - c, 1)
        cps["2", p] = remote(s2[p].at[0], r2[p].at[0], ys.at[4 * p + 1], yrs.at[4 * p + 1], t2, c)
        cps["3", p] = remote(s2[p].at[1], r2[p].at[1], ys.at[4 * p + 2], yrs.at[4 * p + 2], t2, 1 - c)
        sc[p][...] = yp[rows_of(1 - c, t), o] + got(1 - c, 0)
        cps["4", p] = remote(sc[p], rc[p], ys.at[4 * p + 3], yrs.at[4 * p + 3], t, 1 - c)
        yk[p][...] = yp[rows_of(c, t), o] + got(c, 0)

    def y_done(p):
        for k in "234":
            cps[k, p].wait_recv()
        o, w = PIECES[p]
        for q, tot in ((c, yk[p][...] + r2[p][0]), (1 - c, rc[p][...] + r2[p][1])):
            cols = pl.ds(pl.multiple_of(q * d_half + o, 128), w)
            y_ref[:, cols] = (x_v[:, cols].astype(F32) + tot).astype(BF16)

    def g_part(j):
        pg[j] = lax.dot_general(gc[...], wd[j * FC:(j + 1) * FC, :], NT, preferred_element_type=F32)
        cps["g", j] = swap_part(pg, rg, j, 6 * j + 2)

    def grad(j):
        f = slice(j * FC, (j + 1) * FC)
        cps["g", j].wait_recv()
        for r, i in blocks(j):
            g = pg[j, r, :] + rg[j, i, :]
            da[r, f] = (g * rb[j, i, :] * sd[j, i, :]).astype(BF16)
            db[r, f] = (g * ra[j, i, :]).astype(BF16)
        if j < SPLIT:
            own = da.at[pl.ds(mine, half), f]
            cps["da", j] = swap(own, own, 6 * j + 4)
            own = db.at[pl.ds(mine, half), f]
            cps["db", j] = swap(own, own, 6 * j + 5)

    def dx_part(j):
        f = slice(j * FC, (j + 1) * FC)
        if j < SPLIT:
            cps["da", j].wait_recv()
            cps["db", j].wait_recv()
        for n in range(nd):
            o = slice(n * DC, (n + 1) * DC)
            part = (lax.dot_general(da[:, f], wg[o, f], NT, preferred_element_type=F32)
                    + lax.dot_general(db[:, f], wu[o, f], NT, preferred_element_type=F32))
            dxp[:, o] = part if j == 0 else dxp[:, o] + part

    cw[2].wait()
    for j in range(SPLIT):
        cps["h", j].wait_recv()
    y_part(0, (0,))
    y_part(1, (1,))
    y_part(2, (2, 3))
    for cp in sg:
        cp.wait_recv()
    g_part(0)
    g_part(1)
    g_part(2)
    grad(0)
    g_part(3)
    grad(1)
    y_step(0)
    dx_part(0)
    grad(2)
    y_step(1)
    dx_part(1)
    grad(3)
    y_step(2)
    y_step(3)
    dx_part(2)
    dx_part(3)

    for i in range(8):
        r = ((i % 2) * 4 + i // 2) * rows
        p_out[i, :, :d_half] = dxp[r:r + rows, :]
        p_out[i, :, d_half:] = yp[r:r + rows, FRONT:]
    for q in range(2):
        p_out[t * 2 + q, :, :d_half] += gc[rows_of(q, t), :].astype(F32)
        p_out[t * 2 + q, :, d_half:] += xc[rows_of(q, t), FRONT:].astype(F32)
    gc_out[...] = gc[...]
    h_out[...] = h[...]
    da_out[...] = da[...]
    db_out[...] = db[...]
    for p in range(len(PIECES)):
        y_done(p)

    for cp in sg:
        cp.wait_send()
    for cp in cps.values():
        cp.wait_send()
    out_x.wait()


def _finish(y_in, p, y_ref, dx_ref):
    d_half = y_ref.shape[1] // 2
    for q in range(2):
        o = q * d_half
        tot = (p[q] + p[q + 2] + p[q + 4] + p[q + 6]).astype(BF16)
        dx_ref[:, o:o + d_half] = tot[:, :d_half]
        y_ref[:, o:o + FRONT] = y_in[:, o:o + FRONT]
        y_ref[:, o + FRONT:o + d_half] = tot[:, d_half:]


def _grads(h, da, db, xc_hbm, gc, dwd_hbm, dwg_hbm, dwu_hbm, buf_d, buf_g, xc, sem_d, sem_g, sem_x):
    ff = h.shape[1]
    d_half = xc.shape[1]
    nb_d, tr_d = buf_d.shape[:2]
    nb_g, tr_g = buf_g.shape[:2]
    cx = pltpu.make_async_copy(xc_hbm, xc, sem_x)
    cx.start()

    def run(lhs, rhs, out, buf, sem, n, tr, nb, start, prev_out):
        def step(i, carry):
            slot = lax.rem(i + start, nb)
            r = pl.multiple_of(i * tr, tr)

            def drain():
                pltpu.make_async_copy(buf.at[slot], prev_out.at[pl.ds(0, tr), :], sem.at[slot]).wait()

            if start >= nb:
                drain()
            else:
                pl.when(i + start >= nb)(drain)
            buf[slot] = lax.dot_general(lhs[:, pl.ds(r, tr)], rhs[...], TN, preferred_element_type=F32)
            pltpu.make_async_copy(buf.at[slot], out.at[pl.ds(r, tr), :], sem.at[slot]).start()
            return carry

        lax.fori_loop(0, n, step, 0)

    n_d = ff // tr_d
    n_g = d_half // tr_g
    run(h, gc, dwd_hbm, buf_d, sem_d, n_d, tr_d, nb_d, 0, dwd_hbm)
    cx.wait()
    run(xc, da, dwg_hbm, buf_g, sem_g, n_g, tr_g, nb_g, 0, dwg_hbm)
    run(xc, db, dwu_hbm, buf_g, sem_g, n_g, tr_g, nb_g, n_g, dwu_hbm)
    for s in range(nb_d):
        pltpu.make_async_copy(buf_d.at[s], dwd_hbm.at[pl.ds(0, tr_d), :], sem_d.at[s]).wait()
    for s in range(nb_g):
        pltpu.make_async_copy(buf_g.at[s], dwu_hbm.at[pl.ds(0, tr_g), :], sem_g.at[s]).wait()


def solution(mesh):
    def local_step(x, wg, wu, wd, gy):
        rows, d_full = x.shape
        d_half, ff = wg.shape
        tok = rows * 8
        nf = ff // FC
        nd = d_half // DC
        any_ = pl.BlockSpec(memory_space=pl.ANY)
        hbm = pl.BlockSpec(memory_space=pltpu.HBM)
        vm = pl.BlockSpec(memory_space=pltpu.VMEM)
        S = jax.ShapeDtypeStruct
        dma = pltpu.SemaphoreType.DMA
        full = pltpu.VMEM((nf, tok, FC), F32)
        y, xc, gc, h, da, db, parts = pl.pallas_call(
            _front,
            name="front",
            out_shape=(S((rows, d_full), BF16),
                       pltpu.HBM((tok, d_half), BF16), S((tok, d_half), BF16),
                       S((tok, ff), BF16), S((tok, ff), BF16), S((tok, ff), BF16))
            + (S((8, rows, 2 * d_half - FRONT), F32),),
            in_specs=[hbm] * 5,
            out_specs=(vm, hbm, vm, vm, vm, vm, vm),
            scratch_shapes=[
                pltpu.VMEM((rows, d_full), BF16), pltpu.VMEM((rows, d_full), BF16),
                pltpu.VMEM((d_half, ff), BF16), pltpu.VMEM((d_half, ff), BF16), pltpu.VMEM((ff, d_half), BF16),
                pltpu.VMEM((tok, d_half), BF16), pltpu.VMEM((tok, d_half), BF16),
                full, full, full, full, full, full, full,
                pltpu.VMEM((tok, ff), BF16), pltpu.VMEM((tok, ff), BF16), pltpu.VMEM((tok, ff), BF16),
                pltpu.VMEM((tok, d_half), F32),
                [pltpu.VMEM((4 * rows, w), F32) for _, w in PIECES], [pltpu.VMEM((4 * rows, w), F32) for _, w in PIECES],
                [pltpu.VMEM((2, rows, w), F32) for _, w in PIECES], [pltpu.VMEM((2, rows, w), F32) for _, w in PIECES],
                *([pltpu.VMEM((rows, w), F32) for _, w in PIECES] for _ in range(3)),
                pltpu.VMEM((tok, d_half), F32),
                dma((5,)), dma((1,)), dma((7,)), dma((7,)), dma((7,)), dma((7,)),
                dma((6 * nf,)), dma((6 * nf,)), dma((4 * len(PIECES),)), dma((4 * len(PIECES),)),
            ],
            compiler_params=pltpu.CompilerParams(collective_id=0, has_side_effects=True,
                                                 vmem_limit_bytes=50 * 1024 * 1024),
        )(*(pltpu.with_memory_space_constraint(v, pltpu.HBM) for v in (x, wg, wu, wd, gy)))
        parts = lax.all_to_all(parts, ("tp", "dp"), 0, 0, tiled=True)

        tr = 256
        dwd, dwg, dwu = pl.pallas_call(
            _grads,
            name="grads",
            out_shape=(S((ff, d_half), F32), S((d_half, ff), F32), S((d_half, ff), F32)),
            in_specs=[vm, vm, vm, hbm, vm],
            out_specs=(any_, any_, any_),
            scratch_shapes=[pltpu.VMEM((8, tr, d_half), F32), pltpu.VMEM((6, tr, ff), F32),
                            pltpu.VMEM((tok, d_half), BF16), dma((8,)), dma((6,)), dma(())],
            cost_estimate=pl.CostEstimate(flops=6 * tok * d_half * ff, bytes_accessed=12 * d_half * ff,
                                          transcendentals=0),
            compiler_params=pltpu.CompilerParams(vmem_limit_bytes=34 * 1024 * 1024),
        )(h, da, db, pltpu.with_memory_space_constraint(xc, pltpu.HBM), gc)
        y, dx = pl.pallas_call(
            _finish,
            name="finish",
            out_shape=(S((rows, d_full), BF16), S((rows, d_full), BF16)),
            in_specs=[vm] * 2,
            out_specs=(vm, vm),
            compiler_params=pltpu.CompilerParams(vmem_limit_bytes=6 * 1024 * 1024),
        )(y, parts)
        return y, dx, dwg, dwu, dwd

    row_spec = P(("dp", "tp"), None)
    up_spec = P("dp", "tp")
    down_spec = P("tp", "dp")
    return jax.shard_map(local_step, mesh=mesh,
                         in_specs=(row_spec, up_spec, up_spec, down_spec, row_spec),
                         out_specs=(row_spec, row_spec, up_spec, up_spec, down_spec),
                         check_vma=False)
```

```python
import functools

import jax
import jax.numpy as jnp
from jax import lax
from jax.experimental import pallas as pl
from jax.experimental.pallas import tpu as pltpu
from jax.sharding import PartitionSpec as P

MESH = pl.DeviceIdType.MESH
F32 = jnp.float32
BF16 = jnp.bfloat16

NT = (((1,), (1,)), ((), ()))
TN = (((0,), (0,)), ((), ()))

FC = 512
DC = 512
PIECES = ((0, 512), (512, 512), (1024, 256), (1280, 128))
FRONT = 1408
SPLIT = 2
RB = 32


def _front(x_hbm, wg_hbm, wu_hbm, wd_hbm, gy_hbm,
           y_ref, xc_out, gc, h, da, db, p_out,
           x_v, gy_v, wg, wu, wd, xc,
           pa, pb, pg, ra, rb, rg, sd,
           yp, s1, r1, s2, r2, sc, rc, yk, dxp,
           w_sem, o_sem, xs, xrs, gs, grs, es, ers, ys, yrs):
    rows, d_full = x_v.shape
    tok, d_half = xc.shape
    half = tok // 2
    nf = wg.shape[1] // FC
    nd = d_half // DC
    t = lax.axis_index("tp")
    c = lax.axis_index("dp")
    ty, tx = t // 2, t % 2
    tx_n = ty * 2 + 1 - tx
    ty_n = (1 - ty) * 2 + tx
    t_d = 3 - t
    t1 = (1 - c) * tx_n + c * ty_n
    t2 = (1 - c) * ty_n + c * tx_n
    order = ((t_d, c), (t_d, 1 - c), (tx_n, c), (tx_n, 1 - c), (ty_n, c), (ty_n, 1 - c), (t, 1 - c))

    def rows_of(q, chip):
        return pl.ds(pl.multiple_of((q * 4 + chip) * rows, rows), rows)

    def cols_of(q):
        return pl.ds(pl.multiple_of(q * d_half, d_half), d_half)

    cx = pltpu.make_async_copy(x_hbm, x_v, w_sem.at[0])
    cg = pltpu.make_async_copy(gy_hbm, gy_v, w_sem.at[1])
    cw = [pltpu.make_async_copy(a, b, w_sem.at[2 + i])
          for i, (a, b) in enumerate(((wg_hbm, wg), (wu_hbm, wu), (wd_hbm, wd)))]
    cx.start()
    cg.start()
    for w in cw:
        w.start()

    barrier = pltpu.get_barrier_semaphore()
    for chip, q in order:
        pl.semaphore_signal(barrier, inc=1, device_id={"tp": chip, "dp": q}, device_id_type=MESH)
    pl.semaphore_wait(barrier, 7)

    def remote(src, dst, ssem, rsem, chip, q):
        cp = pltpu.make_async_remote_copy(src_ref=src, dst_ref=dst, send_sem=ssem, recv_sem=rsem,
                                          device_id={"tp": chip, "dp": q}, device_id_type=MESH)
        cp.start()
        return cp

    def swap(src, dst, i):
        return remote(src, dst, es.at[i], ers.at[i], t, 1 - c)

    def spread(own, cols, ssem, rsem):
        return [remote(own.at[:, cols_of(q)], cols.at[rows_of(c, t), :], ssem.at[k], rsem.at[k], chip, q)
                for k, (chip, q) in enumerate(order)]

    cx.wait()
    sx = spread(x_v, xc, xs, xrs)
    xc[rows_of(c, t), :] = x_v[:, cols_of(c)]
    cg.wait()
    for cp in sx:
        cp.wait_send()
    sg = spread(gy_v, gc, gs, grs)
    gc[rows_of(c, t), :] = gy_v[:, cols_of(c)]

    mine = pl.multiple_of(c * half, half)
    theirs = pl.ds(pl.multiple_of((1 - c) * half, half), half)
    cw[0].wait()
    cw[1].wait()
    for cp in sx:
        cp.wait_recv()
    out_x = pltpu.make_async_copy(xc, xc_out, o_sem.at[0])
    out_x.start()
    cps = {}

    def swap_part(part, got, j, i):
        if j < SPLIT:
            return swap(part.at[j, theirs, :], got.at[j, pl.ds(0, half), :], i)
        return swap(part.at[j], got.at[j], i)

    for j in range(nf):
        f = slice(j * FC, (j + 1) * FC)
        pa[j] = jnp.dot(xc[...], wg[:, f], preferred_element_type=F32)
        cps["a", j] = swap_part(pa, ra, j, 6 * j)
        pb[j] = jnp.dot(xc[...], wu[:, f], preferred_element_type=F32)
        cps["b", j] = swap_part(pb, rb, j, 6 * j + 1)

    def blocks(j):
        for i in range(0, half if j < SPLIT else tok, RB):
            yield pl.ds(pl.multiple_of(mine + i, RB), RB) if j < SPLIT else slice(i, i + RB), slice(i, i + RB)

    for j in range(nf):
        f = slice(j * FC, (j + 1) * FC)
        cps["a", j].wait_recv()
        cps["b", j].wait_recv()
        for r, i in blocks(j):
            a = pa[j, r, :] + ra[j, i, :]
            b = pb[j, r, :] + rb[j, i, :]
            s = jax.nn.sigmoid(a)
            u = a * s
            h[r, f] = (u * b).astype(BF16)
            sd[j, i, :] = s * (1.0 + a * (1.0 - s))
            ra[j, i, :] = u
            rb[j, i, :] = b
        if j < SPLIT:
            own = h.at[pl.ds(mine, half), f]
            cps["h", j] = swap(own, own, 6 * j + 3)
    def y_part(n, pieces):
        o = slice(n * DC, (n + 1) * DC)
        yp[:, o] = jnp.dot(h[...], wd[:, o], preferred_element_type=F32)
        for p in pieces:
            o = slice(PIECES[p][0], sum(PIECES[p]))
            for q in range(2):
                for e, chip in enumerate((t1, t_d)):
                    s1[p][(q * 2 + e) * rows:(q * 2 + e + 1) * rows, :] = yp[rows_of(q, chip), o]
            cps["1", p] = remote(s1[p], r1[p], ys.at[4 * p], yrs.at[4 * p], t1, c)

    def y_step(p):
        o = slice(PIECES[p][0], sum(PIECES[p]))
        cps["1", p].wait_recv()

        def got(q, e):
            return r1[p][pl.ds(pl.multiple_of((q * 2 + e) * rows, rows), rows), :]

        s2[p][0] = yp[rows_of(c, t2), o] + got(c, 1)
        s2[p][1] = yp[rows_of(1 - c, t2), o] + got(1 - c, 1)
        cps["2", p] = remote(s2[p].at[0], r2[p].at[0], ys.at[4 * p + 1], yrs.at[4 * p + 1], t2, c)
        cps["3", p] = remote(s2[p].at[1], r2[p].at[1], ys.at[4 * p + 2], yrs.at[4 * p + 2], t2, 1 - c)
        sc[p][...] = yp[rows_of(1 - c, t), o] + got(1 - c, 0)
        cps["4", p] = remote(sc[p], rc[p], ys.at[4 * p + 3], yrs.at[4 * p + 3], t, 1 - c)
        yk[p][...] = yp[rows_of(c, t), o] + got(c, 0)

    def y_done(p):
        for k in "234":
            cps[k, p].wait_recv()
        o, w = PIECES[p]
        for q, tot in ((c, yk[p][...] + r2[p][0]), (1 - c, rc[p][...] + r2[p][1])):
            cols = pl.ds(pl.multiple_of(q * d_half + o, 128), w)
            y_ref[:, cols] = (x_v[:, cols].astype(F32) + tot).astype(BF16)

    def g_part(j):
        pg[j] = lax.dot_general(gc[...], wd[j * FC:(j + 1) * FC, :], NT, preferred_element_type=F32)
        cps["g", j] = swap_part(pg, rg, j, 6 * j + 2)

    def grad(j):
        f = slice(j * FC, (j + 1) * FC)
        cps["g", j].wait_recv()
        for r, i in blocks(j):
            g = pg[j, r, :] + rg[j, i, :]
            da[r, f] = (g * rb[j, i, :] * sd[j, i, :]).astype(BF16)
            db[r, f] = (g * ra[j, i, :]).astype(BF16)
        if j < SPLIT:
            own = da.at[pl.ds(mine, half), f]
            cps["da", j] = swap(own, own, 6 * j + 4)
            own = db.at[pl.ds(mine, half), f]
            cps["db", j] = swap(own, own, 6 * j + 5)

    def dx_part(j):
        f = slice(j * FC, (j + 1) * FC)
        if j < SPLIT:
            cps["da", j].wait_recv()
            cps["db", j].wait_recv()
        for n in range(nd):
            o = slice(n * DC, (n + 1) * DC)
            part = (lax.dot_general(da[:, f], wg[o, f], NT, preferred_element_type=F32)
                    + lax.dot_general(db[:, f], wu[o, f], NT, preferred_element_type=F32))
            dxp[:, o] = part if j == 0 else dxp[:, o] + part

    cw[2].wait()
    for j in range(SPLIT):
        cps["h", j].wait_recv()
    y_part(0, (0,))
    y_part(1, (1,))
    y_part(2, (2, 3))
    for cp in sg:
        cp.wait_recv()
    g_part(0)
    g_part(1)
    g_part(2)
    grad(0)
    g_part(3)
    grad(1)
    y_step(0)
    dx_part(0)
    grad(2)
    y_step(1)
    dx_part(1)
    grad(3)
    y_step(2)
    y_step(3)
    dx_part(2)
    dx_part(3)

    for i in range(8):
        r = ((i % 2) * 4 + i // 2) * rows
        p_out[i, :, :d_half] = dxp[r:r + rows, :]
        p_out[i, :, d_half:] = yp[r:r + rows, FRONT:]
    for q in range(2):
        p_out[t * 2 + q, :, :d_half] += gc[rows_of(q, t), :].astype(F32)
        p_out[t * 2 + q, :, d_half:] += xc[rows_of(q, t), FRONT:].astype(F32)
    for p in range(len(PIECES)):
        y_done(p)

    for cp in sg:
        cp.wait_send()
    for cp in cps.values():
        cp.wait_send()
    out_x.wait()


def _finish(y_in, p, y_ref, dx_ref):
    d_half = y_ref.shape[1] // 2
    for q in range(2):
        o = q * d_half
        tot = (p[q] + p[q + 2] + p[q + 4] + p[q + 6]).astype(BF16)
        dx_ref[:, o:o + d_half] = tot[:, :d_half]
        y_ref[:, o:o + FRONT] = y_in[:, o:o + FRONT]
        y_ref[:, o + FRONT:o + d_half] = tot[:, d_half:]


def _grads(h, da, db, xc_hbm, gc, dwd_hbm, dwg_hbm, dwu_hbm, buf_d, buf_g, xc, sem_d, sem_g, sem_x):
    ff = h.shape[1]
    d_half = xc.shape[1]
    nb_d, tr_d = buf_d.shape[:2]
    nb_g, tr_g = buf_g.shape[:2]
    cx = pltpu.make_async_copy(xc_hbm, xc, sem_x)
    cx.start()

    def run(lhs, rhs, out, buf, sem, n, tr, nb, start, prev_out):
        def step(i, carry):
            slot = lax.rem(i + start, nb)
            r = pl.multiple_of(i * tr, tr)

            def drain():
                pltpu.make_async_copy(buf.at[slot], prev_out.at[pl.ds(0, tr), :], sem.at[slot]).wait()

            if start >= nb:
                drain()
            else:
                pl.when(i + start >= nb)(drain)
            buf[slot] = lax.dot_general(lhs[:, pl.ds(r, tr)], rhs[...], TN, preferred_element_type=F32)
            pltpu.make_async_copy(buf.at[slot], out.at[pl.ds(r, tr), :], sem.at[slot]).start()
            return carry

        lax.fori_loop(0, n, step, 0)

    n_d = ff // tr_d
    n_g = d_half // tr_g
    run(h, gc, dwd_hbm, buf_d, sem_d, n_d, tr_d, nb_d, 0, dwd_hbm)
    cx.wait()
    run(xc, da, dwg_hbm, buf_g, sem_g, n_g, tr_g, nb_g, 0, dwg_hbm)
    run(xc, db, dwu_hbm, buf_g, sem_g, n_g, tr_g, nb_g, n_g, dwu_hbm)
    for s in range(nb_d):
        pltpu.make_async_copy(buf_d.at[s], dwd_hbm.at[pl.ds(0, tr_d), :], sem_d.at[s]).wait()
    for s in range(nb_g):
        pltpu.make_async_copy(buf_g.at[s], dwu_hbm.at[pl.ds(0, tr_g), :], sem_g.at[s]).wait()


def solution(mesh):
    def local_step(x, wg, wu, wd, gy):
        rows, d_full = x.shape
        d_half, ff = wg.shape
        tok = rows * 8
        nf = ff // FC
        nd = d_half // DC
        any_ = pl.BlockSpec(memory_space=pl.ANY)
        hbm = pl.BlockSpec(memory_space=pltpu.HBM)
        vm = pl.BlockSpec(memory_space=pltpu.VMEM)
        S = jax.ShapeDtypeStruct
        dma = pltpu.SemaphoreType.DMA
        full = pltpu.VMEM((nf, tok, FC), F32)
        y, xc, gc, h, da, db, parts = pl.pallas_call(
            _front,
            name="front",
            out_shape=(S((rows, d_full), BF16),
                       pltpu.HBM((tok, d_half), BF16), S((tok, d_half), BF16),
                       S((tok, ff), BF16), S((tok, ff), BF16), S((tok, ff), BF16))
            + (S((8, rows, 2 * d_half - FRONT), F32),),
            in_specs=[hbm] * 5,
            out_specs=(vm, hbm, vm, vm, vm, vm, vm),
            scratch_shapes=[
                pltpu.VMEM((rows, d_full), BF16), pltpu.VMEM((rows, d_full), BF16),
                pltpu.VMEM((d_half, ff), BF16), pltpu.VMEM((d_half, ff), BF16), pltpu.VMEM((ff, d_half), BF16),
                pltpu.VMEM((tok, d_half), BF16),
                full, full, full, full, full, full, full,
                pltpu.VMEM((tok, d_half), F32),
                [pltpu.VMEM((4 * rows, w), F32) for _, w in PIECES], [pltpu.VMEM((4 * rows, w), F32) for _, w in PIECES],
                [pltpu.VMEM((2, rows, w), F32) for _, w in PIECES], [pltpu.VMEM((2, rows, w), F32) for _, w in PIECES],
                *([pltpu.VMEM((rows, w), F32) for _, w in PIECES] for _ in range(3)),
                pltpu.VMEM((tok, d_half), F32),
                dma((5,)), dma((1,)), dma((7,)), dma((7,)), dma((7,)), dma((7,)),
                dma((6 * nf,)), dma((6 * nf,)), dma((4 * len(PIECES),)), dma((4 * len(PIECES),)),
            ],
            compiler_params=pltpu.CompilerParams(collective_id=0, has_side_effects=True,
                                                 vmem_limit_bytes=50 * 1024 * 1024),
        )(*(pltpu.with_memory_space_constraint(v, pltpu.HBM) for v in (x, wg, wu, wd, gy)))
        parts = lax.all_to_all(parts, ("tp", "dp"), 0, 0, tiled=True)

        tr = 256
        dwd, dwg, dwu = pl.pallas_call(
            _grads,
            name="grads",
            out_shape=(S((ff, d_half), F32), S((d_half, ff), F32), S((d_half, ff), F32)),
            in_specs=[vm, vm, vm, hbm, vm],
            out_specs=(any_, any_, any_),
            scratch_shapes=[pltpu.VMEM((8, tr, d_half), F32), pltpu.VMEM((6, tr, ff), F32),
                            pltpu.VMEM((tok, d_half), BF16), dma((8,)), dma((6,)), dma(())],
            cost_estimate=pl.CostEstimate(flops=6 * tok * d_half * ff, bytes_accessed=12 * d_half * ff,
                                          transcendentals=0),
            compiler_params=pltpu.CompilerParams(vmem_limit_bytes=34 * 1024 * 1024),
        )(h, da, db, pltpu.with_memory_space_constraint(xc, pltpu.HBM), gc)
        y, dx = pl.pallas_call(
            _finish,
            name="finish",
            out_shape=(S((rows, d_full), BF16), S((rows, d_full), BF16)),
            in_specs=[vm] * 2,
            out_specs=(vm, vm),
            compiler_params=pltpu.CompilerParams(vmem_limit_bytes=6 * 1024 * 1024),
        )(y, parts)
        return y, dx, dwg, dwu, dwd

    row_spec = P(("dp", "tp"), None)
    up_spec = P("dp", "tp")
    down_spec = P("tp", "dp")
    return jax.shard_map(local_step, mesh=mesh,
                         in_specs=(row_spec, up_spec, up_spec, down_spec, row_spec),
                         out_specs=(row_spec, row_spec, up_spec, up_spec, down_spec),
                         check_vma=False)
```

```python
import functools

import jax
import jax.numpy as jnp
from jax import lax
from jax.experimental import pallas as pl
from jax.experimental.pallas import tpu as pltpu
from jax.sharding import PartitionSpec as P

MESH = pl.DeviceIdType.MESH
F32 = jnp.float32
BF16 = jnp.bfloat16

NT = (((1,), (1,)), ((), ()))
TN = (((0,), (0,)), ((), ()))

FC = 512
DC = 512
PIECES = ((0, 512), (512, 512), (1024, 256), (1280, 128))
FRONT = 1408
SPLIT = 2
RB = 32


def _front(x_hbm, wg_hbm, wu_hbm, wd_hbm, gy_hbm,
           y_ref, xc_out, gc, h, da, db, p_out,
           x_v, gy_v, wg, wu, wd, xc,
           pa, pb, pg, ra, rb, rg, sd,
           yp, s1, r1, s2, r2, sc, rc, yk, dxp,
           w_sem, o_sem, xs, xrs, gs, grs, es, ers, ys, yrs):
    rows, d_full = x_v.shape
    tok, d_half = xc.shape
    half = tok // 2
    nf = wg.shape[1] // FC
    nd = d_half // DC
    t = lax.axis_index("tp")
    c = lax.axis_index("dp")
    ty, tx = t // 2, t % 2
    tx_n = ty * 2 + 1 - tx
    ty_n = (1 - ty) * 2 + tx
    t_d = 3 - t
    t1 = (1 - c) * tx_n + c * ty_n
    t2 = (1 - c) * ty_n + c * tx_n
    order = ((t_d, c), (t_d, 1 - c), (tx_n, c), (tx_n, 1 - c), (ty_n, c), (ty_n, 1 - c), (t, 1 - c))

    def rows_of(q, chip):
        return pl.ds(pl.multiple_of((q * 4 + chip) * rows, rows), rows)

    def cols_of(q):
        return pl.ds(pl.multiple_of(q * d_half, d_half), d_half)

    cx = pltpu.make_async_copy(x_hbm, x_v, w_sem.at[0])
    cg = pltpu.make_async_copy(gy_hbm, gy_v, w_sem.at[1])
    cw = [pltpu.make_async_copy(a, b, w_sem.at[2 + i])
          for i, (a, b) in enumerate(((wg_hbm, wg), (wu_hbm, wu), (wd_hbm, wd)))]
    cx.start()
    cg.start()
    for w in cw:
        w.start()

    barrier = pltpu.get_barrier_semaphore()
    for chip, q in order:
        pl.semaphore_signal(barrier, inc=1, device_id={"tp": chip, "dp": q}, device_id_type=MESH)
    pl.semaphore_wait(barrier, 7)

    def remote(src, dst, ssem, rsem, chip, q):
        cp = pltpu.make_async_remote_copy(src_ref=src, dst_ref=dst, send_sem=ssem, recv_sem=rsem,
                                          device_id={"tp": chip, "dp": q}, device_id_type=MESH)
        cp.start()
        return cp

    def swap(src, dst, i):
        return remote(src, dst, es.at[i], ers.at[i], t, 1 - c)

    def spread(own, cols, ssem, rsem):
        return [remote(own.at[:, cols_of(q)], cols.at[rows_of(c, t), :], ssem.at[k], rsem.at[k], chip, q)
                for k, (chip, q) in enumerate(order)]

    cx.wait()
    sx = spread(x_v, xc, xs, xrs)
    xc[rows_of(c, t), :] = x_v[:, cols_of(c)]
    cg.wait()
    for cp in sx:
        cp.wait_send()
    sg = spread(gy_v, gc, gs, grs)
    gc[rows_of(c, t), :] = gy_v[:, cols_of(c)]

    mine = pl.multiple_of(c * half, half)
    theirs = pl.ds(pl.multiple_of((1 - c) * half, half), half)
    cw[0].wait()
    cw[1].wait()
    for cp in sx:
        cp.wait_recv()
    out_x = pltpu.make_async_copy(xc, xc_out, o_sem.at[0])
    out_x.start()
    cps = {}

    def swap_part(part, got, j, i):
        if j < SPLIT:
            return swap(part.at[j, theirs, :], got.at[j, pl.ds(0, half), :], i)
        return swap(part.at[j], got.at[j], i)

    for j in range(nf):
        f = slice(j * FC, (j + 1) * FC)
        pa[j] = jnp.dot(xc[...], wg[:, f], preferred_element_type=F32)
        cps["a", j] = swap_part(pa, ra, j, 6 * j)
        pb[j] = jnp.dot(xc[...], wu[:, f], preferred_element_type=F32)
        cps["b", j] = swap_part(pb, rb, j, 6 * j + 1)

    def blocks(j):
        for i in range(0, half if j < SPLIT else tok, RB):
            yield pl.ds(pl.multiple_of(mine + i, RB), RB) if j < SPLIT else slice(i, i + RB), slice(i, i + RB)

    for j in range(nf):
        f = slice(j * FC, (j + 1) * FC)
        cps["a", j].wait_recv()
        cps["b", j].wait_recv()
        for r, i in blocks(j):
            a = pa[j, r, :] + ra[j, i, :]
            b = pb[j, r, :] + rb[j, i, :]
            s = jax.nn.sigmoid(a)
            u = a * s
            h[r, f] = (u * b).astype(BF16)
            sd[j, i, :] = s * (1.0 + a * (1.0 - s))
            ra[j, i, :] = u
            rb[j, i, :] = b
        if j < SPLIT:
            own = h.at[pl.ds(mine, half), f]
            cps["h", j] = swap(own, own, 6 * j + 3)
    def y_part(n, pieces):
        o = slice(n * DC, (n + 1) * DC)
        yp[:, o] = jnp.dot(h[...], wd[:, o], preferred_element_type=F32)
        for p in pieces:
            o = slice(PIECES[p][0], sum(PIECES[p]))
            for q in range(2):
                for e, chip in enumerate((t1, t_d)):
                    s1[p][(q * 2 + e) * rows:(q * 2 + e + 1) * rows, :] = yp[rows_of(q, chip), o]
            cps["1", p] = remote(s1[p], r1[p], ys.at[4 * p], yrs.at[4 * p], t1, c)

    def y_step(p):
        o = slice(PIECES[p][0], sum(PIECES[p]))
        cps["1", p].wait_recv()

        def got(q, e):
            return r1[p][pl.ds(pl.multiple_of((q * 2 + e) * rows, rows), rows), :]

        s2[p][0] = yp[rows_of(c, t2), o] + got(c, 1)
        s2[p][1] = yp[rows_of(1 - c, t2), o] + got(1 - c, 1)
        cps["2", p] = remote(s2[p].at[0], r2[p].at[0], ys.at[4 * p + 1], yrs.at[4 * p + 1], t2, c)
        cps["3", p] = remote(s2[p].at[1], r2[p].at[1], ys.at[4 * p + 2], yrs.at[4 * p + 2], t2, 1 - c)
        sc[p][...] = yp[rows_of(1 - c, t), o] + got(1 - c, 0)
        cps["4", p] = remote(sc[p], rc[p], ys.at[4 * p + 3], yrs.at[4 * p + 3], t, 1 - c)
        yk[p][...] = yp[rows_of(c, t), o] + got(c, 0)

    def y_done(p):
        for k in "234":
            cps[k, p].wait_recv()
        o, w = PIECES[p]
        for q, tot in ((c, yk[p][...] + r2[p][0]), (1 - c, rc[p][...] + r2[p][1])):
            cols = pl.ds(pl.multiple_of(q * d_half + o, 128), w)
            y_ref[:, cols] = (x_v[:, cols].astype(F32) + tot).astype(BF16)

    def g_part(j):
        pg[j] = lax.dot_general(gc[...], wd[j * FC:(j + 1) * FC, :], NT, preferred_element_type=F32)
        cps["g", j] = swap_part(pg, rg, j, 6 * j + 2)

    def grad(j):
        f = slice(j * FC, (j + 1) * FC)
        cps["g", j].wait_recv()
        for r, i in blocks(j):
            g = pg[j, r, :] + rg[j, i, :]
            da[r, f] = (g * rb[j, i, :] * sd[j, i, :]).astype(BF16)
            db[r, f] = (g * ra[j, i, :]).astype(BF16)
        if j < SPLIT:
            own = da.at[pl.ds(mine, half), f]
            cps["da", j] = swap(own, own, 6 * j + 4)
            own = db.at[pl.ds(mine, half), f]
            cps["db", j] = swap(own, own, 6 * j + 5)

    def dx_part(j):
        f = slice(j * FC, (j + 1) * FC)
        if j < SPLIT:
            cps["da", j].wait_recv()
            cps["db", j].wait_recv()
        for n in range(nd):
            o = slice(n * DC, (n + 1) * DC)
            part = (lax.dot_general(da[:, f], wg[o, f], NT, preferred_element_type=F32)
                    + lax.dot_general(db[:, f], wu[o, f], NT, preferred_element_type=F32))
            dxp[:, o] = part if j == 0 else dxp[:, o] + part

    cw[2].wait()
    for j in range(SPLIT):
        cps["h", j].wait_recv()
    y_part(0, (0,))
    y_part(1, (1,))
    y_part(2, (2, 3))
    for cp in sg:
        cp.wait_recv()
    g_part(0)
    g_part(1)
    g_part(2)
    grad(0)
    g_part(3)
    grad(1)
    y_step(0)
    dx_part(0)
    grad(2)
    y_step(1)
    grad(3)
    y_step(2)
    y_step(3)
    dx_part(1)
    dx_part(2)
    dx_part(3)

    for i in range(8):
        r = ((i % 2) * 4 + i // 2) * rows
        p_out[i, :, :d_half] = dxp[r:r + rows, :]
        p_out[i, :, d_half:] = yp[r:r + rows, FRONT:]
    for q in range(2):
        p_out[t * 2 + q, :, :d_half] += gc[rows_of(q, t), :].astype(F32)
        p_out[t * 2 + q, :, d_half:] += xc[rows_of(q, t), FRONT:].astype(F32)
    for p in range(len(PIECES)):
        y_done(p)

    for cp in sg:
        cp.wait_send()
    for cp in cps.values():
        cp.wait_send()
    out_x.wait()


def _finish(y_in, p, y_ref, dx_ref):
    d_half = y_ref.shape[1] // 2
    for q in range(2):
        o = q * d_half
        tot = (p[q] + p[q + 2] + p[q + 4] + p[q + 6]).astype(BF16)
        dx_ref[:, o:o + d_half] = tot[:, :d_half]
        y_ref[:, o:o + FRONT] = y_in[:, o:o + FRONT]
        y_ref[:, o + FRONT:o + d_half] = tot[:, d_half:]


def _grads(h, da, db, xc_hbm, gc, dwd_hbm, dwg_hbm, dwu_hbm, buf_d, buf_g, xc, sem_d, sem_g, sem_x):
    ff = h.shape[1]
    d_half = xc.shape[1]
    nb_d, tr_d = buf_d.shape[:2]
    nb_g, tr_g = buf_g.shape[:2]
    cx = pltpu.make_async_copy(xc_hbm, xc, sem_x)
    cx.start()

    def run(lhs, rhs, out, buf, sem, n, tr, nb, start, prev_out):
        def step(i, carry):
            slot = lax.rem(i + start, nb)
            r = pl.multiple_of(i * tr, tr)

            def drain():
                pltpu.make_async_copy(buf.at[slot], prev_out.at[pl.ds(0, tr), :], sem.at[slot]).wait()

            if start >= nb:
                drain()
            else:
                pl.when(i + start >= nb)(drain)
            buf[slot] = lax.dot_general(lhs[:, pl.ds(r, tr)], rhs[...], TN, preferred_element_type=F32)
            pltpu.make_async_copy(buf.at[slot], out.at[pl.ds(r, tr), :], sem.at[slot]).start()
            return carry

        lax.fori_loop(0, n, step, 0)

    n_d = ff // tr_d
    n_g = d_half // tr_g
    run(h, gc, dwd_hbm, buf_d, sem_d, n_d, tr_d, nb_d, 0, dwd_hbm)
    cx.wait()
    run(xc, da, dwg_hbm, buf_g, sem_g, n_g, tr_g, nb_g, 0, dwg_hbm)
    run(xc, db, dwu_hbm, buf_g, sem_g, n_g, tr_g, nb_g, n_g, dwu_hbm)
    for s in range(nb_d):
        pltpu.make_async_copy(buf_d.at[s], dwd_hbm.at[pl.ds(0, tr_d), :], sem_d.at[s]).wait()
    for s in range(nb_g):
        pltpu.make_async_copy(buf_g.at[s], dwu_hbm.at[pl.ds(0, tr_g), :], sem_g.at[s]).wait()


def solution(mesh):
    def local_step(x, wg, wu, wd, gy):
        rows, d_full = x.shape
        d_half, ff = wg.shape
        tok = rows * 8
        nf = ff // FC
        nd = d_half // DC
        any_ = pl.BlockSpec(memory_space=pl.ANY)
        hbm = pl.BlockSpec(memory_space=pltpu.HBM)
        vm = pl.BlockSpec(memory_space=pltpu.VMEM)
        S = jax.ShapeDtypeStruct
        dma = pltpu.SemaphoreType.DMA
        full = pltpu.VMEM((nf, tok, FC), F32)
        y, xc, gc, h, da, db, parts = pl.pallas_call(
            _front,
            name="front",
            out_shape=(S((rows, d_full), BF16),
                       pltpu.HBM((tok, d_half), BF16), S((tok, d_half), BF16),
                       S((tok, ff), BF16), S((tok, ff), BF16), S((tok, ff), BF16))
            + (S((8, rows, 2 * d_half - FRONT), F32),),
            in_specs=[hbm] * 5,
            out_specs=(vm, hbm, vm, vm, vm, vm, vm),
            scratch_shapes=[
                pltpu.VMEM((rows, d_full), BF16), pltpu.VMEM((rows, d_full), BF16),
                pltpu.VMEM((d_half, ff), BF16), pltpu.VMEM((d_half, ff), BF16), pltpu.VMEM((ff, d_half), BF16),
                pltpu.VMEM((tok, d_half), BF16),
                full, full, full, full, full, full, full,
                pltpu.VMEM((tok, d_half), F32),
                [pltpu.VMEM((4 * rows, w), F32) for _, w in PIECES], [pltpu.VMEM((4 * rows, w), F32) for _, w in PIECES],
                [pltpu.VMEM((2, rows, w), F32) for _, w in PIECES], [pltpu.VMEM((2, rows, w), F32) for _, w in PIECES],
                *([pltpu.VMEM((rows, w), F32) for _, w in PIECES] for _ in range(3)),
                pltpu.VMEM((tok, d_half), F32),
                dma((5,)), dma((1,)), dma((7,)), dma((7,)), dma((7,)), dma((7,)),
                dma((6 * nf,)), dma((6 * nf,)), dma((4 * len(PIECES),)), dma((4 * len(PIECES),)),
            ],
            compiler_params=pltpu.CompilerParams(collective_id=0, has_side_effects=True,
                                                 vmem_limit_bytes=50 * 1024 * 1024),
        )(*(pltpu.with_memory_space_constraint(v, pltpu.HBM) for v in (x, wg, wu, wd, gy)))
        parts = lax.all_to_all(parts, ("tp", "dp"), 0, 0, tiled=True)

        tr = 256
        dwd, dwg, dwu = pl.pallas_call(
            _grads,
            name="grads",
            out_shape=(S((ff, d_half), F32), S((d_half, ff), F32), S((d_half, ff), F32)),
            in_specs=[vm, vm, vm, hbm, vm],
            out_specs=(any_, any_, any_),
            scratch_shapes=[pltpu.VMEM((8, tr, d_half), F32), pltpu.VMEM((6, tr, ff), F32),
                            pltpu.VMEM((tok, d_half), BF16), dma((8,)), dma((6,)), dma(())],
            cost_estimate=pl.CostEstimate(flops=6 * tok * d_half * ff, bytes_accessed=12 * d_half * ff,
                                          transcendentals=0),
            compiler_params=pltpu.CompilerParams(vmem_limit_bytes=34 * 1024 * 1024),
        )(h, da, db, pltpu.with_memory_space_constraint(xc, pltpu.HBM), gc)
        y, dx = pl.pallas_call(
            _finish,
            name="finish",
            out_shape=(S((rows, d_full), BF16), S((rows, d_full), BF16)),
            in_specs=[vm] * 2,
            out_specs=(vm, vm),
            compiler_params=pltpu.CompilerParams(vmem_limit_bytes=6 * 1024 * 1024),
        )(y, parts)
        return y, dx, dwg, dwu, dwd

    row_spec = P(("dp", "tp"), None)
    up_spec = P("dp", "tp")
    down_spec = P("tp", "dp")
    return jax.shard_map(local_step, mesh=mesh,
                         in_specs=(row_spec, up_spec, up_spec, down_spec, row_spec),
                         out_specs=(row_spec, row_spec, up_spec, up_spec, down_spec),
                         check_vma=False)
```

```python
import functools

import jax
import jax.numpy as jnp
from jax import lax
from jax.experimental import pallas as pl
from jax.experimental.pallas import tpu as pltpu
from jax.sharding import PartitionSpec as P

MESH = pl.DeviceIdType.MESH
F32 = jnp.float32
BF16 = jnp.bfloat16

NT = (((1,), (1,)), ((), ()))
TN = (((0,), (0,)), ((), ()))

FC = 512
DC = 512
PIECES = ((0, 512), (512, 512), (1024, 256), (1280, 256))
FRONT = 1536
SPLIT = 2
RB = 32


def _front(x_hbm, wg_hbm, wu_hbm, wd_hbm, gy_hbm,
           y_ref, xc_out, gc, h, da, db, p_out,
           x_v, gy_v, wg, wu, wd, xc,
           pa, pb, pg, ra, rb, rg, sd,
           yp, s1, r1, s2, r2, sc, rc, yk, dxp,
           w_sem, o_sem, xs, xrs, gs, grs, es, ers, ys, yrs):
    rows, d_full = x_v.shape
    tok, d_half = xc.shape
    half = tok // 2
    nf = wg.shape[1] // FC
    nd = d_half // DC
    t = lax.axis_index("tp")
    c = lax.axis_index("dp")
    ty, tx = t // 2, t % 2
    tx_n = ty * 2 + 1 - tx
    ty_n = (1 - ty) * 2 + tx
    t_d = 3 - t
    t1 = (1 - c) * tx_n + c * ty_n
    t2 = (1 - c) * ty_n + c * tx_n
    order = ((t_d, c), (t_d, 1 - c), (tx_n, c), (tx_n, 1 - c), (ty_n, c), (ty_n, 1 - c), (t, 1 - c))

    def rows_of(q, chip):
        return pl.ds(pl.multiple_of((q * 4 + chip) * rows, rows), rows)

    def cols_of(q):
        return pl.ds(pl.multiple_of(q * d_half, d_half), d_half)

    cx = pltpu.make_async_copy(x_hbm, x_v, w_sem.at[0])
    cg = pltpu.make_async_copy(gy_hbm, gy_v, w_sem.at[1])
    cw = [pltpu.make_async_copy(a, b, w_sem.at[2 + i])
          for i, (a, b) in enumerate(((wg_hbm, wg), (wu_hbm, wu), (wd_hbm, wd)))]
    cx.start()
    cg.start()
    for w in cw:
        w.start()

    barrier = pltpu.get_barrier_semaphore()
    for chip, q in order:
        pl.semaphore_signal(barrier, inc=1, device_id={"tp": chip, "dp": q}, device_id_type=MESH)
    pl.semaphore_wait(barrier, 7)

    def remote(src, dst, ssem, rsem, chip, q):
        cp = pltpu.make_async_remote_copy(src_ref=src, dst_ref=dst, send_sem=ssem, recv_sem=rsem,
                                          device_id={"tp": chip, "dp": q}, device_id_type=MESH)
        cp.start()
        return cp

    def swap(src, dst, i):
        return remote(src, dst, es.at[i], ers.at[i], t, 1 - c)

    def spread(own, cols, ssem, rsem):
        return [remote(own.at[:, cols_of(q)], cols.at[rows_of(c, t), :], ssem.at[k], rsem.at[k], chip, q)
                for k, (chip, q) in enumerate(order)]

    cx.wait()
    sx = spread(x_v, xc, xs, xrs)
    xc[rows_of(c, t), :] = x_v[:, cols_of(c)]
    cg.wait()
    for cp in sx:
        cp.wait_send()
    sg = spread(gy_v, gc, gs, grs)
    gc[rows_of(c, t), :] = gy_v[:, cols_of(c)]

    mine = pl.multiple_of(c * half, half)
    theirs = pl.ds(pl.multiple_of((1 - c) * half, half), half)
    cw[0].wait()
    cw[1].wait()
    for cp in sx:
        cp.wait_recv()
    out_x = pltpu.make_async_copy(xc, xc_out, o_sem.at[0])
    out_x.start()
    cps = {}

    def swap_part(part, got, j, i):
        if j < SPLIT:
            return swap(part.at[j, theirs, :], got.at[j, pl.ds(0, half), :], i)
        return swap(part.at[j], got.at[j], i)

    for j in range(nf):
        f = slice(j * FC, (j + 1) * FC)
        pa[j] = jnp.dot(xc[...], wg[:, f], preferred_element_type=F32)
        cps["a", j] = swap_part(pa, ra, j, 6 * j)
        pb[j] = jnp.dot(xc[...], wu[:, f], preferred_element_type=F32)
        cps["b", j] = swap_part(pb, rb, j, 6 * j + 1)

    def blocks(j):
        for i in range(0, half if j < SPLIT else tok, RB):
            yield pl.ds(pl.multiple_of(mine + i, RB), RB) if j < SPLIT else slice(i, i + RB), slice(i, i + RB)

    for j in range(nf):
        f = slice(j * FC, (j + 1) * FC)
        cps["a", j].wait_recv()
        cps["b", j].wait_recv()
        for r, i in blocks(j):
            a = pa[j, r, :] + ra[j, i, :]
            b = pb[j, r, :] + rb[j, i, :]
            s = jax.nn.sigmoid(a)
            u = a * s
            h[r, f] = (u * b).astype(BF16)
            sd[j, i, :] = s * (1.0 + a * (1.0 - s))
            ra[j, i, :] = u
            rb[j, i, :] = b
        if j < SPLIT:
            own = h.at[pl.ds(mine, half), f]
            cps["h", j] = swap(own, own, 6 * j + 3)
    def y_part(n, pieces):
        o = slice(n * DC, (n + 1) * DC)
        yp[:, o] = jnp.dot(h[...], wd[:, o], preferred_element_type=F32)
        for p in pieces:
            o = slice(PIECES[p][0], sum(PIECES[p]))
            for q in range(2):
                for e, chip in enumerate((t1, t_d)):
                    s1[p][(q * 2 + e) * rows:(q * 2 + e + 1) * rows, :] = yp[rows_of(q, chip), o]
            cps["1", p] = remote(s1[p], r1[p], ys.at[4 * p], yrs.at[4 * p], t1, c)

    def y_step(p):
        o = slice(PIECES[p][0], sum(PIECES[p]))
        cps["1", p].wait_recv()

        def got(q, e):
            return r1[p][pl.ds(pl.multiple_of((q * 2 + e) * rows, rows), rows), :]

        s2[p][0] = yp[rows_of(c, t2), o] + got(c, 1)
        s2[p][1] = yp[rows_of(1 - c, t2), o] + got(1 - c, 1)
        cps["2", p] = remote(s2[p].at[0], r2[p].at[0], ys.at[4 * p + 1], yrs.at[4 * p + 1], t2, c)
        cps["3", p] = remote(s2[p].at[1], r2[p].at[1], ys.at[4 * p + 2], yrs.at[4 * p + 2], t2, 1 - c)
        sc[p][...] = yp[rows_of(1 - c, t), o] + got(1 - c, 0)
        cps["4", p] = remote(sc[p], rc[p], ys.at[4 * p + 3], yrs.at[4 * p + 3], t, 1 - c)
        yk[p][...] = yp[rows_of(c, t), o] + got(c, 0)

    def y_done(p):
        for k in "234":
            cps[k, p].wait_recv()
        o, w = PIECES[p]
        for q, tot in ((c, yk[p][...] + r2[p][0]), (1 - c, rc[p][...] + r2[p][1])):
            cols = pl.ds(pl.multiple_of(q * d_half + o, 128), w)
            y_ref[:, cols] = (x_v[:, cols].astype(F32) + tot).astype(BF16)

    def g_part(j):
        pg[j] = lax.dot_general(gc[...], wd[j * FC:(j + 1) * FC, :], NT, preferred_element_type=F32)
        cps["g", j] = swap_part(pg, rg, j, 6 * j + 2)

    def grad(j):
        f = slice(j * FC, (j + 1) * FC)
        cps["g", j].wait_recv()
        for r, i in blocks(j):
            g = pg[j, r, :] + rg[j, i, :]
            da[r, f] = (g * rb[j, i, :] * sd[j, i, :]).astype(BF16)
            db[r, f] = (g * ra[j, i, :]).astype(BF16)
        if j < SPLIT:
            own = da.at[pl.ds(mine, half), f]
            cps["da", j] = swap(own, own, 6 * j + 4)
            own = db.at[pl.ds(mine, half), f]
            cps["db", j] = swap(own, own, 6 * j + 5)

    def dx_part(j):
        f = slice(j * FC, (j + 1) * FC)
        if j < SPLIT:
            cps["da", j].wait_recv()
            cps["db", j].wait_recv()
        for n in range(nd):
            o = slice(n * DC, (n + 1) * DC)
            part = (lax.dot_general(da[:, f], wg[o, f], NT, preferred_element_type=F32)
                    + lax.dot_general(db[:, f], wu[o, f], NT, preferred_element_type=F32))
            dxp[:, o] = part if j == 0 else dxp[:, o] + part

    cw[2].wait()
    for j in range(SPLIT):
        cps["h", j].wait_recv()
    y_part(0, (0,))
    y_part(1, (1,))
    y_part(2, (2, 3))
    for cp in sg:
        cp.wait_recv()
    g_part(0)
    g_part(1)
    g_part(2)
    grad(0)
    g_part(3)
    grad(1)
    y_step(0)
    dx_part(0)
    grad(2)
    y_step(1)
    dx_part(1)
    grad(3)
    y_step(2)
    y_step(3)
    dx_part(2)
    dx_part(3)

    for i in range(8):
        r = ((i % 2) * 4 + i // 2) * rows
        p_out[i, :, :d_half] = dxp[r:r + rows, :]
        if FRONT < d_half:
            p_out[i, :, d_half:] = yp[r:r + rows, FRONT:]
    for q in range(2):
        p_out[t * 2 + q, :, :d_half] += gc[rows_of(q, t), :].astype(F32)
        if FRONT < d_half:
            p_out[t * 2 + q, :, d_half:] += xc[rows_of(q, t), FRONT:].astype(F32)
    for p in range(len(PIECES)):
        y_done(p)

    for cp in sg:
        cp.wait_send()
    for cp in cps.values():
        cp.wait_send()
    out_x.wait()


def _finish(y_in, p, y_ref, dx_ref):
    d_half = y_ref.shape[1] // 2
    for q in range(2):
        o = q * d_half
        tot = (p[q] + p[q + 2] + p[q + 4] + p[q + 6]).astype(BF16)
        dx_ref[:, o:o + d_half] = tot[:, :d_half]
        y_ref[:, o:o + FRONT] = y_in[:, o:o + FRONT]
        if FRONT < d_half:
            y_ref[:, o + FRONT:o + d_half] = tot[:, d_half:]


def _grads(h, da, db, xc_hbm, gc, dwd_hbm, dwg_hbm, dwu_hbm, buf_d, buf_g, xc, sem_d, sem_g, sem_x):
    ff = h.shape[1]
    d_half = xc.shape[1]
    nb_d, tr_d = buf_d.shape[:2]
    nb_g, tr_g = buf_g.shape[:2]
    cx = pltpu.make_async_copy(xc_hbm, xc, sem_x)
    cx.start()

    def run(lhs, rhs, out, buf, sem, n, tr, nb, start, prev_out):
        def step(i, carry):
            slot = lax.rem(i + start, nb)
            r = pl.multiple_of(i * tr, tr)

            def drain():
                pltpu.make_async_copy(buf.at[slot], prev_out.at[pl.ds(0, tr), :], sem.at[slot]).wait()

            if start >= nb:
                drain()
            else:
                pl.when(i + start >= nb)(drain)
            buf[slot] = lax.dot_general(lhs[:, pl.ds(r, tr)], rhs[...], TN, preferred_element_type=F32)
            pltpu.make_async_copy(buf.at[slot], out.at[pl.ds(r, tr), :], sem.at[slot]).start()
            return carry

        lax.fori_loop(0, n, step, 0)

    n_d = ff // tr_d
    n_g = d_half // tr_g
    run(h, gc, dwd_hbm, buf_d, sem_d, n_d, tr_d, nb_d, 0, dwd_hbm)
    cx.wait()
    run(xc, da, dwg_hbm, buf_g, sem_g, n_g, tr_g, nb_g, 0, dwg_hbm)
    run(xc, db, dwu_hbm, buf_g, sem_g, n_g, tr_g, nb_g, n_g, dwu_hbm)
    for s in range(nb_d):
        pltpu.make_async_copy(buf_d.at[s], dwd_hbm.at[pl.ds(0, tr_d), :], sem_d.at[s]).wait()
    for s in range(nb_g):
        pltpu.make_async_copy(buf_g.at[s], dwu_hbm.at[pl.ds(0, tr_g), :], sem_g.at[s]).wait()


def solution(mesh):
    def local_step(x, wg, wu, wd, gy):
        rows, d_full = x.shape
        d_half, ff = wg.shape
        tok = rows * 8
        nf = ff // FC
        nd = d_half // DC
        any_ = pl.BlockSpec(memory_space=pl.ANY)
        hbm = pl.BlockSpec(memory_space=pltpu.HBM)
        vm = pl.BlockSpec(memory_space=pltpu.VMEM)
        S = jax.ShapeDtypeStruct
        dma = pltpu.SemaphoreType.DMA
        full = pltpu.VMEM((nf, tok, FC), F32)
        y, xc, gc, h, da, db, parts = pl.pallas_call(
            _front,
            name="front",
            out_shape=(S((rows, d_full), BF16),
                       pltpu.HBM((tok, d_half), BF16), S((tok, d_half), BF16),
                       S((tok, ff), BF16), S((tok, ff), BF16), S((tok, ff), BF16))
            + (S((8, rows, 2 * d_half - FRONT), F32),),
            in_specs=[hbm] * 5,
            out_specs=(vm, hbm, vm, vm, vm, vm, vm),
            scratch_shapes=[
                pltpu.VMEM((rows, d_full), BF16), pltpu.VMEM((rows, d_full), BF16),
                pltpu.VMEM((d_half, ff), BF16), pltpu.VMEM((d_half, ff), BF16), pltpu.VMEM((ff, d_half), BF16),
                pltpu.VMEM((tok, d_half), BF16),
                full, full, full, full, full, full, full,
                pltpu.VMEM((tok, d_half), F32),
                [pltpu.VMEM((4 * rows, w), F32) for _, w in PIECES], [pltpu.VMEM((4 * rows, w), F32) for _, w in PIECES],
                [pltpu.VMEM((2, rows, w), F32) for _, w in PIECES], [pltpu.VMEM((2, rows, w), F32) for _, w in PIECES],
                *([pltpu.VMEM((rows, w), F32) for _, w in PIECES] for _ in range(3)),
                pltpu.VMEM((tok, d_half), F32),
                dma((5,)), dma((1,)), dma((7,)), dma((7,)), dma((7,)), dma((7,)),
                dma((6 * nf,)), dma((6 * nf,)), dma((4 * len(PIECES),)), dma((4 * len(PIECES),)),
            ],
            compiler_params=pltpu.CompilerParams(collective_id=0, has_side_effects=True,
                                                 vmem_limit_bytes=50 * 1024 * 1024),
        )(*(pltpu.with_memory_space_constraint(v, pltpu.HBM) for v in (x, wg, wu, wd, gy)))
        parts = lax.all_to_all(parts, ("tp", "dp"), 0, 0, tiled=True)

        tr = 256
        dwd, dwg, dwu = pl.pallas_call(
            _grads,
            name="grads",
            out_shape=(S((ff, d_half), F32), S((d_half, ff), F32), S((d_half, ff), F32)),
            in_specs=[vm, vm, vm, hbm, vm],
            out_specs=(any_, any_, any_),
            scratch_shapes=[pltpu.VMEM((8, tr, d_half), F32), pltpu.VMEM((6, tr, ff), F32),
                            pltpu.VMEM((tok, d_half), BF16), dma((8,)), dma((6,)), dma(())],
            cost_estimate=pl.CostEstimate(flops=6 * tok * d_half * ff, bytes_accessed=12 * d_half * ff,
                                          transcendentals=0),
            compiler_params=pltpu.CompilerParams(vmem_limit_bytes=34 * 1024 * 1024),
        )(h, da, db, pltpu.with_memory_space_constraint(xc, pltpu.HBM), gc)
        y, dx = pl.pallas_call(
            _finish,
            name="finish",
            out_shape=(S((rows, d_full), BF16), S((rows, d_full), BF16)),
            in_specs=[vm] * 2,
            out_specs=(vm, vm),
            compiler_params=pltpu.CompilerParams(vmem_limit_bytes=6 * 1024 * 1024),
        )(y, parts)
        return y, dx, dwg, dwu, dwd

    row_spec = P(("dp", "tp"), None)
    up_spec = P("dp", "tp")
    down_spec = P("tp", "dp")
    return jax.shard_map(local_step, mesh=mesh,
                         in_specs=(row_spec, up_spec, up_spec, down_spec, row_spec),
                         out_specs=(row_spec, row_spec, up_spec, up_spec, down_spec),
                         check_vma=False)
```

```python
import functools

import jax
import jax.numpy as jnp
from jax import lax
from jax.experimental import pallas as pl
from jax.experimental.pallas import tpu as pltpu
from jax.sharding import PartitionSpec as P

MESH = pl.DeviceIdType.MESH
F32 = jnp.float32
BF16 = jnp.bfloat16

NT = (((1,), (1,)), ((), ()))
TN = (((0,), (0,)), ((), ()))

FC = 512
DC = 512
PIECES = ((0, 512), (512, 512), (1024, 384), (1408, 128))
FRONT = 1536
SPLIT = 1
RB = 32


def _front(x_hbm, wg_hbm, wu_hbm, wd_hbm, gy_hbm,
           y_ref, xc_out, gc, h, da, db, p_out,
           x_v, gy_v, wg, wu, wd, xc,
           pa, pb, pg, ra, rb, rg, sd,
           yp, s1, r1, s2, r2, sc, rc, yk, dxp,
           w_sem, o_sem, xs, xrs, gs, grs, es, ers, ys, yrs):
    rows, d_full = x_v.shape
    tok, d_half = xc.shape
    half = tok // 2
    nf = wg.shape[1] // FC
    nd = d_half // DC
    t = lax.axis_index("tp")
    c = lax.axis_index("dp")
    ty, tx = t // 2, t % 2
    tx_n = ty * 2 + 1 - tx
    ty_n = (1 - ty) * 2 + tx
    t_d = 3 - t
    t1 = (1 - c) * tx_n + c * ty_n
    t2 = (1 - c) * ty_n + c * tx_n
    order = ((t_d, c), (t_d, 1 - c), (tx_n, c), (tx_n, 1 - c), (ty_n, c), (ty_n, 1 - c), (t, 1 - c))

    def rows_of(q, chip):
        return pl.ds(pl.multiple_of((q * 4 + chip) * rows, rows), rows)

    def cols_of(q):
        return pl.ds(pl.multiple_of(q * d_half, d_half), d_half)

    cx = pltpu.make_async_copy(x_hbm, x_v, w_sem.at[0])
    cg = pltpu.make_async_copy(gy_hbm, gy_v, w_sem.at[1])
    cw = [pltpu.make_async_copy(a, b, w_sem.at[2 + i])
          for i, (a, b) in enumerate(((wg_hbm, wg), (wu_hbm, wu), (wd_hbm, wd)))]
    cx.start()
    cg.start()
    for w in cw:
        w.start()

    barrier = pltpu.get_barrier_semaphore()
    for chip, q in order:
        pl.semaphore_signal(barrier, inc=1, device_id={"tp": chip, "dp": q}, device_id_type=MESH)
    pl.semaphore_wait(barrier, 7)

    def remote(src, dst, ssem, rsem, chip, q):
        cp = pltpu.make_async_remote_copy(src_ref=src, dst_ref=dst, send_sem=ssem, recv_sem=rsem,
                                          device_id={"tp": chip, "dp": q}, device_id_type=MESH)
        cp.start()
        return cp

    def swap(src, dst, i):
        return remote(src, dst, es.at[i], ers.at[i], t, 1 - c)

    def spread(own, cols, ssem, rsem):
        return [remote(own.at[:, cols_of(q)], cols.at[rows_of(c, t), :], ssem.at[k], rsem.at[k], chip, q)
                for k, (chip, q) in enumerate(order)]

    cx.wait()
    sx = spread(x_v, xc, xs, xrs)
    xc[rows_of(c, t), :] = x_v[:, cols_of(c)]
    cg.wait()
    for cp in sx:
        cp.wait_send()
    sg = spread(gy_v, gc, gs, grs)
    gc[rows_of(c, t), :] = gy_v[:, cols_of(c)]

    mine = pl.multiple_of(c * half, half)
    theirs = pl.ds(pl.multiple_of((1 - c) * half, half), half)
    cw[0].wait()
    cw[1].wait()
    for cp in sx:
        cp.wait_recv()
    out_x = pltpu.make_async_copy(xc, xc_out, o_sem.at[0])
    out_x.start()
    cps = {}

    def swap_part(part, got, j, i):
        if j < SPLIT:
            return swap(part.at[j, theirs, :], got.at[j, pl.ds(0, half), :], i)
        return swap(part.at[j], got.at[j], i)

    for j in range(nf):
        f = slice(j * FC, (j + 1) * FC)
        pa[j] = jnp.dot(xc[...], wg[:, f], preferred_element_type=F32)
        cps["a", j] = swap_part(pa, ra, j, 6 * j)
        pb[j] = jnp.dot(xc[...], wu[:, f], preferred_element_type=F32)
        cps["b", j] = swap_part(pb, rb, j, 6 * j + 1)

    def blocks(j):
        for i in range(0, half if j < SPLIT else tok, RB):
            yield pl.ds(pl.multiple_of(mine + i, RB), RB) if j < SPLIT else slice(i, i + RB), slice(i, i + RB)

    for j in range(nf):
        f = slice(j * FC, (j + 1) * FC)
        cps["a", j].wait_recv()
        cps["b", j].wait_recv()
        for r, i in blocks(j):
            a = pa[j, r, :] + ra[j, i, :]
            b = pb[j, r, :] + rb[j, i, :]
            s = jax.nn.sigmoid(a)
            u = a * s
            h[r, f] = (u * b).astype(BF16)
            sd[j, i, :] = s * (1.0 + a * (1.0 - s))
            ra[j, i, :] = u
            rb[j, i, :] = b
        if j < SPLIT:
            own = h.at[pl.ds(mine, half), f]
            cps["h", j] = swap(own, own, 6 * j + 3)
    def y_part(n, pieces):
        o = slice(n * DC, (n + 1) * DC)
        yp[:, o] = jnp.dot(h[...], wd[:, o], preferred_element_type=F32)
        for p in pieces:
            o = slice(PIECES[p][0], sum(PIECES[p]))
            for q in range(2):
                for e, chip in enumerate((t1, t_d)):
                    s1[p][(q * 2 + e) * rows:(q * 2 + e + 1) * rows, :] = yp[rows_of(q, chip), o]
            cps["1", p] = remote(s1[p], r1[p], ys.at[4 * p], yrs.at[4 * p], t1, c)

    def y_step(p):
        o = slice(PIECES[p][0], sum(PIECES[p]))
        cps["1", p].wait_recv()

        def got(q, e):
            return r1[p][pl.ds(pl.multiple_of((q * 2 + e) * rows, rows), rows), :]

        s2[p][0] = yp[rows_of(c, t2), o] + got(c, 1)
        s2[p][1] = yp[rows_of(1 - c, t2), o] + got(1 - c, 1)
        cps["2", p] = remote(s2[p].at[0], r2[p].at[0], ys.at[4 * p + 1], yrs.at[4 * p + 1], t2, c)
        cps["3", p] = remote(s2[p].at[1], r2[p].at[1], ys.at[4 * p + 2], yrs.at[4 * p + 2], t2, 1 - c)
        sc[p][...] = yp[rows_of(1 - c, t), o] + got(1 - c, 0)
        cps["4", p] = remote(sc[p], rc[p], ys.at[4 * p + 3], yrs.at[4 * p + 3], t, 1 - c)
        yk[p][...] = yp[rows_of(c, t), o] + got(c, 0)

    def y_done(p):
        for k in "234":
            cps[k, p].wait_recv()
        o, w = PIECES[p]
        for q, tot in ((c, yk[p][...] + r2[p][0]), (1 - c, rc[p][...] + r2[p][1])):
            cols = pl.ds(pl.multiple_of(q * d_half + o, 128), w)
            y_ref[:, cols] = (x_v[:, cols].astype(F32) + tot).astype(BF16)

    def g_part(j):
        pg[j] = lax.dot_general(gc[...], wd[j * FC:(j + 1) * FC, :], NT, preferred_element_type=F32)
        cps["g", j] = swap_part(pg, rg, j, 6 * j + 2)

    def grad(j):
        f = slice(j * FC, (j + 1) * FC)
        cps["g", j].wait_recv()
        for r, i in blocks(j):
            g = pg[j, r, :] + rg[j, i, :]
            da[r, f] = (g * rb[j, i, :] * sd[j, i, :]).astype(BF16)
            db[r, f] = (g * ra[j, i, :]).astype(BF16)
        if j < SPLIT:
            own = da.at[pl.ds(mine, half), f]
            cps["da", j] = swap(own, own, 6 * j + 4)
            own = db.at[pl.ds(mine, half), f]
            cps["db", j] = swap(own, own, 6 * j + 5)

    def dx_part(j):
        f = slice(j * FC, (j + 1) * FC)
        if j < SPLIT:
            cps["da", j].wait_recv()
            cps["db", j].wait_recv()
        for n in range(nd):
            o = slice(n * DC, (n + 1) * DC)
            part = (lax.dot_general(da[:, f], wg[o, f], NT, preferred_element_type=F32)
                    + lax.dot_general(db[:, f], wu[o, f], NT, preferred_element_type=F32))
            dxp[:, o] = part if j == 0 else dxp[:, o] + part

    cw[2].wait()
    for j in range(SPLIT):
        cps["h", j].wait_recv()
    y_part(0, (0,))
    y_part(1, (1,))
    y_part(2, (2, 3))
    for cp in sg:
        cp.wait_recv()
    g_part(0)
    g_part(1)
    g_part(2)
    grad(0)
    g_part(3)
    grad(1)
    y_step(0)
    dx_part(0)
    grad(2)
    y_step(1)
    dx_part(1)
    grad(3)
    y_step(2)
    y_step(3)
    dx_part(2)
    dx_part(3)

    for i in range(8):
        r = ((i % 2) * 4 + i // 2) * rows
        p_out[i, :, :d_half] = dxp[r:r + rows, :]
        if FRONT < d_half:
            p_out[i, :, d_half:] = yp[r:r + rows, FRONT:]
    for q in range(2):
        p_out[t * 2 + q, :, :d_half] += gc[rows_of(q, t), :].astype(F32)
        if FRONT < d_half:
            p_out[t * 2 + q, :, d_half:] += xc[rows_of(q, t), FRONT:].astype(F32)
    for p in range(len(PIECES)):
        y_done(p)

    for cp in sg:
        cp.wait_send()
    for cp in cps.values():
        cp.wait_send()
    out_x.wait()


def _finish(y_in, p, y_ref, dx_ref):
    d_half = y_ref.shape[1] // 2
    for q in range(2):
        o = q * d_half
        tot = (p[q] + p[q + 2] + p[q + 4] + p[q + 6]).astype(BF16)
        dx_ref[:, o:o + d_half] = tot[:, :d_half]
        y_ref[:, o:o + FRONT] = y_in[:, o:o + FRONT]
        if FRONT < d_half:
            y_ref[:, o + FRONT:o + d_half] = tot[:, d_half:]


def _grads(h, da, db, xc_hbm, gc, dwd_hbm, dwg_hbm, dwu_hbm, buf_d, buf_g, xc, sem_d, sem_g, sem_x):
    ff = h.shape[1]
    d_half = xc.shape[1]
    nb_d, tr_d = buf_d.shape[:2]
    nb_g, tr_g = buf_g.shape[:2]
    cx = pltpu.make_async_copy(xc_hbm, xc, sem_x)
    cx.start()

    def run(lhs, rhs, out, buf, sem, n, tr, nb, start, prev_out):
        def step(i, carry):
            slot = lax.rem(i + start, nb)
            r = pl.multiple_of(i * tr, tr)

            def drain():
                pltpu.make_async_copy(buf.at[slot], prev_out.at[pl.ds(0, tr), :], sem.at[slot]).wait()

            if start >= nb:
                drain()
            else:
                pl.when(i + start >= nb)(drain)
            buf[slot] = lax.dot_general(lhs[:, pl.ds(r, tr)], rhs[...], TN, preferred_element_type=F32)
            pltpu.make_async_copy(buf.at[slot], out.at[pl.ds(r, tr), :], sem.at[slot]).start()
            return carry

        lax.fori_loop(0, n, step, 0)

    n_d = ff // tr_d
    n_g = d_half // tr_g
    run(h, gc, dwd_hbm, buf_d, sem_d, n_d, tr_d, nb_d, 0, dwd_hbm)
    cx.wait()
    run(xc, da, dwg_hbm, buf_g, sem_g, n_g, tr_g, nb_g, 0, dwg_hbm)
    run(xc, db, dwu_hbm, buf_g, sem_g, n_g, tr_g, nb_g, n_g, dwu_hbm)
    for s in range(nb_d):
        pltpu.make_async_copy(buf_d.at[s], dwd_hbm.at[pl.ds(0, tr_d), :], sem_d.at[s]).wait()
    for s in range(nb_g):
        pltpu.make_async_copy(buf_g.at[s], dwu_hbm.at[pl.ds(0, tr_g), :], sem_g.at[s]).wait()


def solution(mesh):
    def local_step(x, wg, wu, wd, gy):
        rows, d_full = x.shape
        d_half, ff = wg.shape
        tok = rows * 8
        nf = ff // FC
        nd = d_half // DC
        any_ = pl.BlockSpec(memory_space=pl.ANY)
        hbm = pl.BlockSpec(memory_space=pltpu.HBM)
        vm = pl.BlockSpec(memory_space=pltpu.VMEM)
        S = jax.ShapeDtypeStruct
        dma = pltpu.SemaphoreType.DMA
        full = pltpu.VMEM((nf, tok, FC), F32)
        y, xc, gc, h, da, db, parts = pl.pallas_call(
            _front,
            name="front",
            out_shape=(S((rows, d_full), BF16),
                       pltpu.HBM((tok, d_half), BF16), S((tok, d_half), BF16),
                       S((tok, ff), BF16), S((tok, ff), BF16), S((tok, ff), BF16))
            + (S((8, rows, 2 * d_half - FRONT), F32),),
            in_specs=[hbm] * 5,
            out_specs=(vm, hbm, vm, vm, vm, vm, vm),
            scratch_shapes=[
                pltpu.VMEM((rows, d_full), BF16), pltpu.VMEM((rows, d_full), BF16),
                pltpu.VMEM((d_half, ff), BF16), pltpu.VMEM((d_half, ff), BF16), pltpu.VMEM((ff, d_half), BF16),
                pltpu.VMEM((tok, d_half), BF16),
                full, full, full, full, full, full, full,
                pltpu.VMEM((tok, d_half), F32),
                [pltpu.VMEM((4 * rows, w), F32) for _, w in PIECES], [pltpu.VMEM((4 * rows, w), F32) for _, w in PIECES],
                [pltpu.VMEM((2, rows, w), F32) for _, w in PIECES], [pltpu.VMEM((2, rows, w), F32) for _, w in PIECES],
                *([pltpu.VMEM((rows, w), F32) for _, w in PIECES] for _ in range(3)),
                pltpu.VMEM((tok, d_half), F32),
                dma((5,)), dma((1,)), dma((7,)), dma((7,)), dma((7,)), dma((7,)),
                dma((6 * nf,)), dma((6 * nf,)), dma((4 * len(PIECES),)), dma((4 * len(PIECES),)),
            ],
            compiler_params=pltpu.CompilerParams(collective_id=0, has_side_effects=True,
                                                 vmem_limit_bytes=50 * 1024 * 1024),
        )(*(pltpu.with_memory_space_constraint(v, pltpu.HBM) for v in (x, wg, wu, wd, gy)))
        parts = lax.all_to_all(parts, ("tp", "dp"), 0, 0, tiled=True)

        tr = 256
        dwd, dwg, dwu = pl.pallas_call(
            _grads,
            name="grads",
            out_shape=(S((ff, d_half), F32), S((d_half, ff), F32), S((d_half, ff), F32)),
            in_specs=[vm, vm, vm, hbm, vm],
            out_specs=(any_, any_, any_),
            scratch_shapes=[pltpu.VMEM((8, tr, d_half), F32), pltpu.VMEM((6, tr, ff), F32),
                            pltpu.VMEM((tok, d_half), BF16), dma((8,)), dma((6,)), dma(())],
            cost_estimate=pl.CostEstimate(flops=6 * tok * d_half * ff, bytes_accessed=12 * d_half * ff,
                                          transcendentals=0),
            compiler_params=pltpu.CompilerParams(vmem_limit_bytes=34 * 1024 * 1024),
        )(h, da, db, pltpu.with_memory_space_constraint(xc, pltpu.HBM), gc)
        y, dx = pl.pallas_call(
            _finish,
            name="finish",
            out_shape=(S((rows, d_full), BF16), S((rows, d_full), BF16)),
            in_specs=[vm] * 2,
            out_specs=(vm, vm),
            compiler_params=pltpu.CompilerParams(vmem_limit_bytes=6 * 1024 * 1024),
        )(y, parts)
        return y, dx, dwg, dwu, dwd

    row_spec = P(("dp", "tp"), None)
    up_spec = P("dp", "tp")
    down_spec = P("tp", "dp")
    return jax.shard_map(local_step, mesh=mesh,
                         in_specs=(row_spec, up_spec, up_spec, down_spec, row_spec),
                         out_specs=(row_spec, row_spec, up_spec, up_spec, down_spec),
                         check_vma=False)
```

```python
import functools

import jax
import jax.numpy as jnp
from jax import lax
from jax.experimental import pallas as pl
from jax.experimental.pallas import tpu as pltpu
from jax.sharding import PartitionSpec as P

MESH = pl.DeviceIdType.MESH
F32 = jnp.float32
BF16 = jnp.bfloat16

NT = (((1,), (1,)), ((), ()))
TN = (((0,), (0,)), ((), ()))

FC = 512
DC = 512
PIECES = ((0, 512), (512, 512), (1024, 256), (1280, 256))
FRONT = 1536
SPLIT = 2
RB = 32


def _front(x_hbm, wg_hbm, wu_hbm, wd_hbm, gy_hbm,
           y_ref, xc_out, gc, h, da, db, p_out,
           x_v, gy_v, wg, wu, wd, xc,
           pa, pb, pg, ra, rb, rg, sd,
           yp, s1, r1, s2, r2, sc, rc, yk, dxp,
           w_sem, o_sem, xs, xrs, gs, grs, es, ers, ys, yrs):
    rows, d_full = x_v.shape
    tok, d_half = xc.shape
    half = tok // 2
    nf = wg.shape[1] // FC
    nd = d_half // DC
    t = lax.axis_index("tp")
    c = lax.axis_index("dp")
    ty, tx = t // 2, t % 2
    tx_n = ty * 2 + 1 - tx
    ty_n = (1 - ty) * 2 + tx
    t_d = 3 - t
    t1 = (1 - c) * tx_n + c * ty_n
    t2 = (1 - c) * ty_n + c * tx_n
    order = ((t_d, c), (t_d, 1 - c), (tx_n, c), (tx_n, 1 - c), (ty_n, c), (ty_n, 1 - c), (t, 1 - c))

    def rows_of(q, chip):
        return pl.ds(pl.multiple_of((q * 4 + chip) * rows, rows), rows)

    def cols_of(q):
        return pl.ds(pl.multiple_of(q * d_half, d_half), d_half)

    cx = pltpu.make_async_copy(x_hbm, x_v, w_sem.at[0])
    cg = pltpu.make_async_copy(gy_hbm, gy_v, w_sem.at[1])
    cw = [pltpu.make_async_copy(a, b, w_sem.at[2 + i])
          for i, (a, b) in enumerate(((wg_hbm, wg), (wu_hbm, wu), (wd_hbm, wd)))]
    cx.start()
    cg.start()
    for w in cw:
        w.start()

    barrier = pltpu.get_barrier_semaphore()
    for chip, q in order:
        pl.semaphore_signal(barrier, inc=1, device_id={"tp": chip, "dp": q}, device_id_type=MESH)
    pl.semaphore_wait(barrier, 7)

    def remote(src, dst, ssem, rsem, chip, q):
        cp = pltpu.make_async_remote_copy(src_ref=src, dst_ref=dst, send_sem=ssem, recv_sem=rsem,
                                          device_id={"tp": chip, "dp": q}, device_id_type=MESH)
        cp.start()
        return cp

    def swap(src, dst, i):
        return remote(src, dst, es.at[i], ers.at[i], t, 1 - c)

    def spread(own, cols, ssem, rsem):
        return [remote(own.at[:, cols_of(q)], cols.at[rows_of(c, t), :], ssem.at[k], rsem.at[k], chip, q)
                for k, (chip, q) in enumerate(order)]

    cx.wait()
    sx = spread(x_v, xc, xs, xrs)
    xc[rows_of(c, t), :] = x_v[:, cols_of(c)]
    cg.wait()
    for cp in sx:
        cp.wait_send()
    sg = spread(gy_v, gc, gs, grs)
    gc[rows_of(c, t), :] = gy_v[:, cols_of(c)]

    mine = pl.multiple_of(c * half, half)
    theirs = pl.ds(pl.multiple_of((1 - c) * half, half), half)
    cw[0].wait()
    cw[1].wait()
    for cp in sx:
        cp.wait_recv()
    out_x = pltpu.make_async_copy(xc, xc_out, o_sem.at[0])
    out_x.start()
    cps = {}

    def swap_part(part, got, j, i):
        if j < SPLIT:
            return swap(part.at[j, theirs, :], got.at[j, pl.ds(0, half), :], i)
        return swap(part.at[j], got.at[j], i)

    for j in range(nf):
        f = slice(j * FC, (j + 1) * FC)
        pa[j] = jnp.dot(xc[...], wg[:, f], preferred_element_type=F32)
        cps["a", j] = swap_part(pa, ra, j, 6 * j)
        pb[j] = jnp.dot(xc[...], wu[:, f], preferred_element_type=F32)
        cps["b", j] = swap_part(pb, rb, j, 6 * j + 1)

    def blocks(j):
        for i in range(0, half if j < SPLIT else tok, RB):
            yield pl.ds(pl.multiple_of(mine + i, RB), RB) if j < SPLIT else slice(i, i + RB), slice(i, i + RB)

    for j in range(nf):
        f = slice(j * FC, (j + 1) * FC)
        cps["a", j].wait_recv()
        cps["b", j].wait_recv()
        for r, i in blocks(j):
            a = pa[j, r, :] + ra[j, i, :]
            b = pb[j, r, :] + rb[j, i, :]
            s = jax.nn.sigmoid(a)
            u = a * s
            h[r, f] = (u * b).astype(BF16)
            sd[j, i, :] = s * (1.0 + a * (1.0 - s))
            ra[j, i, :] = u
            rb[j, i, :] = b
        if j < SPLIT:
            own = h.at[pl.ds(mine, half), f]
            cps["h", j] = swap(own, own, 6 * j + 3)
    def y_part(n, pieces):
        o = slice(n * DC, (n + 1) * DC)
        yp[:, o] = jnp.dot(h[...], wd[:, o], preferred_element_type=F32)
        for p in pieces:
            o = slice(PIECES[p][0], sum(PIECES[p]))
            for q in range(2):
                for e, chip in enumerate((t1, t_d)):
                    s1[p][(q * 2 + e) * rows:(q * 2 + e + 1) * rows, :] = yp[rows_of(q, chip), o]
            cps["1", p] = remote(s1[p], r1[p], ys.at[4 * p], yrs.at[4 * p], t1, c)

    def y_step(p):
        o = slice(PIECES[p][0], sum(PIECES[p]))
        cps["1", p].wait_recv()

        def got(q, e):
            return r1[p][pl.ds(pl.multiple_of((q * 2 + e) * rows, rows), rows), :]

        s2[p][0] = yp[rows_of(c, t2), o] + got(c, 1)
        s2[p][1] = yp[rows_of(1 - c, t2), o] + got(1 - c, 1)
        cps["2", p] = remote(s2[p].at[0], r2[p].at[0], ys.at[4 * p + 1], yrs.at[4 * p + 1], t2, c)
        cps["3", p] = remote(s2[p].at[1], r2[p].at[1], ys.at[4 * p + 2], yrs.at[4 * p + 2], t2, 1 - c)
        sc[p][...] = yp[rows_of(1 - c, t), o] + got(1 - c, 0)
        cps["4", p] = remote(sc[p], rc[p], ys.at[4 * p + 3], yrs.at[4 * p + 3], t, 1 - c)
        yk[p][...] = yp[rows_of(c, t), o] + got(c, 0)

    def y_done(p):
        for k in "234":
            cps[k, p].wait_recv()
        o, w = PIECES[p]
        for q, tot in ((c, yk[p][...] + r2[p][0]), (1 - c, rc[p][...] + r2[p][1])):
            cols = pl.ds(pl.multiple_of(q * d_half + o, 128), w)
            y_ref[:, cols] = (x_v[:, cols].astype(F32) + tot).astype(BF16)

    def g_part(j):
        pg[j] = lax.dot_general(gc[...], wd[j * FC:(j + 1) * FC, :], NT, preferred_element_type=F32)
        cps["g", j] = swap_part(pg, rg, j, 6 * j + 2)

    def grad(j):
        f = slice(j * FC, (j + 1) * FC)
        cps["g", j].wait_recv()
        for r, i in blocks(j):
            g = pg[j, r, :] + rg[j, i, :]
            da[r, f] = (g * rb[j, i, :] * sd[j, i, :]).astype(BF16)
            db[r, f] = (g * ra[j, i, :]).astype(BF16)
        if j < SPLIT:
            own = da.at[pl.ds(mine, half), f]
            cps["da", j] = swap(own, own, 6 * j + 4)
            own = db.at[pl.ds(mine, half), f]
            cps["db", j] = swap(own, own, 6 * j + 5)

    def dx_part(j):
        f = slice(j * FC, (j + 1) * FC)
        if j < SPLIT:
            cps["da", j].wait_recv()
            cps["db", j].wait_recv()
        for n in range(nd):
            o = slice(n * DC, (n + 1) * DC)
            part = (lax.dot_general(da[:, f], wg[o, f], NT, preferred_element_type=F32)
                    + lax.dot_general(db[:, f], wu[o, f], NT, preferred_element_type=F32))
            dxp[:, o] = part if j == 0 else dxp[:, o] + part

    cw[2].wait()
    for j in range(SPLIT):
        cps["h", j].wait_recv()
    y_part(0, (0,))
    y_part(1, (1,))
    y_part(2, (2, 3))
    for cp in sg:
        cp.wait_recv()
    g_part(0)
    g_part(1)
    g_part(2)
    grad(0)
    g_part(3)
    grad(1)
    y_step(0)
    dx_part(0)
    grad(2)
    y_step(1)
    dx_part(1)
    grad(3)
    y_step(2)
    y_step(3)
    dx_part(2)
    dx_part(3)

    for i in range(8):
        r = ((i % 2) * 4 + i // 2) * rows
        p_out[i, :, :d_half] = dxp[r:r + rows, :]
        if FRONT < d_half:
            p_out[i, :, d_half:] = yp[r:r + rows, FRONT:]
    for q in range(2):
        p_out[t * 2 + q, :, :d_half] += gc[rows_of(q, t), :].astype(F32)
        if FRONT < d_half:
            p_out[t * 2 + q, :, d_half:] += xc[rows_of(q, t), FRONT:].astype(F32)
    for p in range(len(PIECES)):
        y_done(p)

    for cp in sg:
        cp.wait_send()
    for cp in cps.values():
        cp.wait_send()
    out_x.wait()


def _finish(p, dx_ref):
    d_half = p.shape[2]
    for q in range(2):
        dx_ref[:, q * d_half:(q + 1) * d_half] = (p[q] + p[q + 2] + p[q + 4] + p[q + 6]).astype(BF16)


def _grads(h, da, db, xc_hbm, gc, y, dwd_hbm, dwg_hbm, dwu_hbm, y_hbm, buf_d, buf_g, xc, sem_d, sem_g, sem_x, sem_y):
    ff = h.shape[1]
    d_half = xc.shape[1]
    nb_d, tr_d = buf_d.shape[:2]
    nb_g, tr_g = buf_g.shape[:2]
    cx = pltpu.make_async_copy(xc_hbm, xc, sem_x)
    cx.start()
    cy = pltpu.make_async_copy(y, y_hbm, sem_y)
    cy.start()

    def run(lhs, rhs, out, buf, sem, n, tr, nb, start, prev_out):
        def step(i, carry):
            slot = lax.rem(i + start, nb)
            r = pl.multiple_of(i * tr, tr)

            def drain():
                pltpu.make_async_copy(buf.at[slot], prev_out.at[pl.ds(0, tr), :], sem.at[slot]).wait()

            if start >= nb:
                drain()
            else:
                pl.when(i + start >= nb)(drain)
            buf[slot] = lax.dot_general(lhs[:, pl.ds(r, tr)], rhs[...], TN, preferred_element_type=F32)
            pltpu.make_async_copy(buf.at[slot], out.at[pl.ds(r, tr), :], sem.at[slot]).start()
            return carry

        lax.fori_loop(0, n, step, 0)

    n_d = ff // tr_d
    n_g = d_half // tr_g
    run(h, gc, dwd_hbm, buf_d, sem_d, n_d, tr_d, nb_d, 0, dwd_hbm)
    cx.wait()
    run(xc, da, dwg_hbm, buf_g, sem_g, n_g, tr_g, nb_g, 0, dwg_hbm)
    run(xc, db, dwu_hbm, buf_g, sem_g, n_g, tr_g, nb_g, n_g, dwu_hbm)
    for s in range(nb_d):
        pltpu.make_async_copy(buf_d.at[s], dwd_hbm.at[pl.ds(0, tr_d), :], sem_d.at[s]).wait()
    for s in range(nb_g):
        pltpu.make_async_copy(buf_g.at[s], dwu_hbm.at[pl.ds(0, tr_g), :], sem_g.at[s]).wait()
    cy.wait()


def solution(mesh):
    def local_step(x, wg, wu, wd, gy):
        rows, d_full = x.shape
        d_half, ff = wg.shape
        tok = rows * 8
        nf = ff // FC
        nd = d_half // DC
        any_ = pl.BlockSpec(memory_space=pl.ANY)
        hbm = pl.BlockSpec(memory_space=pltpu.HBM)
        vm = pl.BlockSpec(memory_space=pltpu.VMEM)
        S = jax.ShapeDtypeStruct
        dma = pltpu.SemaphoreType.DMA
        full = pltpu.VMEM((nf, tok, FC), F32)
        y, xc, gc, h, da, db, parts = pl.pallas_call(
            _front,
            name="front",
            out_shape=(S((rows, d_full), BF16),
                       pltpu.HBM((tok, d_half), BF16), S((tok, d_half), BF16),
                       S((tok, ff), BF16), S((tok, ff), BF16), S((tok, ff), BF16))
            + (S((8, rows, 2 * d_half - FRONT), F32),),
            in_specs=[hbm] * 5,
            out_specs=(vm, hbm, vm, vm, vm, vm, vm),
            scratch_shapes=[
                pltpu.VMEM((rows, d_full), BF16), pltpu.VMEM((rows, d_full), BF16),
                pltpu.VMEM((d_half, ff), BF16), pltpu.VMEM((d_half, ff), BF16), pltpu.VMEM((ff, d_half), BF16),
                pltpu.VMEM((tok, d_half), BF16),
                full, full, full, full, full, full, full,
                pltpu.VMEM((tok, d_half), F32),
                [pltpu.VMEM((4 * rows, w), F32) for _, w in PIECES], [pltpu.VMEM((4 * rows, w), F32) for _, w in PIECES],
                [pltpu.VMEM((2, rows, w), F32) for _, w in PIECES], [pltpu.VMEM((2, rows, w), F32) for _, w in PIECES],
                *([pltpu.VMEM((rows, w), F32) for _, w in PIECES] for _ in range(3)),
                pltpu.VMEM((tok, d_half), F32),
                dma((5,)), dma((1,)), dma((7,)), dma((7,)), dma((7,)), dma((7,)),
                dma((6 * nf,)), dma((6 * nf,)), dma((4 * len(PIECES),)), dma((4 * len(PIECES),)),
            ],
            compiler_params=pltpu.CompilerParams(collective_id=0, has_side_effects=True,
                                                 vmem_limit_bytes=50 * 1024 * 1024),
        )(*(pltpu.with_memory_space_constraint(v, pltpu.HBM) for v in (x, wg, wu, wd, gy)))
        parts = lax.all_to_all(parts, ("tp", "dp"), 0, 0, tiled=True)

        tr = 256
        dwd, dwg, dwu, y = pl.pallas_call(
            _grads,
            name="grads",
            out_shape=(S((ff, d_half), F32), S((d_half, ff), F32), S((d_half, ff), F32), S((rows, d_full), BF16)),
            in_specs=[vm, vm, vm, hbm, vm, vm],
            out_specs=(any_, any_, any_, hbm),
            scratch_shapes=[pltpu.VMEM((8, tr, d_half), F32), pltpu.VMEM((6, tr, ff), F32),
                            pltpu.VMEM((tok, d_half), BF16), dma((8,)), dma((6,)), dma(()), dma(())],
            cost_estimate=pl.CostEstimate(flops=6 * tok * d_half * ff, bytes_accessed=12 * d_half * ff,
                                          transcendentals=0),
            compiler_params=pltpu.CompilerParams(vmem_limit_bytes=34 * 1024 * 1024),
        )(h, da, db, pltpu.with_memory_space_constraint(xc, pltpu.HBM), gc, y)
        dx = pl.pallas_call(
            _finish,
            name="finish",
            out_shape=S((rows, d_full), BF16),
            in_specs=[vm],
            out_specs=vm,
            compiler_params=pltpu.CompilerParams(vmem_limit_bytes=6 * 1024 * 1024),
        )(parts)
        return y, dx, dwg, dwu, dwd

    row_spec = P(("dp", "tp"), None)
    up_spec = P("dp", "tp")
    down_spec = P("tp", "dp")
    return jax.shard_map(local_step, mesh=mesh,
                         in_specs=(row_spec, up_spec, up_spec, down_spec, row_spec),
                         out_specs=(row_spec, row_spec, up_spec, up_spec, down_spec),
                         check_vma=False)
```

```python
import functools

import jax
import jax.numpy as jnp
from jax import lax
from jax.experimental import pallas as pl
from jax.experimental.pallas import tpu as pltpu
from jax.sharding import PartitionSpec as P

MESH = pl.DeviceIdType.MESH
F32 = jnp.float32
BF16 = jnp.bfloat16

NT = (((1,), (1,)), ((), ()))
TN = (((0,), (0,)), ((), ()))

FC = 512
DC = 512
PIECES = ((0, 512), (512, 512), (1024, 256), (1280, 256))
FRONT = 1536
SPLIT = 2
RB = 32


def _front(x_hbm, wg_hbm, wu_hbm, wd_hbm, gy_hbm,
           y_ref, xc_out, gc, h, da, db, p_out,
           x_v, gy_v, wg, wu, wd, xc,
           pa, pb, pg, ra, rb, rg, sd,
           yp, s1, r1, s2, r2, sc, rc, yk, dxp,
           w_sem, o_sem, xs, xrs, gs, grs, es, ers, ys, yrs):
    rows, d_full = x_v.shape
    tok, d_half = xc.shape
    half = tok // 2
    nf = wg.shape[1] // FC
    nd = d_half // DC
    t = lax.axis_index("tp")
    c = lax.axis_index("dp")
    ty, tx = t // 2, t % 2
    tx_n = ty * 2 + 1 - tx
    ty_n = (1 - ty) * 2 + tx
    t_d = 3 - t
    t1 = (1 - c) * tx_n + c * ty_n
    t2 = (1 - c) * ty_n + c * tx_n
    order = ((t_d, c), (t_d, 1 - c), (tx_n, c), (tx_n, 1 - c), (ty_n, c), (ty_n, 1 - c), (t, 1 - c))

    def rows_of(q, chip):
        return pl.ds(pl.multiple_of((q * 4 + chip) * rows, rows), rows)

    def cols_of(q):
        return pl.ds(pl.multiple_of(q * d_half, d_half), d_half)

    cx = pltpu.make_async_copy(x_hbm, x_v, w_sem.at[0])
    cg = pltpu.make_async_copy(gy_hbm, gy_v, w_sem.at[1])
    cw = [pltpu.make_async_copy(a, b, w_sem.at[2 + i])
          for i, (a, b) in enumerate(((wg_hbm, wg), (wu_hbm, wu), (wd_hbm, wd)))]
    cx.start()
    cg.start()
    for w in cw:
        w.start()

    barrier = pltpu.get_barrier_semaphore()
    for chip, q in order:
        pl.semaphore_signal(barrier, inc=1, device_id={"tp": chip, "dp": q}, device_id_type=MESH)
    pl.semaphore_wait(barrier, 7)

    def remote(src, dst, ssem, rsem, chip, q):
        cp = pltpu.make_async_remote_copy(src_ref=src, dst_ref=dst, send_sem=ssem, recv_sem=rsem,
                                          device_id={"tp": chip, "dp": q}, device_id_type=MESH)
        cp.start()
        return cp

    def swap(src, dst, i):
        return remote(src, dst, es.at[i], ers.at[i], t, 1 - c)

    def spread(own, cols, ssem, rsem):
        return [remote(own.at[:, cols_of(q)], cols.at[rows_of(c, t), :], ssem.at[k], rsem.at[k], chip, q)
                for k, (chip, q) in enumerate(order)]

    cx.wait()
    sx = spread(x_v, xc, xs, xrs)
    xc[rows_of(c, t), :] = x_v[:, cols_of(c)]
    cg.wait()
    for cp in sx:
        cp.wait_send()
    sg = spread(gy_v, gc, gs, grs)
    gc[rows_of(c, t), :] = gy_v[:, cols_of(c)]

    mine = pl.multiple_of(c * half, half)
    theirs = pl.ds(pl.multiple_of((1 - c) * half, half), half)
    cw[0].wait()
    cw[1].wait()
    for cp in sx:
        cp.wait_recv()
    out_x = pltpu.make_async_copy(xc, xc_out, o_sem.at[0])
    out_x.start()
    cps = {}

    def swap_part(part, got, j, i):
        if j < SPLIT:
            return swap(part.at[j, theirs, :], got.at[j, pl.ds(0, half), :], i)
        return swap(part.at[j], got.at[j], i)

    for j in range(nf):
        f = slice(j * FC, (j + 1) * FC)
        pa[j] = jnp.dot(xc[...], wg[:, f], preferred_element_type=F32)
        cps["a", j] = swap_part(pa, ra, j, 6 * j)
        pb[j] = jnp.dot(xc[...], wu[:, f], preferred_element_type=F32)
        cps["b", j] = swap_part(pb, rb, j, 6 * j + 1)

    def blocks(j):
        for i in range(0, half if j < SPLIT else tok, RB):
            yield pl.ds(pl.multiple_of(mine + i, RB), RB) if j < SPLIT else slice(i, i + RB), slice(i, i + RB)

    for j in range(nf):
        f = slice(j * FC, (j + 1) * FC)
        cps["a", j].wait_recv()
        cps["b", j].wait_recv()
        for r, i in blocks(j):
            a = pa[j, r, :] + ra[j, i, :]
            b = pb[j, r, :] + rb[j, i, :]
            s = jax.nn.sigmoid(a)
            u = a * s
            h[r, f] = (u * b).astype(BF16)
            sd[j, i, :] = s * (1.0 + a * (1.0 - s))
            ra[j, i, :] = u
            rb[j, i, :] = b
        if j < SPLIT:
            own = h.at[pl.ds(mine, half), f]
            cps["h", j] = swap(own, own, 6 * j + 3)
    def y_part(n, pieces):
        o = slice(n * DC, (n + 1) * DC)
        yp[:, o] = jnp.dot(h[...], wd[:, o], preferred_element_type=F32)
        for p in pieces:
            o = slice(PIECES[p][0], sum(PIECES[p]))
            for q in range(2):
                for e, chip in enumerate((t1, t_d)):
                    s1[p][(q * 2 + e) * rows:(q * 2 + e + 1) * rows, :] = yp[rows_of(q, chip), o]
            cps["1", p] = remote(s1[p], r1[p], ys.at[4 * p], yrs.at[4 * p], t1, c)

    def y_step(p):
        o = slice(PIECES[p][0], sum(PIECES[p]))
        cps["1", p].wait_recv()

        def got(q, e):
            return r1[p][pl.ds(pl.multiple_of((q * 2 + e) * rows, rows), rows), :]

        s2[p][0] = yp[rows_of(c, t2), o] + got(c, 1)
        s2[p][1] = yp[rows_of(1 - c, t2), o] + got(1 - c, 1)
        cps["2", p] = remote(s2[p].at[0], r2[p].at[0], ys.at[4 * p + 1], yrs.at[4 * p + 1], t2, c)
        cps["3", p] = remote(s2[p].at[1], r2[p].at[1], ys.at[4 * p + 2], yrs.at[4 * p + 2], t2, 1 - c)
        sc[p][...] = yp[rows_of(1 - c, t), o] + got(1 - c, 0)
        cps["4", p] = remote(sc[p], rc[p], ys.at[4 * p + 3], yrs.at[4 * p + 3], t, 1 - c)
        yk[p][...] = yp[rows_of(c, t), o] + got(c, 0)

    def y_done(p):
        for k in "234":
            cps[k, p].wait_recv()
        o, w = PIECES[p]
        for q, tot in ((c, yk[p][...] + r2[p][0]), (1 - c, rc[p][...] + r2[p][1])):
            cols = pl.ds(pl.multiple_of(q * d_half + o, 128), w)
            y_ref[:, cols] = (x_v[:, cols].astype(F32) + tot).astype(BF16)

    def g_part(j):
        pg[j] = lax.dot_general(gc[...], wd[j * FC:(j + 1) * FC, :], NT, preferred_element_type=F32)
        cps["g", j] = swap_part(pg, rg, j, 6 * j + 2)

    def grad(j):
        f = slice(j * FC, (j + 1) * FC)
        cps["g", j].wait_recv()
        for r, i in blocks(j):
            g = pg[j, r, :] + rg[j, i, :]
            da[r, f] = (g * rb[j, i, :] * sd[j, i, :]).astype(BF16)
            db[r, f] = (g * ra[j, i, :]).astype(BF16)
        if j < SPLIT:
            own = da.at[pl.ds(mine, half), f]
            cps["da", j] = swap(own, own, 6 * j + 4)
            own = db.at[pl.ds(mine, half), f]
            cps["db", j] = swap(own, own, 6 * j + 5)

    def dx_part(j):
        f = slice(j * FC, (j + 1) * FC)
        if j < SPLIT:
            cps["da", j].wait_recv()
            cps["db", j].wait_recv()
        for n in range(nd):
            o = slice(n * DC, (n + 1) * DC)
            part = (lax.dot_general(da[:, f], wg[o, f], NT, preferred_element_type=F32)
                    + lax.dot_general(db[:, f], wu[o, f], NT, preferred_element_type=F32))
            dxp[:, o] = part if j == 0 else dxp[:, o] + part

    cw[2].wait()
    for j in range(SPLIT):
        cps["h", j].wait_recv()
    y_part(0, (0,))
    y_part(1, (1,))
    y_part(2, (2, 3))
    for cp in sg:
        cp.wait_recv()
    g_part(0)
    g_part(1)
    g_part(2)
    grad(0)
    g_part(3)
    grad(1)
    y_step(0)
    dx_part(0)
    grad(2)
    y_step(1)
    dx_part(1)
    grad(3)
    y_step(2)
    y_step(3)
    dx_part(2)
    dx_part(3)

    for i in range(8):
        r = ((i % 2) * 4 + i // 2) * rows
        p_out[i, :, :d_half] = dxp[r:r + rows, :]
        if FRONT < d_half:
            p_out[i, :, d_half:] = yp[r:r + rows, FRONT:]
    for q in range(2):
        p_out[t * 2 + q, :, :d_half] += gc[rows_of(q, t), :].astype(F32)
        if FRONT < d_half:
            p_out[t * 2 + q, :, d_half:] += xc[rows_of(q, t), FRONT:].astype(F32)
    for p in range(len(PIECES)):
        y_done(p)

    for cp in sg:
        cp.wait_send()
    for cp in cps.values():
        cp.wait_send()
    out_x.wait()


def _finish(p, dx_ref):
    d_half = p.shape[2]
    for q in range(2):
        dx_ref[:, q * d_half:(q + 1) * d_half] = (p[q] + p[q + 2] + p[q + 4] + p[q + 6]).astype(BF16)


def _grads(h, da, db, xc_hbm, gc, y, dwd_hbm, dwg_hbm, dwu_hbm, y_hbm, buf_d, buf_g, xc, sem_d, sem_g, sem_x, sem_y):
    ff = h.shape[1]
    d_half = xc.shape[1]
    nb_d, tr_d = buf_d.shape[:2]
    nb_g, tr_g = buf_g.shape[:2]
    cx = pltpu.make_async_copy(xc_hbm, xc, sem_x)
    cx.start()
    cy = pltpu.make_async_copy(y, y_hbm, sem_y)
    cy.start()

    def run(lhs, rhs, out, buf, sem, n, tr, nb, start, prev_out, first=0):
        def step(i, carry):
            slot = lax.rem(i + start, nb)
            r = pl.multiple_of(i * tr, tr)

            def drain():
                pltpu.make_async_copy(buf.at[slot], prev_out.at[pl.ds(0, tr), :], sem.at[slot]).wait()

            if start >= nb:
                drain()
            else:
                pl.when(i + start >= nb)(drain)
            buf[slot] = lax.dot_general(lhs[:, pl.ds(r, tr)], rhs[...], TN, preferred_element_type=F32)
            pltpu.make_async_copy(buf.at[slot], out.at[pl.ds(r, tr), :], sem.at[slot]).start()
            return carry

        lax.fori_loop(first, n, step, 0)

    n_d = ff // tr_d
    n_g = d_half // tr_g
    for r in range(0, tr_d, tr_d // 2):
        i = pl.ds(r, tr_d // 2)
        buf_d[0, i, :] = lax.dot_general(h[:, i], gc[...], TN, preferred_element_type=F32)
        pltpu.make_async_copy(buf_d.at[0, i, :], dwd_hbm.at[i, :], sem_d.at[0]).start()
    run(h, gc, dwd_hbm, buf_d, sem_d, n_d, tr_d, nb_d, 0, dwd_hbm, 1)
    cx.wait()
    run(xc, da, dwg_hbm, buf_g, sem_g, n_g, tr_g, nb_g, 0, dwg_hbm)
    run(xc, db, dwu_hbm, buf_g, sem_g, n_g, tr_g, nb_g, n_g, dwu_hbm)
    for s in range(nb_d):
        pltpu.make_async_copy(buf_d.at[s], dwd_hbm.at[pl.ds(0, tr_d), :], sem_d.at[s]).wait()
    for s in range(nb_g):
        pltpu.make_async_copy(buf_g.at[s], dwu_hbm.at[pl.ds(0, tr_g), :], sem_g.at[s]).wait()
    cy.wait()


def solution(mesh):
    def local_step(x, wg, wu, wd, gy):
        rows, d_full = x.shape
        d_half, ff = wg.shape
        tok = rows * 8
        nf = ff // FC
        nd = d_half // DC
        any_ = pl.BlockSpec(memory_space=pl.ANY)
        hbm = pl.BlockSpec(memory_space=pltpu.HBM)
        vm = pl.BlockSpec(memory_space=pltpu.VMEM)
        S = jax.ShapeDtypeStruct
        dma = pltpu.SemaphoreType.DMA
        full = pltpu.VMEM((nf, tok, FC), F32)
        y, xc, gc, h, da, db, parts = pl.pallas_call(
            _front,
            name="front",
            out_shape=(S((rows, d_full), BF16),
                       pltpu.HBM((tok, d_half), BF16), S((tok, d_half), BF16),
                       S((tok, ff), BF16), S((tok, ff), BF16), S((tok, ff), BF16))
            + (S((8, rows, 2 * d_half - FRONT), F32),),
            in_specs=[hbm] * 5,
            out_specs=(vm, hbm, vm, vm, vm, vm, vm),
            scratch_shapes=[
                pltpu.VMEM((rows, d_full), BF16), pltpu.VMEM((rows, d_full), BF16),
                pltpu.VMEM((d_half, ff), BF16), pltpu.VMEM((d_half, ff), BF16), pltpu.VMEM((ff, d_half), BF16),
                pltpu.VMEM((tok, d_half), BF16),
                full, full, full, full, full, full, full,
                pltpu.VMEM((tok, d_half), F32),
                [pltpu.VMEM((4 * rows, w), F32) for _, w in PIECES], [pltpu.VMEM((4 * rows, w), F32) for _, w in PIECES],
                [pltpu.VMEM((2, rows, w), F32) for _, w in PIECES], [pltpu.VMEM((2, rows, w), F32) for _, w in PIECES],
                *([pltpu.VMEM((rows, w), F32) for _, w in PIECES] for _ in range(3)),
                pltpu.VMEM((tok, d_half), F32),
                dma((5,)), dma((1,)), dma((7,)), dma((7,)), dma((7,)), dma((7,)),
                dma((6 * nf,)), dma((6 * nf,)), dma((4 * len(PIECES),)), dma((4 * len(PIECES),)),
            ],
            compiler_params=pltpu.CompilerParams(collective_id=0, has_side_effects=True,
                                                 vmem_limit_bytes=50 * 1024 * 1024),
        )(*(pltpu.with_memory_space_constraint(v, pltpu.HBM) for v in (x, wg, wu, wd, gy)))
        parts = lax.all_to_all(parts, ("tp", "dp"), 0, 0, tiled=True)

        tr = 256
        dwd, dwg, dwu, y = pl.pallas_call(
            _grads,
            name="grads",
            out_shape=(S((ff, d_half), F32), S((d_half, ff), F32), S((d_half, ff), F32), S((rows, d_full), BF16)),
            in_specs=[vm, vm, vm, hbm, vm, vm],
            out_specs=(any_, any_, any_, hbm),
            scratch_shapes=[pltpu.VMEM((8, tr, d_half), F32), pltpu.VMEM((6, tr, ff), F32),
                            pltpu.VMEM((tok, d_half), BF16), dma((8,)), dma((6,)), dma(()), dma(())],
            cost_estimate=pl.CostEstimate(flops=6 * tok * d_half * ff, bytes_accessed=12 * d_half * ff,
                                          transcendentals=0),
            compiler_params=pltpu.CompilerParams(vmem_limit_bytes=34 * 1024 * 1024),
        )(h, da, db, pltpu.with_memory_space_constraint(xc, pltpu.HBM), gc, y)
        dx = pl.pallas_call(
            _finish,
            name="finish",
            out_shape=S((rows, d_full), BF16),
            in_specs=[vm],
            out_specs=vm,
            compiler_params=pltpu.CompilerParams(vmem_limit_bytes=6 * 1024 * 1024),
        )(parts)
        return y, dx, dwg, dwu, dwd

    row_spec = P(("dp", "tp"), None)
    up_spec = P("dp", "tp")
    down_spec = P("tp", "dp")
    return jax.shard_map(local_step, mesh=mesh,
                         in_specs=(row_spec, up_spec, up_spec, down_spec, row_spec),
                         out_specs=(row_spec, row_spec, up_spec, up_spec, down_spec),
                         check_vma=False)
```
